32 devices in a mesh: dp: 1 (over z), ep: 32 (over y, x, core).
Axes of the slice: x: 4, y: 4, z: 1, core: 2. Of those that a mesh axis runs over, the one named last changes fastest.
The devices are a block of a 4x4x8 slice.
Arguments:
- h0: bfloat16 [32, 1024, 2048], P(('dp', 'ep'))
- idx: int32 [32, 1024, 6], P(('dp', 'ep'))
- slot: int32 [32, 1024, 6], P(('dp', 'ep'))
- ln_attn: bfloat16 [2048], replicated
- wq: bfloat16 [2048, 2048], replicated
- wk: bfloat16 [2048, 2048], replicated
- wv: bfloat16 [2048, 2048], replicated
- wo: bfloat16 [2048, 2048], replicated
- ln_ffn: bfloat16 [2048], replicated
- ws1: bfloat16 [2048, 2816], replicated
- ws3: bfloat16 [2048, 2816], replicated
- ws2: bfloat16 [2816, 2048], replicated
- ln_moe: bfloat16 [2048], replicated
- wr: bfloat16 [2048, 64], replicated
- ue1: bfloat16 [64, 2048, 1408], P('ep')
- ue3: bfloat16 [64, 2048, 1408], P('ep')
- ue2: bfloat16 [64, 1408, 2048], P('ep')
Outputs:
- output: bfloat16 [32, 1024, 2048], P(('dp', 'ep'))
All inputs are finite; a program needn't handle non-finite values.
Results may differ from the reference program's by a relative error of at most 0.0102654.
Values are sent between devices in bfloat16 or wider.
A program may use at most 768 MiB of HBM per device.

```python
import jax
import jax.numpy as jnp
from jax import lax

D = 2048
HEADS = 16
HEAD = 128
EXPERTS = 64
TOP = 6
FE = 1408
FS = 2816
SEQ = 1024
SEQS = 1
G = 32
CAP = 192

T = SEQS * SEQ
EPS = 1e-6


def _dot(a, b):
    return jnp.dot(a, b, preferred_element_type=jnp.float32)


def _rms(x, w):
    xf = x.astype(jnp.float32)
    r = lax.rsqrt(jnp.mean(xf * xf, axis=-1, keepdims=True) + EPS)
    return (xf * r * w.astype(jnp.float32)).astype(jnp.bfloat16)


def _rope(x):
    half = HEAD // 2
    freq = 10000.0 ** (-jnp.arange(half, dtype=jnp.float32) / half)
    ang = jnp.arange(SEQ, dtype=jnp.float32)[:, None] * freq[None, :]
    c = jnp.cos(ang)[:, None, :]
    s = jnp.sin(ang)[:, None, :]
    x1, x2 = x[..., :half], x[..., half:]
    return jnp.concatenate([x1 * c - x2 * s, x2 * c + x1 * s], axis=-1)


def _normal(key, shape, scale):
    return (jax.random.normal(key, shape, jnp.float32) * scale).astype(jnp.bfloat16)


def _scale(key):
    return jax.random.uniform(key, (D,), jnp.float32, 0.8, 1.2).astype(jnp.bfloat16)


def _expert_weight(weight_key):
    levels = jnp.sum(jax.random.randint(weight_key, (9, EXPERTS), 0, 10, jnp.int32), axis=0)
    hot_bias = 12 * (jnp.arange(EXPERTS) < EXPERTS // G).astype(jnp.int32)
    quarter = jnp.maximum(levels + hot_bias - 16, 0)
    return jnp.left_shift(4 + quarter % 4, quarter // 4).astype(jnp.int32)


def _route(route_key, weight):
    draw_rows = jax.random.bits(route_key, (T, TOP), jnp.uint32)

    def step(counts, draw_row):
        open_weight = jnp.where(counts < CAP, weight, 0).astype(jnp.int32)
        picked_list = []
        for choice in range(TOP):
            cumulative = jnp.cumsum(open_weight)
            total_weight = cumulative[-1].astype(jnp.uint32)
            target_val = (draw_row[choice] % total_weight).astype(jnp.int32)
            pick_id = jnp.searchsorted(cumulative, target_val, side='right').astype(jnp.int32)
            picked_list.append(pick_id)
            open_weight = open_weight.at[pick_id].set(0)
        chosen = jnp.stack(picked_list)
        return counts.at[chosen].add(1), (chosen, counts[chosen])

    _, (chosen, slots) = lax.scan(step, jnp.zeros((EXPERTS,), jnp.int32), draw_rows)
    return chosen.astype(jnp.int32), slots.astype(jnp.int32)


def setup_inputs(seed: int = 0, part: int = 0) -> dict:
    key = jax.random.PRNGKey(seed)
    kh, kr = jax.random.split(jax.random.fold_in(key, part))
    ks = jax.random.split(key, 15)
    hd = HEADS * HEAD
    expert_weight = _expert_weight(jax.random.fold_in(ks[14], 7))
    idx, slot = jax.vmap(lambda k: _route(k, expert_weight))(jax.random.split(kr, G))
    return {
        'h0': _normal(kh, (G * SEQS, SEQ, D), 1.0),
        'idx': idx.reshape(G * SEQS, SEQ, TOP),
        'slot': slot.reshape(G * SEQS, SEQ, TOP),
        'ln_attn': _scale(ks[0]),
        'wq': _normal(ks[1], (D, hd), 1.5 * D ** -0.5),
        'wk': _normal(ks[2], (D, hd), 1.5 * D ** -0.5),
        'wv': _normal(ks[3], (D, hd), D ** -0.5),
        'wo': _normal(ks[4], (hd, D), hd ** -0.5),
        'ln_ffn': _scale(ks[5]),
        'ws1': _normal(ks[6], (D, FS), D ** -0.5),
        'ws3': _normal(ks[7], (D, FS), D ** -0.5),
        'ws2': _normal(ks[8], (FS, D), FS ** -0.5),
        'ln_moe': _scale(ks[9]),
        'wr': _normal(ks[10], (D, EXPERTS), 1.5 * D ** -0.5),
        'ue1': _normal(ks[11], (EXPERTS, D, FE), D ** -0.5),
        'ue3': _normal(ks[12], (EXPERTS, D, FE), D ** -0.5),
        'ue2': _normal(ks[13], (EXPERTS, FE, D), 2.0 * FE ** -0.5),
    }


def reference(h0, idx, slot, ln_attn, wq, wk, wv, wo, ln_ffn, ws1, ws3, ws2, ln_moe, wr, ue1, ue3, ue2):
    nb = h0.shape[0]
    n = nb * SEQ
    x1 = _rms(h0, ln_attn)
    causal = jnp.arange(SEQ)[:, None] >= jnp.arange(SEQ)[None, :]

    def attn(xs):
        q = _rope(_dot(xs, wq).reshape(SEQ, HEADS, HEAD)).astype(jnp.bfloat16)
        k = _rope(_dot(xs, wk).reshape(SEQ, HEADS, HEAD)).astype(jnp.bfloat16)
        v = _dot(xs, wv).astype(jnp.bfloat16).reshape(SEQ, HEADS, HEAD)
        s = jnp.einsum('qhe,khe->hqk', q.astype(jnp.float32), k.astype(jnp.float32)) * HEAD ** -0.5
        p = jax.nn.softmax(jnp.where(causal[None], s, -1e30), axis=-1).astype(jnp.bfloat16)
        o = jnp.einsum('hqk,khe->qhe', p.astype(jnp.float32), v.astype(jnp.float32))
        return o.astype(jnp.bfloat16).reshape(SEQ, HEADS * HEAD)

    o = lax.map(attn, x1).reshape(n, HEADS * HEAD)
    h = h0.reshape(n, D)
    a = (h.astype(jnp.float32) + _dot(o, wo)).astype(jnp.bfloat16)
    x2 = _rms(a, ln_ffn)
    hs = (jax.nn.silu(_dot(x2, ws1)) * _dot(x2, ws3)).astype(jnp.bfloat16)
    f = _dot(hs, ws2)

    u = _rms(h, ln_moe)
    gi = idx.reshape(n, TOP)
    sl = slot.reshape(n, TOP)
    g = jax.nn.softmax(jnp.take_along_axis(_dot(u, wr), gi, axis=1), axis=-1)
    dev = jnp.arange(n, dtype=jnp.int32) // T
    pos = gi * (G * CAP) + dev[:, None] * CAP + sl
    src = jnp.full((EXPERTS * G * CAP,), n, jnp.int32).at[pos.reshape(-1)].set(
        jnp.arange(n * TOP, dtype=jnp.int32) // TOP)
    u_pad = jnp.concatenate([u, jnp.zeros((1, D), jnp.bfloat16)], axis=0)
    buf = u_pad[src].reshape(EXPERTS, G * CAP, D)

    def expert(args):
        x, w1, w3, w2 = args
        he = (jax.nn.silu(_dot(x, w1)) * _dot(x, w3)).astype(jnp.bfloat16)
        return _dot(he, w2).astype(jnp.bfloat16)

    y = lax.map(expert, (buf, ue1, ue3, ue2)).reshape(EXPERTS * G * CAP, D)
    m = jnp.sum(g[:, :, None] * y[pos].astype(jnp.float32), axis=1)
    out = a.astype(jnp.float32) + f + m
    return out.astype(jnp.bfloat16).reshape(nb, SEQ, D)
```

```python
import functools
import math

import jax
import jax.numpy as jnp
from jax import lax
from jax.experimental import pallas as pl
from jax.experimental.pallas import tpu as pltpu
from jax.sharding import PartitionSpec as P

HEAD = 128
EPS = 1e-6
CAP_FACTOR = 2
CORES = 2
EXTRA = 16
F32 = jnp.float32
BF16 = jnp.bfloat16
MESH = pl.DeviceIdType.MESH


def _mm(form, a, b):
    return jnp.einsum(form, a, b, preferred_element_type=jnp.float32)


def _rms(x, w):
    xf = x.astype(jnp.float32)
    r = lax.rsqrt(jnp.mean(xf * xf, axis=-1, keepdims=True) + EPS)
    return (xf * r * w.astype(jnp.float32)).astype(jnp.bfloat16)


def _rope(x):
    s, half = x.shape[1], x.shape[-1] // 2
    freq = 10000.0 ** (-jnp.arange(half, dtype=jnp.float32) / half)
    ang = jnp.arange(s, dtype=jnp.float32)[:, None] * freq[None, :]
    c = jnp.cos(ang)[None, :, None, :]
    sn = jnp.sin(ang)[None, :, None, :]
    x1, x2 = x[..., :half], x[..., half:]
    return jnp.concatenate([x1 * c - x2 * sn, x2 * c + x1 * sn], axis=-1)


def _dense(h0, ln_attn, wq, wk, wv, wo, ln_ffn, ws1, ws3, ws2):
    b, s, _ = h0.shape
    nh = wq.shape[1] // HEAD
    x1 = _rms(h0, ln_attn)
    q = _rope(_mm('bsd,de->bse', x1, wq).reshape(b, s, nh, HEAD)).astype(jnp.bfloat16)
    k = _rope(_mm('bsd,de->bse', x1, wk).reshape(b, s, nh, HEAD)).astype(jnp.bfloat16)
    v = _mm('bsd,de->bse', x1, wv).astype(jnp.bfloat16).reshape(b, s, nh, HEAD)
    sc = _mm('bqhe,bkhe->bhqk', q, k) * HEAD ** -0.5
    causal = jnp.arange(s)[:, None] >= jnp.arange(s)[None, :]
    p = jax.nn.softmax(jnp.where(causal, sc, -1e30), axis=-1).astype(jnp.bfloat16)
    o = _mm('bhqk,bkhe->bqhe', p, v).astype(jnp.bfloat16).reshape(b, s, nh * HEAD)
    a = (h0.astype(jnp.float32) + _mm('bse,ed->bsd', o, wo)).astype(jnp.bfloat16)
    x2 = _rms(a, ln_ffn)
    hs = (jax.nn.silu(_mm('bsd,df->bsf', x2, ws1)) * _mm('bsd,df->bsf', x2, ws3)).astype(jnp.bfloat16)
    return a, _mm('bsf,fd->bsd', hs, ws2)


def _gate(u, wr, gi):
    lg = _mm('td,de->te', u, wr)
    hit = gi[..., None] == jnp.arange(wr.shape[1], dtype=gi.dtype)
    return jax.nn.softmax(jnp.sum(jnp.where(hit, lg[:, None, :], 0.0), axis=-1), axis=-1)


def _parts(c):
    hi = c.astype(jnp.bfloat16)
    r = c - hi.astype(jnp.float32)
    mid = r.astype(jnp.bfloat16)
    lo = (r - mid.astype(jnp.float32)).astype(jnp.bfloat16)
    return hi, mid, lo


def _place(n):
    side = math.isqrt(n // CORES)
    me = lax.axis_index('ep')
    return side, me, (me // CORES) % side, me // (CORES * side), me % CORES


def _order(k, side):
    i, b = k % side, k // side
    return side - 1 - (i + b + 1) % side, side - 1 - i


def _k1(n, cap, slots, ug, qr, ue1, ue3, ue2, r_out, w13, w2, u, pm, xs, h, ys, wsem, w2sem, usem, ssem, rsem):
    side, me, x, y, c = _place(n)
    t, d = u.shape[1], u.shape[2]
    f = h.shape[1]
    dh = d // 2
    steps = side * side
    total = steps * 2

    def chip(k):
        dx, dy = _order(k, side)
        return (x + dx) % side, (y + dy) % side

    def u_copy(k):
        cx, cy = chip(k)
        return pltpu.make_async_copy(ug.at[pl.ds((cy * side + cx) * CORES, CORES), pl.ds(0, t)], u, usem)

    u_copy(0).start()
    for el in range(2):
        for j in range(f // 128):
            pltpu.make_async_copy(ue1.at[el, :, pl.ds(128 * j, 128)], w13.at[el, :, pl.ds(256 * j, 128)], wsem.at[el]).start()
            pltpu.make_async_copy(ue3.at[el, :, pl.ds(128 * j, 128)], w13.at[el, :, pl.ds(256 * j + 128, 128)], wsem.at[el]).start()
        pltpu.make_async_copy(ue2.at[el], w2.at[el], w2sem.at[el]).start()

    barrier = pltpu.get_barrier_semaphore()
    peers = 0
    for off in range(side):
        for dc in range(CORES):
            if off or dc:
                cc = (c + dc) % CORES
                pl.semaphore_signal(barrier, inc=1, device_id={'ep': (((y + off) % side) * side + x) * CORES + cc}, device_id_type=MESH)
                peers += 1
                if off:
                    pl.semaphore_signal(barrier, inc=1, device_id={'ep': (y * side + (x + off) % side) * CORES + cc}, device_id_type=MESH)
                    peers += 1
    pl.semaphore_wait(barrier, peers)

    def send(it):
        k, el = it // 2, it % 2
        s = it % slots
        dx, dy = _order(k, side)
        cx, cy = chip(k)
        for cc in range(CORES):
            for half, off, line, mine, dest in (
                (0, dy, cx, y, (cy * side + x) * CORES + cc),
                (1, dx, cy, x, (y * side + cx) * CORES + cc),
            ):
                src = ys.at[s, pl.ds(cc * cap, cap), pl.ds(half * dh, dh)]
                dst = r_out.at[half, line, pl.ds((mine * CORES + c) * (2 * cap) + el * cap, cap)]
                own = (off == 0) & (c == cc)

                @pl.when(own)
                def _():
                    pltpu.make_async_copy(src, dst, ssem.at[s]).start()

                @pl.when(jnp.logical_not(own))
                def _():
                    pltpu.make_async_remote_copy(src, dst, ssem.at[s], rsem, device_id={'ep': dest}, device_id_type=MESH).start()

    def wait_sent(s):
        pltpu.make_async_copy(ys.at[s], ys.at[s], ssem.at[s]).wait()

    @pl.loop(0, steps)
    def _(k):
        cx, cy = chip(k)
        u_copy(k).wait()

        @pl.loop(0, CORES)
        def _(cc):
            q = qr[(cy * side + cx) * CORES + cc]
            slot = lax.broadcasted_iota(jnp.int32, (cap, t), 0).astype(F32)
            for el in range(2):
                pm[pl.ds(el * cap, cap)] = jnp.where(slot == q[el:el + 1], 1.0, 0.0).astype(BF16)
            wide = min(512, d)
            for m in range(d // wide):
                cols = pl.ds(m * wide, wide)
                got = jnp.dot(pm[...], u[cc, :, cols], preferred_element_type=F32).astype(BF16)
                for el in range(2):
                    xs[el, pl.ds(pl.multiple_of(cc * cap, 16), cap), cols] = got[el * cap:(el + 1) * cap]

        @pl.when(k + 1 < steps)
        def _():
            u_copy(k + 1).start()

        @pl.loop(0, 2)
        def _(el):
            it = 2 * k + el
            s = it % slots

            @pl.when(it >= 1)
            def _():
                send(it - 1)

            @pl.when(it >= slots)
            def _():
                wait_sent(s)

            @pl.when(k == 0)
            def _():
                pltpu.make_async_copy(w13.at[el], w13.at[el], wsem.at[el]).wait()
                pltpu.make_async_copy(w2.at[el], w2.at[el], w2sem.at[el]).wait()

            group = 2
            for j in range(0, f // 128, group):
                g = min(group, f // 128 - j)
                a = jnp.dot(xs[el], w13[el, :, pl.ds(256 * j, 256 * g)], preferred_element_type=F32)
                for i in range(g):
                    a1, a3 = a[:, 256 * i:256 * i + 128], a[:, 256 * i + 128:256 * i + 256]
                    h[:, pl.ds(128 * (j + i), 128)] = (jax.nn.silu(a1) * a3).astype(BF16)
            wide = min(512, d)
            for m in range(d // wide):
                cols = pl.ds(m * wide, wide)
                ys[s, :, cols] = jnp.dot(h[...], w2[el, :, cols], preferred_element_type=F32).astype(BF16)

    send(total - 1)
    for s in range(slots):
        wait_sent(s)
    got = r_out.at[:, :, pl.ds(0, (CORES * side - 1) * 2 * cap)]
    pltpu.make_async_copy(got, got, rsem).wait()


def _k2(n, cap, r, pg, z, out, rb, mr, mt, pm, sb, rx2, rxf, zb, ob, lsem, msem, ssem, r2sem, rfsem, zsem, osem):
    side, me, x, y, c = _place(n)
    t = mt.shape[0]
    kk, dh = rb.shape[1], rb.shape[2]
    nm = rx2.shape[2] * 2
    tile = rx2.shape[3]
    keep = sb.shape[0] // nm
    units = 2 * side

    def role(w):
        s = side - 1 - w // 2
        return w % 2, s + (s // 2) * (1 - 2 * (s % 2))

    def at(half, off):
        return ((y + half * off) % side * side + (x + (1 - half) * off) % side) * CORES + c

    def line(w):
        half, off = role(w)
        return half, (x * (1 - half) + y * half + off) % side

    def loads(w):
        half, at_line = line(w)
        b = w % 2
        return (
            pltpu.make_async_copy(r.at[half, at_line], rb.at[b], lsem.at[b]),
            pltpu.make_async_copy(pg.at[half, at_line], mr.at[b], msem.at[b]),
        )

    for cp in loads(0):
        cp.start()

    barrier = pltpu.get_barrier_semaphore()
    for half in range(2):
        for off in (1, side - 1):
            pl.semaphore_signal(barrier, inc=1, device_id={'ep': at(half, off)}, device_id_type=MESH)
    pl.semaphore_wait(barrier, 4)

    def z_copy(half, m):
        return pltpu.make_async_copy(z.at[pl.ds(m * tile, tile), pl.ds(half * dh, dh)], zb, zsem)

    def o_copy(half, m, b):
        return pltpu.make_async_copy(ob.at[b], out.at[pl.ds(m * tile, tile), pl.ds(half * dh, dh)], osem.at[b])

    def send(w, m):
        half, off = role(w)
        b = w % keep
        src = sb.at[b * nm + m]

        def go(dst, sem, step):
            pltpu.make_async_remote_copy(src, dst, ssem.at[b], sem, device_id={'ep': at(half, step)}, device_id_type=MESH).start()

        @pl.when((off == 2) & (m < nm // 2))
        def _():
            go(rx2.at[half, 0, m], r2sem.at[half, 0, m], 1)

        @pl.when((off == 2) & (m >= nm // 2))
        def _():
            go(rx2.at[half, 1, m - nm // 2], r2sem.at[half, 1, m - nm // 2], side - 1)

        @pl.when(off == 1)
        def _():
            go(rxf.at[half, 0, m], rfsem.at[half, 0, m], 1)

        @pl.when(off == side - 1)
        def _():
            go(rxf.at[half, 1, m], rfsem.at[half, 1, m], side - 1)

    def wait_recv(ref, sem):
        pltpu.make_async_copy(ref, ref, sem).wait()

    def wait_sent(b):
        sent = sb.at[pl.ds(b * nm, nm)]
        pltpu.make_async_copy(sent, sent, ssem.at[b]).wait()

    @pl.loop(0, units)
    def _(w):
        half, off = role(w)
        for cp in loads(w):
            cp.wait()

        @pl.when(w + 1 < units)
        def _():
            for cp in loads(w + 1):
                cp.start()

        meta = mr[w % 2]
        mt[...] = jnp.concatenate([meta, jnp.zeros((128 - meta.shape[0], t), F32)], axis=0).T

        @pl.when((w >= keep) & (w < units - 2))
        def _():
            wait_sent(w % keep)

        @pl.loop(0, nm)
        def _(m):
            it = w * nm + m

            @pl.when((it >= 1) & (it <= (units - 2) * nm))
            def _():
                send((it - 1) // nm, (it - 1) % nm)

            @pl.when(off == 0)
            def _():
                z_copy(half, m).start()

            rows = mt[pl.ds(m * tile, tile)]
            step = kk // 6
            for kc in range(0, kk, step):
                at_k = lax.broadcasted_iota(jnp.int32, (tile, step), 1).astype(F32) + float(kc)
                v = jnp.zeros((tile, step), F32)
                for j in range(6):
                    v = jnp.where(at_k == rows[:, j:j + 1], rows[:, 8 + j:9 + j], v)
                for i, part in enumerate(_parts(v)):
                    pm[pl.ds(i * tile, tile), pl.ds(kc, step)] = part

            wide = min(512, dh)
            own = w // (units - 2)
            here = (1 - own) * (w % keep * nm + m) + own * (keep * nm)
            for i in range(dh // wide):
                cols = pl.ds(i * wide, wide)
                o = jnp.dot(pm[...], rb[w % 2, :, cols], preferred_element_type=F32)
                sb[here, :, cols] = o[:tile] + o[tile:2 * tile] + o[2 * tile:]

            @pl.when((off == 1) & (m < nm // 2))
            def _():
                wait_recv(rx2.at[half, 0, m], r2sem.at[half, 0, m])
                sb[here] = sb[here] + rx2[half, 0, m]

            @pl.when((off == side - 1) & (m >= nm // 2))
            def _():
                wait_recv(rx2.at[half, 1, m - nm // 2], r2sem.at[half, 1, m - nm // 2])
                sb[here] = sb[here] + rx2[half, 1, m - nm // 2]

            @pl.when(off == 0)
            def _():
                done = half * nm + m

                @pl.when(done >= 2)
                def _():
                    o_copy((done - 2) // nm, (done - 2) % nm, m % 2).wait()

                wait_recv(rxf.at[half, 0, m], rfsem.at[half, 0, m])
                wait_recv(rxf.at[half, 1, m], rfsem.at[half, 1, m])
                z_copy(half, m).wait()
                total = zb[...] + (sb[here] + rxf[half, 0, m] + rxf[half, 1, m])
                ob[m % 2] = total.astype(BF16)
                o_copy(half, m, m % 2).start()

    for w in range(units - 2 - keep, units - 2):
        wait_sent(w % keep)
    for m in (nm - 2, nm - 1):
        o_copy(1, m, m % 2).wait()


def _experts(ug, qr, ue1, ue3, ue2, n, cap):
    t, d, f = qr.shape[-1], ug.shape[-1], ue1.shape[-1]
    side = math.isqrt(n // CORES)
    slots = 4
    any_ = pl.BlockSpec(memory_space=pl.ANY)
    flops = n * 2 * cap * (2 * t * d + 6 * d * f)
    return pl.pallas_call(
        functools.partial(_k1, n, cap, slots),
        out_shape=jax.ShapeDtypeStruct((2, side, CORES * side * 2 * cap, d // 2), BF16),
        in_specs=[any_, pl.BlockSpec(memory_space=pltpu.VMEM), any_, any_, any_],
        out_specs=any_,
        scratch_shapes=[
            pltpu.VMEM((2, d, 2 * f), BF16),
            pltpu.VMEM((2, f, d), BF16),
            pltpu.VMEM((CORES, t, d), BF16),
            pltpu.VMEM((2 * cap, t), BF16),
            pltpu.VMEM((2, CORES * cap, d), BF16),
            pltpu.VMEM((CORES * cap, f), BF16),
            pltpu.VMEM((slots, CORES * cap, d), BF16),
            pltpu.SemaphoreType.DMA((2,)),
            pltpu.SemaphoreType.DMA((2,)),
            pltpu.SemaphoreType.DMA,
            pltpu.SemaphoreType.DMA((slots,)),
            pltpu.SemaphoreType.DMA,
        ],
        cost_estimate=pl.CostEstimate(flops=flops, bytes_accessed=4 * n * t * d, transcendentals=n * 2 * cap * f),
        compiler_params=pltpu.CompilerParams(collective_id=0, has_side_effects=True, vmem_limit_bytes=67043328),
        name='experts',
    )(ug, qr, ue1, ue3, ue2)


def _combine(r, pg, z, n, cap):
    t, d = z.shape
    dh = d // 2
    side = math.isqrt(n // CORES)
    nm = 4
    tile = t // nm
    kk = r.shape[2]
    keep = 3
    any_ = pl.BlockSpec(memory_space=pl.ANY)
    return pl.pallas_call(
        functools.partial(_k2, n, cap),
        out_shape=jax.ShapeDtypeStruct((t, d), BF16),
        in_specs=[any_, any_, any_],
        out_specs=any_,
        scratch_shapes=[
            pltpu.VMEM((2, kk, dh), BF16),
            pltpu.VMEM((2, pg.shape[2], t), F32),
            pltpu.VMEM((t, 128), F32),
            pltpu.VMEM((3 * tile, kk), BF16),
            pltpu.VMEM((keep * nm + 1, tile, dh), F32),
            pltpu.VMEM((2, 2, nm // 2, tile, dh), F32),
            pltpu.VMEM((2, 2, nm, tile, dh), F32),
            pltpu.VMEM((tile, dh), F32),
            pltpu.VMEM((2, tile, dh), BF16),
            pltpu.SemaphoreType.DMA((2,)),
            pltpu.SemaphoreType.DMA((2,)),
            pltpu.SemaphoreType.DMA((keep,)),
            pltpu.SemaphoreType.DMA((2, 2, nm // 2)),
            pltpu.SemaphoreType.DMA((2, 2, nm)),
            pltpu.SemaphoreType.DMA,
            pltpu.SemaphoreType.DMA((2,)),
        ],
        cost_estimate=pl.CostEstimate(flops=2 * side * 3 * 2 * t * kk * dh, bytes_accessed=2 * r.size, transcendentals=0),
        compiler_params=pltpu.CompilerParams(collective_id=1, has_side_effects=True, vmem_limit_bytes=67043328),
        name='combine',
    )(r, pg, z)


def _encode(gi, sl, gate, t, d):
    rows = [gi.T.astype(BF16), sl.T.astype(BF16)] + [p.T for p in _parts(gate)]
    e = jnp.concatenate(rows, axis=0)
    e = jnp.pad(e, ((0, EXTRA * d // t - e.shape[0]), (0, 0)))
    return e.reshape(EXTRA, d)


def _decode(extra, top, t, n, cap):
    side = math.isqrt(n // CORES)
    me = lax.axis_index('ep')
    x, y = (me // CORES) % side, me // (CORES * side)
    e = extra.reshape(n, -1, t).astype(F32)
    ex, sl = e[:, :top].astype(jnp.int32), e[:, top:2 * top].astype(jnp.int32)
    g = e[:, 2 * top:3 * top] + e[:, 3 * top:4 * top] + e[:, 4 * top:5 * top]
    q = []
    for el in range(2):
        mine = ex == me * 2 + el
        q.append(jnp.sum(jnp.where(mine, sl + 1, 0), axis=1) - 1)
    qr = jnp.stack(q + [q[0]] * 6, axis=1).astype(F32)
    chip_x, chip_y = (ex // (2 * CORES)) % side, ex // (2 * CORES * side)
    low = (ex % (2 * CORES)) * cap + sl
    pa = jnp.where(chip_x == x, chip_y * (2 * CORES * cap) + low, -1)
    pb = jnp.where(chip_y == y, chip_x * (2 * CORES * cap) + low, -1)
    pad = jnp.zeros((n, 8 - top, t), F32)
    out = []
    for p in (pa, pb):
        out.append(jnp.concatenate([p.astype(F32), pad, g, pad], axis=1))
    grid = lambda v: v.reshape(side, side, CORES, 16, t)
    c = me % CORES
    va = lax.dynamic_slice(grid(out[0]), (y, 0, c, 0, 0), (1, side, 1, 16, t)).reshape(side, 16, t)
    vb = lax.dynamic_slice(grid(out[1]), (0, x, c, 0, 0), (side, 1, 1, 16, t)).reshape(side, 16, t)
    return qr, jnp.stack([va, vb])


def solution(mesh):
    n = mesh.shape['ep']
    rows = P(('dp', 'ep'))
    rep = P()

    def local(h0, idx, slot, ln_attn, wq, wk, wv, wo, ln_ffn, ws1, ws3, ws2, ln_moe, wr, ue1, ue3, ue2):
        b, s, d = h0.shape
        top = idx.shape[-1]
        ne = ue1.shape[0] * n
        t = b * s
        cap = CAP_FACTOR * t * top // ne
        u = _rms(h0, ln_moe).reshape(t, d)
        gi, sl = idx.reshape(t, top), slot.reshape(t, top)
        gate = _gate(u, wr, gi)
        ug = lax.all_gather(jnp.concatenate([u, _encode(gi, sl, gate, t, d)], axis=0), 'ep')
        a, fo = _dense(h0, ln_attn, wq, wk, wv, wo, ln_ffn, ws1, ws3, ws2)
        z = (a.astype(F32) + fo).reshape(t, d)
        qr, pg = _decode(ug[:, t:], top, t, n, cap)
        r = _experts(ug, qr, ue1, ue3, ue2, n, cap)
        return _combine(r, pg, z, n, cap).reshape(b, s, d)

    specs = (rows, rows, rows) + (rep,) * 11 + (P('ep'), P('ep'), P('ep'))
    return jax.shard_map(local, mesh=mesh, in_specs=specs, out_specs=rows, check_vma=False)
```

```python
import functools
import math

import jax
import jax.numpy as jnp
from jax import lax
from jax.experimental import pallas as pl
from jax.experimental.pallas import tpu as pltpu
from jax.sharding import PartitionSpec as P

HEAD = 128
EPS = 1e-6
CAP_FACTOR = 2
CORES = 2
EXTRA = 16
F32 = jnp.float32
BF16 = jnp.bfloat16
MESH = pl.DeviceIdType.MESH


def _mm(form, a, b):
    return jnp.einsum(form, a, b, preferred_element_type=jnp.float32)


def _rms(x, w):
    xf = x.astype(jnp.float32)
    r = lax.rsqrt(jnp.mean(xf * xf, axis=-1, keepdims=True) + EPS)
    return (xf * r * w.astype(jnp.float32)).astype(jnp.bfloat16)


def _rope(x):
    s, half = x.shape[1], x.shape[-1] // 2
    freq = 10000.0 ** (-jnp.arange(half, dtype=jnp.float32) / half)
    ang = jnp.arange(s, dtype=jnp.float32)[:, None] * freq[None, :]
    c = jnp.cos(ang)[None, :, None, :]
    sn = jnp.sin(ang)[None, :, None, :]
    x1, x2 = x[..., :half], x[..., half:]
    return jnp.concatenate([x1 * c - x2 * sn, x2 * c + x1 * sn], axis=-1)


def _dense(h0, ln_attn, wq, wk, wv, wo, ln_ffn, ws1, ws3, ws2):
    b, s, _ = h0.shape
    nh = wq.shape[1] // HEAD
    x1 = _rms(h0, ln_attn)
    q = _rope(_mm('bsd,de->bse', x1, wq).reshape(b, s, nh, HEAD)).astype(jnp.bfloat16)
    k = _rope(_mm('bsd,de->bse', x1, wk).reshape(b, s, nh, HEAD)).astype(jnp.bfloat16)
    v = _mm('bsd,de->bse', x1, wv).astype(jnp.bfloat16).reshape(b, s, nh, HEAD)
    sc = _mm('bqhe,bkhe->bhqk', q, k) * HEAD ** -0.5
    causal = jnp.arange(s)[:, None] >= jnp.arange(s)[None, :]
    p = jax.nn.softmax(jnp.where(causal, sc, -1e30), axis=-1).astype(jnp.bfloat16)
    o = _mm('bhqk,bkhe->bqhe', p, v).astype(jnp.bfloat16).reshape(b, s, nh * HEAD)
    a = (h0.astype(jnp.float32) + _mm('bse,ed->bsd', o, wo)).astype(jnp.bfloat16)
    x2 = _rms(a, ln_ffn)
    hs = (jax.nn.silu(_mm('bsd,df->bsf', x2, ws1)) * _mm('bsd,df->bsf', x2, ws3)).astype(jnp.bfloat16)
    return a, _mm('bsf,fd->bsd', hs, ws2)


def _gate(u, wr, gi):
    lg = _mm('td,de->te', u, wr)
    hit = gi[..., None] == jnp.arange(wr.shape[1], dtype=gi.dtype)
    return jax.nn.softmax(jnp.sum(jnp.where(hit, lg[:, None, :], 0.0), axis=-1), axis=-1)


def _parts(c):
    hi = c.astype(jnp.bfloat16)
    r = c - hi.astype(jnp.float32)
    mid = r.astype(jnp.bfloat16)
    lo = (r - mid.astype(jnp.float32)).astype(jnp.bfloat16)
    return hi, mid, lo


def _place(n):
    side = math.isqrt(n // CORES)
    me = lax.axis_index('ep')
    return side, me, (me // CORES) % side, me // (CORES * side), me % CORES


def _turn(i, side):
    s = side - 1 - i
    return s + (s // 2) * (1 - 2 * (s % 2))


def _order(k, side):
    i, b = k % side, k // side
    return _turn((i + b + 1) % side, side), _turn(i, side)


def _routing(rows, t):
    e = rows.astype(F32)
    left, right = e[:, :t], e[:, t:]
    lo = jnp.concatenate([left[12:16], right[12:14]], axis=0)
    return left[0:6], left[6:12], right[0:6] + right[6:12] + lo


def _k1(n, cap, slots, ug, ue1, ue3, ue2, r_out, rl, w13, w2, u, pm, xs, h, ys, wsem, w2sem, usem, ssem, rsem, relsem, fsem):
    side, me, x, y, c = _place(n)
    t, d = pm.shape[1], u.shape[2]
    f = h.shape[1]
    dh = d // 2
    steps = side * side
    total = steps * 2
    far = side // 2
    lag = 4

    def chip(k):
        dx, dy = _order(k, side)
        return (x + dx) % side, (y + dy) % side

    def u_copy(k):
        cx, cy = chip(k)
        return pltpu.make_async_copy(ug.at[pl.ds((cy * side + cx) * CORES, CORES)], u, usem)

    u_copy(0).start()
    for el in range(2):
        for j in range(f // 128):
            pltpu.make_async_copy(ue1.at[el, :, pl.ds(128 * j, 128)], w13.at[el, :, pl.ds(256 * j, 128)], wsem.at[el]).start()
            pltpu.make_async_copy(ue3.at[el, :, pl.ds(128 * j, 128)], w13.at[el, :, pl.ds(256 * j + 128, 128)], wsem.at[el]).start()
        pltpu.make_async_copy(ue2.at[el], w2.at[el], w2sem.at[el]).start()

    def device(half, off, cc):
        return ((y + (1 - half) * off) % side * side + (x + half * off) % side) * CORES + cc

    barrier = pltpu.get_barrier_semaphore()
    peers = 0
    for off in range(side):
        for dc in range(CORES):
            for half in range(2):
                if off or (dc and not half):
                    pl.semaphore_signal(barrier, inc=1, device_id={'ep': device(half, off, (c + dc) % CORES)}, device_id_type=MESH)
                    peers += 1
    pl.semaphore_wait(barrier, peers)

    def remote(src, dst, send_sem, recv_sem, dest):
        return pltpu.make_async_remote_copy(src, dst, send_sem, recv_sem, device_id={'ep': dest}, device_id_type=MESH)

    def send(it):
        k, el = it // 2, it % 2
        s = it % slots
        dx, dy = _order(k, side)
        cx, cy = chip(k)
        for cc in range(CORES):
            for half, off, line, mine in ((0, dy, cx, y), (1, dx, cy, x)):
                src = ys.at[s, pl.ds(cc * cap, cap), pl.ds(half * dh, dh)]
                dst = r_out.at[half, line, pl.ds((mine * CORES + c) * (2 * cap) + el * cap, cap)]
                own = (off == 0) & (c == cc)

                @pl.when(own)
                def _():
                    pltpu.make_async_copy(src, dst, ssem.at[s]).start()

                @pl.when(jnp.logical_not(own) & (off != far))
                def _():
                    remote(src, dst, ssem.at[s], rsem, device(half, off, cc)).start()

                @pl.when(off == far)
                def _():
                    at = (half, cc, k // side, el)
                    remote(src, rl.at[at], ssem.at[s], relsem.at[at], device(half, 1 - 2 * cc, c)).start()

    def forward(it):
        k, el = it // 2, it % 2
        dx, dy = _order(k, side)
        cx, cy = chip(k)
        for half, off, line, mine in ((0, dy, cx, y), (1, dx, cy, x)):
            @pl.when(off == far)
            def _():
                for cc in range(CORES):
                    at = (half, cc, k // side, el)
                    step = 1 - 2 * cc
                    pltpu.make_async_copy(rl.at[at], rl.at[at], relsem.at[at]).wait()
                    origin = (mine - step + side) % side
                    dst = r_out.at[half, line, pl.ds((origin * CORES + c) * (2 * cap) + el * cap, cap)]
                    remote(rl.at[at], dst, fsem, rsem, device(half, step, cc)).start()

    def wait_sent(s):
        pltpu.make_async_copy(ys.at[s], ys.at[s], ssem.at[s]).wait()

    @pl.loop(0, steps)
    def _(k):
        u_copy(k).wait()

        @pl.loop(0, CORES)
        def _(cc):
            ex, sl, _ = _routing(u[cc, t:], t)
            slot = lax.broadcasted_iota(jnp.int32, (cap, t), 0).astype(F32)
            for el in range(2):
                mine = (me * 2 + el).astype(F32)
                q = jnp.sum(jnp.where(ex == mine, sl + 1.0, 0.0), axis=0, keepdims=True) - 1.0
                pm[pl.ds(el * cap, cap)] = jnp.where(slot == q, 1.0, 0.0).astype(BF16)
            wide = min(512, d)
            for m in range(d // wide):
                cols = pl.ds(m * wide, wide)
                got = jnp.dot(pm[...], u[cc, :t, cols], preferred_element_type=F32).astype(BF16)
                for el in range(2):
                    xs[el, pl.ds(pl.multiple_of(cc * cap, 16), cap), cols] = got[el * cap:(el + 1) * cap]

        @pl.when(k + 1 < steps)
        def _():
            u_copy(k + 1).start()

        @pl.loop(0, 2)
        def _(el):
            it = 2 * k + el
            s = it % slots

            @pl.when(it >= 1)
            def _():
                send(it - 1)

            @pl.when(it >= 1 + lag)
            def _():
                forward(it - 1 - lag)

            @pl.when(it >= slots)
            def _():
                wait_sent(s)

            @pl.when(k == 0)
            def _():
                pltpu.make_async_copy(w13.at[el], w13.at[el], wsem.at[el]).wait()
                pltpu.make_async_copy(w2.at[el], w2.at[el], w2sem.at[el]).wait()

            group = 2
            for j in range(0, f // 128, group):
                g = min(group, f // 128 - j)
                a = jnp.dot(xs[el], w13[el, :, pl.ds(256 * j, 256 * g)], preferred_element_type=F32)
                for i in range(g):
                    a1, a3 = a[:, 256 * i:256 * i + 128], a[:, 256 * i + 128:256 * i + 256]
                    h[:, pl.ds(128 * (j + i), 128)] = (jax.nn.silu(a1) * a3).astype(BF16)
            wide = min(512, d)
            for m in range(d // wide):
                cols = pl.ds(m * wide, wide)
                ys[s, :, cols] = jnp.dot(h[...], w2[el, :, cols], preferred_element_type=F32).astype(BF16)

    send(total - 1)
    for s in range(slots):
        wait_sent(s)
    pltpu.make_async_copy(rl, rl, fsem).wait()
    got = r_out.at[:, :, pl.ds(0, (CORES * side - 1) * 2 * cap)]
    pltpu.make_async_copy(got, got, rsem).wait()


def _k2(n, cap, keep, ug, r, z, out, rb, mr, mt, pma, pmb, sb, rx2, rxf, zb, ob, lsem, msem, ssem, r2sem, rfsem, zsem, osem):
    side, me, x, y, c = _place(n)
    kk, dh = rb.shape[1], rb.shape[2]
    tile = zb.shape[1]
    t = 4 * tile
    experts = kk // cap
    units = 16
    sending = 12
    far = side // 2

    def role(w):
        q, half, b = w // 4, w % 4 // 2, w % 2
        first = 1 - (q + 3) // 4
        middle = (q + 1) // 2 % 2
        off = first * far + middle * (1 + (side - 2) * b)
        return half, off, b + middle * (q % 2) * (1 - 2 * b)

    def at(half, off):
        return ((y + half * off) % side * side + (x + (1 - half) * off) % side) * CORES + c

    def line(half, off):
        return (x * (1 - half) + y * half + off) % side

    def load(w):
        half, off, _ = role(w)
        return pltpu.make_async_copy(r.at[half, line(half, off)], rb.at[w % 2], lsem.at[w % 2])

    load(0).start()
    for half in range(2):
        for off in range(side):
            pltpu.make_async_copy(ug.at[at(half, off), pl.ds(t, mr.shape[2])], mr.at[half, off], msem).start()

    barrier = pltpu.get_barrier_semaphore()
    for half in range(2):
        for off in (1, side - 1):
            pl.semaphore_signal(barrier, inc=1, device_id={'ep': at(half, off)}, device_id_type=MESH)
    pl.semaphore_wait(barrier, 4)
    pltpu.make_async_copy(mr, mr, msem).wait()

    def prepare(w):
        half, off, mh = role(w)
        hf = half.astype(F32) if hasattr(half, 'astype') else float(half)
        ex, sl, g = _routing(mr[half, off], t)
        cy = jnp.floor(ex * (1.0 / (2 * CORES * side)))
        cx = jnp.floor((ex - cy * (2 * CORES * side)) * (1.0 / (2 * CORES)))
        low = ex - cy * (2 * CORES * side) - cx * (2 * CORES)
        mine = x.astype(F32) * (1.0 - hf) + y.astype(F32) * hf
        across = cx * (1.0 - hf) + cy * hf
        along = cy * (1.0 - hf) + cx * hf
        e = jnp.where(across == mine, along * (2 * CORES) + low, -1.0)
        gap = jnp.zeros((2, t), F32)
        m = jnp.concatenate([e, gap, sl, gap, g, jnp.zeros((106, t), F32)], axis=0)
        for i in range(2):
            @pl.when(mh == i)
            def _():
                mt[w % 2] = m[:, i * 2 * tile:(i + 1) * 2 * tile].T

    def build(pm, w, i):
        rows = mt[w % 2, pl.ds(i * tile, tile)]
        lane = lax.broadcasted_iota(jnp.int32, (tile, 128), 1).astype(F32)
        slot = jnp.zeros((tile, 128), F32)
        gate = jnp.zeros((tile, 128), F32)
        for j in range(6):
            hit = lane == rows[:, j:j + 1]
            slot = slot + jnp.where(hit, rows[:, 8 + j:9 + j] + 4096.0, 0.0)
            gate = gate + jnp.where(hit, rows[:, 16 + j:17 + j], 0.0)
        slot = slot - 4096.0
        for k0 in range(0, kk, 128):
            v = jnp.zeros((tile, 128), F32)
            for e in range(k0 // cap, min(experts - 1, (k0 + 127) // cap) + 1):
                s_e = slot[:, e:e + 1]
                v = jnp.where(lane + float(k0 - e * cap) == s_e, gate[:, e:e + 1], v)
            for p, part in enumerate(_parts(v)):
                pm[pl.ds(p * tile, tile), pl.ds(k0, 128)] = part

    def z_copy(half, m, i):
        return pltpu.make_async_copy(z.at[pl.ds(m * tile, tile), pl.ds(half * dh, dh)], zb.at[i], zsem.at[i])

    def o_copy(half, m, i):
        return pltpu.make_async_copy(ob.at[i], out.at[pl.ds(m * tile, tile), pl.ds(half * dh, dh)], osem.at[i])

    def send(w, i):
        half, off, mh = role(w)
        b = w % keep
        src = sb.at[b * 2 + i]

        def go(dst, sem, step):
            pltpu.make_async_remote_copy(src, dst, ssem.at[b], sem, device_id={'ep': at(half, step)}, device_id_type=MESH).start()

        @pl.when((off == far) & (mh == 0))
        def _():
            go(rx2.at[half, 0, i], r2sem.at[half, 0, i], 1)

        @pl.when((off == far) & (mh == 1))
        def _():
            go(rx2.at[half, 1, i], r2sem.at[half, 1, i], side - 1)

        @pl.when(off == 1)
        def _():
            go(rxf.at[half, 0, mh * 2 + i], rfsem.at[half, 0, mh * 2 + i], 1)

        @pl.when(off == side - 1)
        def _():
            go(rxf.at[half, 1, mh * 2 + i], rfsem.at[half, 1, mh * 2 + i], side - 1)

    def wait_recv(ref, sem):
        pltpu.make_async_copy(ref, ref, sem).wait()

    def wait_sent(b):
        sent = sb.at[pl.ds(b * 2, 2)]
        pltpu.make_async_copy(sent, sent, ssem.at[b]).wait()

    prepare(0)
    build(pma, 0, 0)

    @pl.loop(0, units)
    def _(w):
        half, off, mh = role(w)
        after = w + 1 - (w + 1) // units
        load(w).wait()

        @pl.when(w + 1 < units)
        def _():
            load(w + 1).start()

        @pl.when(w + 1 < units)
        def _():
            prepare(w + 1)

        @pl.when((w >= keep) & (w < sending))
        def _():
            wait_sent(w % keep)

        @pl.when(off == 0)
        def _():
            for i in range(2):
                z_copy(half, mh * 2 + i, i).start()

        own = w // sending
        for i, pm in ((0, pma), (1, pmb)):
            here = (1 - own) * (w % keep * 2 + i) + own * (keep * 2)
            m = mh * 2 + i
            wide = min(512, dh)
            for j in range(dh // wide):
                cols = pl.ds(j * wide, wide)
                o = jnp.dot(pm[...], rb[w % 2, :, cols], preferred_element_type=F32)
                sb[here, :, cols] = o[:tile] + o[tile:2 * tile] + o[2 * tile:]
            if i == 0:
                build(pmb, w, 1)
            else:
                build(pma, after, 0)

            @pl.when((off == 1) & (mh == 0))
            def _():
                wait_recv(rx2.at[half, 0, i], r2sem.at[half, 0, i])
                sb[here] = sb[here] + rx2[half, 0, i]

            @pl.when((off == side - 1) & (mh == 1))
            def _():
                wait_recv(rx2.at[half, 1, i], r2sem.at[half, 1, i])
                sb[here] = sb[here] + rx2[half, 1, i]

            @pl.when(off == 0)
            def _():
                @pl.when(w > sending)
                def _():
                    o_copy(0, 0, i).wait()

                for way in range(2):
                    wait_recv(rxf.at[half, way, m], rfsem.at[half, way, m])
                z_copy(half, m, i).wait()
                total = zb[i] + (sb[here] + rxf[half, 0, m] + rxf[half, 1, m])
                ob[i] = total.astype(BF16)
                o_copy(half, m, i).start()

            @pl.when(w < sending)
            def _():
                send(w, i)

    for w in range(sending - keep, sending):
        wait_sent(w % keep)
    for i in range(2):
        o_copy(0, 0, i).wait()


def _experts(ug, ue1, ue3, ue2, n, cap, t):
    d, f = ug.shape[-1], ue1.shape[-1]
    side = math.isqrt(n // CORES)
    slots = 6
    any_ = pl.BlockSpec(memory_space=pl.ANY)
    flops = n * 2 * cap * (2 * t * d + 6 * d * f)
    return pl.pallas_call(
        functools.partial(_k1, n, cap, slots),
        out_shape=(
            jax.ShapeDtypeStruct((2, side, CORES * side * 2 * cap, d // 2), BF16),
            jax.ShapeDtypeStruct((2, CORES, side, 2, cap, d // 2), BF16),
        ),
        in_specs=[any_] * 4,
        out_specs=(any_, any_),
        scratch_shapes=[
            pltpu.VMEM((2, d, 2 * f), BF16),
            pltpu.VMEM((2, f, d), BF16),
            pltpu.VMEM((CORES, ug.shape[1], d), BF16),
            pltpu.VMEM((2 * cap, t), BF16),
            pltpu.VMEM((2, CORES * cap, d), BF16),
            pltpu.VMEM((CORES * cap, f), BF16),
            pltpu.VMEM((slots, CORES * cap, d), BF16),
            pltpu.SemaphoreType.DMA((2,)),
            pltpu.SemaphoreType.DMA((2,)),
            pltpu.SemaphoreType.DMA,
            pltpu.SemaphoreType.DMA((slots,)),
            pltpu.SemaphoreType.DMA,
            pltpu.SemaphoreType.DMA((2, CORES, side, 2)),
            pltpu.SemaphoreType.DMA,
        ],
        cost_estimate=pl.CostEstimate(flops=flops, bytes_accessed=4 * n * t * d, transcendentals=n * 2 * cap * f),
        compiler_params=pltpu.CompilerParams(collective_id=0, has_side_effects=True, vmem_limit_bytes=67043328),
        name='experts',
    )(ug, ue1, ue3, ue2)[0]


def _combine(ug, r, z, n, cap):
    t, d = z.shape
    dh = d // 2
    side = math.isqrt(n // CORES)
    tile = t // 4
    kk = r.shape[2]
    keep = 4
    any_ = pl.BlockSpec(memory_space=pl.ANY)
    return pl.pallas_call(
        functools.partial(_k2, n, cap, keep),
        out_shape=jax.ShapeDtypeStruct((t, d), BF16),
        in_specs=[any_, any_, any_],
        out_specs=any_,
        scratch_shapes=[
            pltpu.VMEM((2, kk, dh), BF16),
            pltpu.VMEM((2, side, EXTRA, d), BF16),
            pltpu.VMEM((2, 2 * tile, 128), F32),
            pltpu.VMEM((3 * tile, kk), BF16),
            pltpu.VMEM((3 * tile, kk), BF16),
            pltpu.VMEM((keep * 2 + 1, tile, dh), F32),
            pltpu.VMEM((2, 2, 2, tile, dh), F32),
            pltpu.VMEM((2, 2, 4, tile, dh), F32),
            pltpu.VMEM((2, tile, dh), F32),
            pltpu.VMEM((2, tile, dh), BF16),
            pltpu.SemaphoreType.DMA((2,)),
            pltpu.SemaphoreType.DMA,
            pltpu.SemaphoreType.DMA((keep,)),
            pltpu.SemaphoreType.DMA((2, 2, 2)),
            pltpu.SemaphoreType.DMA((2, 2, 4)),
            pltpu.SemaphoreType.DMA((2,)),
            pltpu.SemaphoreType.DMA((2,)),
        ],
        cost_estimate=pl.CostEstimate(flops=2 * side * 3 * 2 * t * kk * dh, bytes_accessed=2 * r.size, transcendentals=0),
        compiler_params=pltpu.CompilerParams(collective_id=1, has_side_effects=True, vmem_limit_bytes=67043328),
        name='combine',
    )(ug, r, z)


def _encode(gi, sl, gate):
    hi, mid, lo = (p.T for p in _parts(gate))
    left = jnp.concatenate([gi.T.astype(BF16), sl.T.astype(BF16), lo[:4]], axis=0)
    right = jnp.concatenate([hi, mid, lo[4:], jnp.zeros((2, gi.shape[0]), BF16)], axis=0)
    return jnp.concatenate([left, right], axis=1)


def solution(mesh):
    n = mesh.shape['ep']
    rows = P(('dp', 'ep'))
    rep = P()

    def local(h0, idx, slot, ln_attn, wq, wk, wv, wo, ln_ffn, ws1, ws3, ws2, ln_moe, wr, ue1, ue3, ue2):
        b, s, d = h0.shape
        top = idx.shape[-1]
        ne = ue1.shape[0] * n
        t = b * s
        cap = CAP_FACTOR * t * top // ne
        u = _rms(h0, ln_moe).reshape(t, d)
        gi, sl = idx.reshape(t, top), slot.reshape(t, top)
        gate = _gate(u, wr, gi)
        ug = lax.all_gather(jnp.concatenate([u, _encode(gi, sl, gate)], axis=0), 'ep')
        a, fo = _dense(h0, ln_attn, wq, wk, wv, wo, ln_ffn, ws1, ws3, ws2)
        z = (a.astype(F32) + fo).reshape(t, d)
        r = _experts(ug, ue1, ue3, ue2, n, cap, t)
        return _combine(ug, r, z, n, cap).reshape(b, s, d)

    specs = (rows, rows, rows) + (rep,) * 11 + (P('ep'), P('ep'), P('ep'))
    return jax.shard_map(local, mesh=mesh, in_specs=specs, out_specs=rows, check_vma=False)
```

```python
import functools
import math

import jax
import jax.numpy as jnp
from jax import lax
from jax.experimental import pallas as pl
from jax.experimental.pallas import tpu as pltpu
from jax.sharding import PartitionSpec as P

HEAD = 128
EPS = 1e-6
CAP_FACTOR = 2
CORES = 2
EXTRA = 16
F32 = jnp.float32
BF16 = jnp.bfloat16
MESH = pl.DeviceIdType.MESH


def _mm(form, a, b):
    return jnp.einsum(form, a, b, preferred_element_type=jnp.float32)


def _rms(x, w):
    xf = x.astype(jnp.float32)
    r = lax.rsqrt(jnp.mean(xf * xf, axis=-1, keepdims=True) + EPS)
    return (xf * r * w.astype(jnp.float32)).astype(jnp.bfloat16)


def _rope(x):
    s, half = x.shape[1], x.shape[-1] // 2
    freq = 10000.0 ** (-jnp.arange(half, dtype=jnp.float32) / half)
    ang = jnp.arange(s, dtype=jnp.float32)[:, None] * freq[None, :]
    c = jnp.cos(ang)[None, :, None, :]
    sn = jnp.sin(ang)[None, :, None, :]
    x1, x2 = x[..., :half], x[..., half:]
    return jnp.concatenate([x1 * c - x2 * sn, x2 * c + x1 * sn], axis=-1)


def _dense(h0, ln_attn, wq, wk, wv, wo, ln_ffn, ws1, ws3, ws2):
    b, s, _ = h0.shape
    nh = wq.shape[1] // HEAD
    x1 = _rms(h0, ln_attn)
    q = _rope(_mm('bsd,de->bse', x1, wq).reshape(b, s, nh, HEAD)).astype(jnp.bfloat16)
    k = _rope(_mm('bsd,de->bse', x1, wk).reshape(b, s, nh, HEAD)).astype(jnp.bfloat16)
    v = _mm('bsd,de->bse', x1, wv).astype(jnp.bfloat16).reshape(b, s, nh, HEAD)
    sc = _mm('bqhe,bkhe->bhqk', q, k) * HEAD ** -0.5
    causal = jnp.arange(s)[:, None] >= jnp.arange(s)[None, :]
    p = jax.nn.softmax(jnp.where(causal, sc, -1e30), axis=-1).astype(jnp.bfloat16)
    o = _mm('bhqk,bkhe->bqhe', p, v).astype(jnp.bfloat16).reshape(b, s, nh * HEAD)
    a = (h0.astype(jnp.float32) + _mm('bse,ed->bsd', o, wo)).astype(jnp.bfloat16)
    x2 = _rms(a, ln_ffn)
    hs = (jax.nn.silu(_mm('bsd,df->bsf', x2, ws1)) * _mm('bsd,df->bsf', x2, ws3)).astype(jnp.bfloat16)
    return a, _mm('bsf,fd->bsd', hs, ws2)


def _gate(u, wr, gi):
    lg = _mm('td,de->te', u, wr)
    hit = gi[..., None] == jnp.arange(wr.shape[1], dtype=gi.dtype)
    return jax.nn.softmax(jnp.sum(jnp.where(hit, lg[:, None, :], 0.0), axis=-1), axis=-1)


def _parts(c):
    hi = c.astype(jnp.bfloat16)
    r = c - hi.astype(jnp.float32)
    mid = r.astype(jnp.bfloat16)
    lo = (r - mid.astype(jnp.float32)).astype(jnp.bfloat16)
    return hi, mid, lo


def _place(n):
    side = math.isqrt(n // CORES)
    me = lax.axis_index('ep')
    return side, me, (me // CORES) % side, me // (CORES * side), me % CORES


def _pick(table, k):
    power = (1 + 3 * (k % 2)) * (1 + 15 * (k // 2 % 2)) * (1 + 255 * (k // 4))
    return table // power % 4


def _pack(values):
    return sum(v * 4 ** i for i, v in enumerate(values))


STEP_X = (_pack((2, 2, 1, 0, 1, 1, 1, 0)), _pack((2, 2, 3, 0, 3, 3, 3, 0)))
STEP_Y = (_pack((2, 1, 2, 2, 1, 3, 0, 1)), _pack((0, 3, 2, 0, 3, 1, 0, 3)))
STEPS = 8


def _order(k, i):
    return _pick(STEP_X[i], k), _pick(STEP_Y[i], k)


def _routing(rows, t):
    e = rows.astype(F32)
    left, right = e[:, :t], e[:, t:]
    lo = jnp.concatenate([left[12:16], right[12:14]], axis=0)
    return left[0:6], left[6:12], right[0:6] + right[6:12] + lo


def _ffn(n, cap, ug, ue1, ue3, ue2, y_out, w13, w2, u, pm, xs, h, ys, wsem, w2sem, usem, ysem, before):
    side, me, x, y, c = _place(n)
    t, d = pm.shape[1], u.shape[2]
    f = h.shape[1]
    dh = d // 2

    def u_copy(k, i):
        dx, dy = _order(k, i)
        return pltpu.make_async_copy(ug.at[(y + dy) % side * side + (x + dx) % side], u.at[i], usem.at[i])

    def weights(el):
        for j in range(f // 128):
            pltpu.make_async_copy(ue1.at[el, :, pl.ds(128 * j, 128)], w13.at[el, :, pl.ds(256 * j, 128)], wsem.at[el]).start()
            pltpu.make_async_copy(ue3.at[el, :, pl.ds(128 * j, 128)], w13.at[el, :, pl.ds(256 * j + 128, 128)], wsem.at[el]).start()
        pltpu.make_async_copy(ue2.at[el], w2.at[el], w2sem.at[el]).start()

    def y_copies(k, el):
        return [
            pltpu.make_async_copy(
                ys.at[el, pl.ds(i * cap, cap), pl.ds(half * dh, dh)], y_out.at[2 * k + i, half, pl.ds(el * cap, cap)], ysem.at[el])
            for i in range(2) for half in range(2)
        ]

    def wait_kept(el):
        pltpu.make_async_copy(ys.at[el], ys.at[el], ysem.at[el]).wait()

    for i in range(2):
        u_copy(0, i).start()
    for el in range(2):
        weights(el)

    @pl.loop(0, STEPS)
    def _(k):
        before(k)

        @pl.loop(0, 2)
        def _(i):
            pltpu.make_async_copy(u.at[i], u.at[i], usem.at[i]).wait()
            ex, sl, _ = _routing(u[i, t:], t)
            slot = lax.broadcasted_iota(jnp.int32, (cap, t), 0).astype(F32)
            for el in range(2):
                mine = (me * 2 + el).astype(F32)
                q = jnp.sum(jnp.where(ex == mine, sl + 1.0, 0.0), axis=0, keepdims=True) - 1.0
                pm[pl.ds(el * cap, cap)] = jnp.where(slot == q, 1.0, 0.0).astype(BF16)
            wide = min(512, d)
            for m in range(d // wide):
                cols = pl.ds(m * wide, wide)
                got = jnp.dot(pm[...], u[i, :t, cols], preferred_element_type=F32).astype(BF16)
                for el in range(2):
                    xs[el, pl.ds(pl.multiple_of(i * cap, 16), cap), cols] = got[el * cap:(el + 1) * cap]

        @pl.when(k + 1 < STEPS)
        def _():
            for i in range(2):
                u_copy(k + 1, i).start()

        @pl.loop(0, 2)
        def _(el):
            @pl.when(k == 0)
            def _():
                pltpu.make_async_copy(w13.at[el], w13.at[el], wsem.at[el]).wait()
                pltpu.make_async_copy(w2.at[el], w2.at[el], w2sem.at[el]).wait()

            group = 2
            for j in range(0, f // 128, group):
                g = min(group, f // 128 - j)
                a = jnp.dot(xs[el], w13[el, :, pl.ds(256 * j, 256 * g)], preferred_element_type=F32)
                for i in range(g):
                    a1, a3 = a[:, 256 * i:256 * i + 128], a[:, 256 * i + 128:256 * i + 256]
                    h[:, pl.ds(128 * (j + i), 128)] = (jax.nn.silu(a1) * a3).astype(BF16)

            @pl.when(k >= 1)
            def _():
                wait_kept(el)

            wide = min(512, d)
            for m in range(d // wide):
                cols = pl.ds(m * wide, wide)
                ys[el, :, cols] = jnp.dot(h[...], w2[el, :, cols], preferred_element_type=F32).astype(BF16)
            for cp in y_copies(k, el):
                cp.start()

    for el in range(2):
        wait_kept(el)


def _ffn_scratch(t, d, f, cap):
    return [
        pltpu.VMEM((2, d, 2 * f), BF16),
        pltpu.VMEM((2, f, d), BF16),
        pltpu.VMEM((2, t + EXTRA, d), BF16),
        pltpu.VMEM((2 * cap, t), BF16),
        pltpu.VMEM((2, 2 * cap, d), BF16),
        pltpu.VMEM((2 * cap, f), BF16),
        pltpu.VMEM((2, 2 * cap, d), BF16),
    ]


FFN_SEMS = [pltpu.SemaphoreType.DMA((2,))] * 4


def _k1(n, cap, ug, ue1, ue3, ue2, y_out, *refs):
    _ffn(n, cap, ug, ue1, ue3, ue2, y_out, *refs, before=lambda k: None)


def _k2(n, cap, keep, ug0, ug1, y0, ue1, ue3, ue2, rxf, y1, r, rl, rx2, mr, wsem, w2sem, usem, ysem,
        ssem, rsem, relsem, fsem, lsem, msem, bsem, r2sem, rfsem):
    side, me, x, y, c = _place(n)
    t, d = rxf.shape[1], rxf.shape[2]
    f = ue1.shape[2]
    kk, dh = r.shape[2], r.shape[3]
    tile = rx2.shape[3]
    experts = kk // cap
    far = side // 2
    units = 16
    ys = (y0, y1)

    def device(axis, off, cc):
        return ((y + axis * off) % side * side + (x + (1 - axis) * off) % side) * CORES + cc

    def remote(src, dst, send_sem, recv_sem, dest):
        return pltpu.make_async_remote_copy(src, dst, send_sem, recv_sem, device_id={'ep': dest}, device_id_type=MESH)

    for p, ug in ((0, ug0), (1, ug1)):
        axis = (c + p) % 2
        for off in range(side):
            pltpu.make_async_copy(ug.at[device(axis, off, 0) // CORES, pl.ds(t, EXTRA)], mr.at[p, off], msem).start()

    barrier = pltpu.get_barrier_semaphore()
    peers = 0
    for off in range(side):
        for dc in range(CORES):
            for axis in range(2):
                if off or (dc and not axis):
                    pl.semaphore_signal(barrier, inc=1, device_id={'ep': device(axis, off, (c + dc) % CORES)}, device_id_type=MESH)
                    peers += 1
    pl.semaphore_wait(barrier, peers)

    def send(p, k, want_far):
        for i in range(2):
            dx, dy = _order(k, i)
            for half, off, other, mine, line in ((0, dy, dx, y, (x + dx) % side), (1, dx, dy, x, (y + dy) % side)):
                cc = (p + half) % 2
                src = ys[p].at[2 * k + i, half]

                def near():
                    own = (off == 0) & (c == cc)
                    dst = r.at[p, line, pl.ds((mine * CORES + c) * (2 * cap), 2 * cap)]

                    @pl.when(own)
                    def _():
                        pltpu.make_async_copy(src, dst, rsem.at[p, line]).start()

                    @pl.when(jnp.logical_not(own) & (off != far))
                    def _():
                        remote(src, dst, ssem.at[p], rsem.at[p, line], device(1 - half, off, cc)).start()

                def relayed():
                    @pl.when(off == far)
                    def _():
                        for el in range(2):
                            at = (p, half, el, other)
                            remote(src.at[pl.ds(el * cap, cap)], rl.at[at], ssem.at[p], relsem.at[at], device(1 - half, 1 - 2 * el, c)).start()

                if want_far != 0:
                    relayed()
                if want_far != 1:
                    near()

    def forward(p, other):
        for half, mine, line in ((0, y, (x + other) % side), (1, x, (y + other) % side)):
            for el in range(2):
                at = (p, half, el, other)
                step = 1 - 2 * el
                pltpu.make_async_copy(rl.at[at], rl.at[at], relsem.at[at]).wait()
                origin = (mine - step + side) % side
                dst = r.at[p, line, pl.ds((origin * CORES + c) * (2 * cap) + el * cap, cap)]
                remote(rl.at[at], dst, fsem.at[p], rsem.at[p, line], device(1 - half, step, (p + half) % 2)).start()

    for want in (1, 0):
        @pl.loop(0, STEPS)
        def _(k):
            send(0, k, want)

    def before(k):
        @pl.when(k == 2)
        def _():
            @pl.loop(0, side)
            def _(other):
                forward(0, other)

        @pl.when((k >= 2) & (k < 6))
        def _():
            send(1, k - 2, 2)

    def experts_phase(*refs):
        _ffn(n, cap, ug1, ue1, ue3, ue2, y1, *refs, wsem, w2sem, usem, ysem, before=before)

    pl.run_scoped(experts_phase, *_ffn_scratch(t, d, f, cap))

    def role(w):
        p, q, b = w // 8, w % 8 // 2, w % 2
        first = 1 - (q + 3) // 4
        middle = (q + 1) // 2 % 2
        off = first * far + middle * (1 + (side - 2) * b)
        return p, (c + p) % 2, off, b + middle * (q % 2) * (1 - 2 * b)

    def combine_phase(rb, mt, pma, pmb, sb):
        def load(w):
            p, axis, off, _ = role(w)
            line = (x * (1 - axis) + y * axis + off) % side
            return r.at[p, line], rsem.at[p, line], pltpu.make_async_copy(r.at[p, line], rb.at[w % 2], lsem.at[w % 2])

        def start_load(w):
            rows, sem, copy = load(w)
            q, b = w % 8 // 2, w % 2

            @pl.when((q == 1) | ((b == 0) & (q != 2)))
            def _():
                pltpu.make_async_copy(rows, rows, sem).wait()

            copy.start()

        def prepare(w):
            p, axis, off, mh = role(w)
            af = axis.astype(F32)
            ex, sl, g = _routing(mr[p, off], t)
            cy = jnp.floor(ex * (1.0 / (2 * CORES * side)))
            cx = jnp.floor((ex - cy * (2 * CORES * side)) * (1.0 / (2 * CORES)))
            low = ex - cy * (2 * CORES * side) - cx * (2 * CORES)
            mine = x.astype(F32) * (1.0 - af) + y.astype(F32) * af
            across = cx * (1.0 - af) + cy * af
            along = cy * (1.0 - af) + cx * af
            e = jnp.where(across == mine, along * (2 * CORES) + low, -1.0)
            gap = jnp.zeros((2, t), F32)
            m = jnp.concatenate([e, gap, sl, gap, g, jnp.zeros((106, t), F32)], axis=0)
            for i in range(2):
                @pl.when(mh == i)
                def _():
                    mt[w % 2] = m[:, i * 2 * tile:(i + 1) * 2 * tile].T

        def build(pm, w, i):
            rows = mt[w % 2, pl.ds(i * tile, tile)]
            lane = lax.broadcasted_iota(jnp.int32, (tile, 128), 1).astype(F32)
            slot = jnp.zeros((tile, 128), F32)
            gate = jnp.zeros((tile, 128), F32)
            for j in range(6):
                hit = lane == rows[:, j:j + 1]
                slot = slot + jnp.where(hit, rows[:, 8 + j:9 + j] + 4096.0, 0.0)
                gate = gate + jnp.where(hit, rows[:, 16 + j:17 + j], 0.0)
            slot = slot - 4096.0
            for k0 in range(0, kk, 128):
                v = jnp.zeros((tile, 128), F32)
                for e in range(k0 // cap, min(experts - 1, (k0 + 127) // cap) + 1):
                    v = jnp.where(lane + float(k0 - e * cap) == slot[:, e:e + 1], gate[:, e:e + 1], v)
                for i_part, part in enumerate(_parts(v)):
                    pm[pl.ds(i_part * tile, tile), pl.ds(k0, 128)] = part

        def send_sum(w, i):
            p, axis, off, mh = role(w)
            b = w % keep
            src = sb.at[b * 2 + i]
            rows = pl.ds((mh * 2 + i) * tile, tile)
            out = [rxf.at[j, rows, pl.ds(pl.multiple_of(axis * dh, dh), dh)] for j in range(3)]

            for way in range(2):
                step = 1 - 2 * way

                @pl.when((off == far) & (mh == way))
                def _():
                    remote(src, rx2.at[p, way, i], bsem.at[b], r2sem.at[p, way, i], device(axis, step, c)).start()

                @pl.when(off == (side + step) % side)
                def _():
                    remote(src, out[way], bsem.at[b], rfsem.at[way], device(axis, step, p)).start()

            @pl.when((off == 0) & (axis == 0))
            def _():
                pltpu.make_async_copy(src, out[2], bsem.at[b]).start()

            @pl.when((off == 0) & (axis == 1))
            def _():
                remote(src, out[2], bsem.at[b], rfsem.at[2], device(axis, 0, p)).start()

        def wait_sent(b):
            sent = sb.at[pl.ds(b * 2, 2)]
            pltpu.make_async_copy(sent, sent, bsem.at[b]).wait()

        pltpu.make_async_copy(mr, mr, msem).wait()
        start_load(0)
        prepare(0)
        build(pma, 0, 0)

        @pl.loop(0, units)
        def _(w):
            p, axis, off, mh = role(w)
            after = w + 1 - (w + 1) // units
            load(w)[2].wait()

            @pl.when(w + 1 < units)
            def _():
                start_load(w + 1)
                prepare(w + 1)

            @pl.when(w == 2)
            def _():
                forward(1, far)

                @pl.loop(4, STEPS)
                def _(k):
                    send(1, k, 0)

            @pl.when(w == 4)
            def _():
                for other in range(side):
                    if other != far:
                        forward(1, other)

            @pl.when(w >= keep)
            def _():
                wait_sent(w % keep)

            for i, pm in ((0, pma), (1, pmb)):
                here = w % keep * 2 + i
                wide = min(512, dh)
                for j in range(dh // wide):
                    cols = pl.ds(j * wide, wide)
                    o = jnp.dot(pm[...], rb[w % 2, :, cols], preferred_element_type=F32)
                    sb[here, :, cols] = o[:tile] + o[tile:2 * tile] + o[2 * tile:]
                if i == 0:
                    build(pmb, w, 1)
                else:
                    build(pma, after, 0)

                for way in range(2):
                    @pl.when((off == (side + 1 - 2 * way) % side) & (mh == way))
                    def _():
                        got = rx2.at[p, way, i]
                        pltpu.make_async_copy(got, got, r2sem.at[p, way, i]).wait()
                        sb[here] = sb[here] + rx2[p, way, i]

                send_sum(w, i)

        for w in range(units - keep, units):
            wait_sent(w % keep)

    pl.run_scoped(
        combine_phase,
        pltpu.VMEM((2, kk, dh), BF16),
        pltpu.VMEM((2, 2 * tile, 128), F32),
        pltpu.VMEM((3 * tile, kk), BF16),
        pltpu.VMEM((3 * tile, kk), BF16),
        pltpu.VMEM((keep * 2, tile, dh), F32),
    )

    for p in range(2):
        blocks = ys[p].at[pl.ds(0, 2 * STEPS - 2)]
        pltpu.make_async_copy(blocks, blocks, ssem.at[p]).wait()
        pltpu.make_async_copy(rl.at[p], rl.at[p], fsem.at[p]).wait()
    for j, got in enumerate((rxf.at[0], rxf.at[1], rxf.at[2, :, pl.ds(dh, dh)])):
        pltpu.make_async_copy(got, got, rfsem.at[j]).wait()


ANY = pl.BlockSpec(memory_space=pl.ANY)


def _experts(ug, ue1, ue3, ue2, n, cap, t):
    d, f = ug.shape[-1], ue1.shape[-1]
    return pl.pallas_call(
        functools.partial(_k1, n, cap),
        out_shape=jax.ShapeDtypeStruct((2 * STEPS, 2, 2 * cap, d // 2), BF16),
        in_specs=[ANY] * 4,
        out_specs=ANY,
        scratch_shapes=_ffn_scratch(t, d, f, cap) + FFN_SEMS,
        cost_estimate=pl.CostEstimate(flops=n * cap * (2 * t * d + 6 * d * f), bytes_accessed=2 * n * t * d, transcendentals=n * cap * f),
        compiler_params=pltpu.CompilerParams(vmem_limit_bytes=67043328),
        name='experts',
    )(ug, ue1, ue3, ue2)


def _exchange(ug0, ug1, y0, ue1, ue3, ue2, n, cap, t):
    d, f = ug0.shape[-1], ue1.shape[-1]
    dh = d // 2
    side = math.isqrt(n // CORES)
    tile = t // 4
    kk = CORES * side * 2 * cap
    keep = 4
    flops = n * cap * (2 * t * d + 6 * d * f) + 2 * side * 3 * 2 * t * kk * dh
    return pl.pallas_call(
        functools.partial(_k2, n, cap, keep),
        out_shape=(
            jax.ShapeDtypeStruct((3, t, d), F32),
            jax.ShapeDtypeStruct(y0.shape, BF16),
            jax.ShapeDtypeStruct((2, side, kk, dh), BF16),
            jax.ShapeDtypeStruct((2, 2, 2, side, cap, dh), BF16),
        ),
        in_specs=[ANY] * 6,
        out_specs=(ANY,) * 4,
        scratch_shapes=[
            pltpu.VMEM((2, 2, 2, tile, dh), F32),
            pltpu.VMEM((2, side, EXTRA, d), BF16),
        ] + FFN_SEMS + [
            pltpu.SemaphoreType.DMA((2,)),
            pltpu.SemaphoreType.DMA((2, side)),
            pltpu.SemaphoreType.DMA((2, 2, 2, side)),
            pltpu.SemaphoreType.DMA((2,)),
            pltpu.SemaphoreType.DMA((2,)),
            pltpu.SemaphoreType.DMA,
            pltpu.SemaphoreType.DMA((keep,)),
            pltpu.SemaphoreType.DMA((2, 2, 2)),
            pltpu.SemaphoreType.DMA((3,)),
        ],
        cost_estimate=pl.CostEstimate(flops=flops, bytes_accessed=4 * n * t * d, transcendentals=n * cap * f),
        compiler_params=pltpu.CompilerParams(collective_id=0, has_side_effects=True, vmem_limit_bytes=67043328),
        name='exchange',
    )(ug0, ug1, y0, ue1, ue3, ue2)[0]


def _encode(gi, sl, gate):
    hi, mid, lo = (p.T for p in _parts(gate))
    left = jnp.concatenate([gi.T.astype(BF16), sl.T.astype(BF16), lo[:4]], axis=0)
    right = jnp.concatenate([hi, mid, lo[4:], jnp.zeros((2, gi.shape[0]), BF16)], axis=0)
    return jnp.concatenate([left, right], axis=1)


def solution(mesh):
    n = mesh.shape['ep']
    rows = P(('dp', 'ep'))
    rep = P()

    def local(h0, idx, slot, ln_attn, wq, wk, wv, wo, ln_ffn, ws1, ws3, ws2, ln_moe, wr, ue1, ue3, ue2):
        b, s, d = h0.shape
        top = idx.shape[-1]
        ne = ue1.shape[0] * n
        t = b * s
        cap = CAP_FACTOR * t * top // ne
        u = _rms(h0, ln_moe).reshape(t, d)
        gi, sl = idx.reshape(t, top), slot.reshape(t, top)
        gate = _gate(u, wr, gi)
        mine = jnp.concatenate([u, _encode(gi, sl, gate)], axis=0)
        part = mine.shape[0] // CORES
        c = lax.axis_index('ep') % CORES
        kept = lax.dynamic_slice_in_dim(mine, c * part, part)
        given = lax.dynamic_slice_in_dim(mine, (1 - c) * part, part)
        taken = lax.ppermute(given, 'ep', [(i, i ^ 1) for i in range(n)])
        ug0 = lax.all_gather(jnp.where(c == 0, kept, taken), 'ep').reshape(n // CORES, -1, d)
        ug1 = lax.all_gather(jnp.where(c == 0, taken, kept), 'ep').reshape(n // CORES, -1, d)
        a, fo = _dense(h0, ln_attn, wq, wk, wv, wo, ln_ffn, ws1, ws3, ws2)
        z = (a.astype(F32) + fo).reshape(t, d)
        ug0, z = lax.optimization_barrier((ug0, z))
        y0 = _experts(ug0, ue1, ue3, ue2, n, cap, t)
        r = _exchange(ug0, ug1, y0, ue1, ue3, ue2, n, cap, t)
        return (z + (r[0] + r[1] + r[2])).astype(BF16).reshape(b, s, d)

    specs = (rows, rows, rows) + (rep,) * 11 + (P('ep'), P('ep'), P('ep'))
    return jax.shard_map(local, mesh=mesh, in_specs=specs, out_specs=rows, check_vma=False)
```

```python
import functools
import math

import jax
import jax.numpy as jnp
from jax import lax
from jax.experimental import pallas as pl
from jax.experimental.pallas import tpu as pltpu
from jax.sharding import PartitionSpec as P

HEAD = 128
LANES = 128
EPS = 1e-6
CAP_FACTOR = 2
CORES = 2
F32 = jnp.float32
BF16 = jnp.bfloat16
MESH = pl.DeviceIdType.MESH
BOTH = (0, 1)
SEM = pltpu.SemaphoreType.DMA
SEM2, SEM4 = SEM((2,)), SEM((4,))


def _mm(form, a, b):
    return jnp.einsum(form, a, b, preferred_element_type=jnp.float32)


def _rms(x, w):
    xf = x.astype(jnp.float32)
    r = lax.rsqrt(jnp.mean(xf * xf, axis=-1, keepdims=True) + EPS)
    return (xf * r * w.astype(jnp.float32)).astype(jnp.bfloat16)


def _rope(x):
    s, half = x.shape[1], x.shape[-1] // 2
    freq = 10000.0 ** (-jnp.arange(half, dtype=jnp.float32) / half)
    ang = jnp.arange(s, dtype=jnp.float32)[:, None] * freq[None, :]
    c = jnp.cos(ang)[None, :, None, :]
    sn = jnp.sin(ang)[None, :, None, :]
    x1, x2 = x[..., :half], x[..., half:]
    return jnp.concatenate([x1 * c - x2 * sn, x2 * c + x1 * sn], axis=-1)


def _dense(h0, ln_attn, wq, wk, wv, wo, ln_ffn, ws1, ws3, ws2):
    b, s, _ = h0.shape
    nh = wq.shape[1] // HEAD
    x1 = _rms(h0, ln_attn)
    q = _rope(_mm('bsd,de->bse', x1, wq).reshape(b, s, nh, HEAD)).astype(jnp.bfloat16)
    k = _rope(_mm('bsd,de->bse', x1, wk).reshape(b, s, nh, HEAD)).astype(jnp.bfloat16)
    v = _mm('bsd,de->bse', x1, wv).astype(jnp.bfloat16).reshape(b, s, nh, HEAD)
    sc = _mm('bqhe,bkhe->bhqk', q, k) * HEAD ** -0.5
    causal = jnp.arange(s)[:, None] >= jnp.arange(s)[None, :]
    p = jax.nn.softmax(jnp.where(causal, sc, -1e30), axis=-1).astype(jnp.bfloat16)
    o = _mm('bhqk,bkhe->bqhe', p, v).astype(jnp.bfloat16).reshape(b, s, nh * HEAD)
    a = (h0.astype(jnp.float32) + _mm('bse,ed->bsd', o, wo)).astype(jnp.bfloat16)
    x2 = _rms(a, ln_ffn)
    hs = (jax.nn.silu(_mm('bsd,df->bsf', x2, ws1)) * _mm('bsd,df->bsf', x2, ws3)).astype(jnp.bfloat16)
    return a, _mm('bsf,fd->bsd', hs, ws2)


def _parts(c):
    hi = c.astype(jnp.bfloat16)
    r = c - hi.astype(jnp.float32)
    mid = r.astype(jnp.bfloat16)
    lo = (r - mid.astype(jnp.float32)).astype(jnp.bfloat16)
    return hi, mid, lo


def _place(n):
    side = math.isqrt(n // CORES)
    me = lax.axis_index('ep')
    return side, me, (me // CORES) % side, me // (CORES * side), me % CORES


def _pick(table, k):
    power = (1 + 3 * (k % 2)) * (1 + 15 * (k // 2 % 2)) * (1 + 255 * (k // 4))
    return table // power % 4


def _pack(values):
    return sum(int(v) * 4 ** i for i, v in enumerate(values))


STEP_X = (_pack('22101110'), _pack('22303330'))
STEP_Y = (_pack('21221301'), _pack('03203103'))
STEPS = 8


def _order(k, i):
    return _pick(STEP_X[i], k), _pick(STEP_Y[i], k)


def _routing(rows, t):
    e = rows.astype(F32)
    half = t // 2

    def block(q):
        return jnp.concatenate([e[i][:, q * half:(q + 1) * half] for i in BOTH], axis=1)

    b = [block(q) for q in range(4)]
    lo = jnp.concatenate([b[0][6:], b[1][6:], b[2][6:]], axis=0)
    return b[0][:6], b[1][:6], b[2][:6] + b[3][:6] + lo


def _k0(n, h0, idx, slot, ln, wr, out0, out1, hb, ub, eb, hsem, lsem, ssem, rsem):
    side, me, x, y, c = _place(n)
    t = hb.shape[0]
    half, tile, ne = t // 2, t // 4, wr.shape[0]
    order = (1 - c, c)

    def h_copy(o, i):
        rows = pl.ds(pl.multiple_of((order[o] * 2 + i) * tile, tile), tile)
        return pltpu.make_async_copy(h0.at[rows], hb.at[pl.ds((o * 2 + i) * tile, tile)], hsem.at[o * 2 + i])

    for o in BOTH:
        for i in BOTH:
            h_copy(o, i).start()

    other = me + 1 - 2 * c
    barrier = pltpu.get_barrier_semaphore()
    pl.semaphore_signal(barrier, inc=1, device_id={'ep': other}, device_id_type=MESH)
    pl.semaphore_wait(barrier, 1)

    def gives(out):
        return [
            pltpu.make_async_remote_copy(src, out.at[rows], ssem.at[j], rsem.at[j], device_id={'ep': other}, device_id_type=MESH)
            for j, (src, rows) in enumerate(((ub.at[0], pl.ds(0, half)), (eb.at[0], pl.ds(half, 8))))
        ]

    def keeps(out):
        return [
            pltpu.make_async_copy(src, out.at[rows], lsem.at[j])
            for j, (src, rows) in enumerate(((ub.at[1], pl.ds(0, half)), (eb.at[1], pl.ds(half, 8))))
        ]

    w = ln[...].astype(F32)
    expert = lax.broadcasted_iota(jnp.int32, (ne, tile), 0)
    for o in BOTH:
        for i in BOTH:
            h_copy(o, i).wait()
            xf = hb[pl.ds((o * 2 + i) * tile, tile)].astype(F32)
            u = (xf * lax.rsqrt(jnp.mean(xf * xf, axis=-1, keepdims=True) + EPS) * w).astype(BF16)
            ub[o, pl.ds(i * tile, tile)] = u
            lg = lax.dot_general(wr[...], u, (((1,), (1,)), ((), ())), preferred_element_type=F32)
            cols = pl.ds(pl.multiple_of((order[o] * 2 + i) * tile, tile), tile)
            ex, sl = idx[:, cols], slot[:, cols]
            pick = [jnp.sum(jnp.where(expert == ex[j:j + 1], lg, 0.0), axis=0, keepdims=True) for j in range(6)]
            top = functools.reduce(jnp.maximum, pick)
            e = [jnp.exp(v - top) for v in pick]
            total = functools.reduce(jnp.add, e)
            parts = [_parts(v / total) for v in e]
            hi, mid, lo = ([p[q].astype(F32) for p in parts] for q in range(3))
            exf, slf = ex.astype(F32), sl.astype(F32)
            zero = jnp.zeros((1, tile), F32)
            blocks = ([exf] + lo[:2], [slf] + lo[2:4], hi + lo[4:], mid + [zero, zero])
            for q, rows in enumerate(blocks):
                eb[o, :, pl.ds(q * half + i * tile, tile)] = jnp.concatenate(rows, axis=0).astype(BF16)
        for p, out in enumerate((out0, out1)):
            @pl.when(c == p)
            def _():
                for cp in (gives(out) if o == 0 else keeps(out)):
                    cp.start()
    for cp in gives(out0) + keeps(out0):
        cp.wait()


def _ffn(n, cap, ugs, ue1, ue3, ue2, y_out, w13, w2, u, ur, pm, xs, h, ys, wsem, w2sem, usem, ysem, before):
    side, me, x, y, c = _place(n)
    t, d = pm.shape[1], u.shape[2]
    f = h.shape[1]
    dh, th = d // 2, t // 2

    def load_u(ug, k):
        for i in BOTH:
            dx, dy = _order(k, i)
            chip = (y + dy) % side * side + (x + dx) % side
            for j in BOTH:
                pltpu.make_async_copy(ug.at[chip, j, pl.ds(0, th)], u.at[i, pl.ds(j * th, th)], usem.at[i]).start()
                pltpu.make_async_copy(ug.at[chip, j, pl.ds(th, 8)], ur.at[i, j], usem.at[2 + i]).start()

    def weights(el):
        for j in range(f // LANES):
            pltpu.make_async_copy(ue1.at[el, :, pl.ds(LANES * j, LANES)], w13.at[el, :, pl.ds(256 * j, LANES)], wsem.at[el]).start()
            pltpu.make_async_copy(ue3.at[el, :, pl.ds(LANES * j, LANES)], w13.at[el, :, pl.ds(256 * j + LANES, LANES)], wsem.at[el]).start()
        pltpu.make_async_copy(ue2.at[el], w2.at[el], w2sem.at[el]).start()

    def keep(p, k, el):
        for i in BOTH:
            for half in BOTH:
                pltpu.make_async_copy(
                    ys.at[el, pl.ds(i * cap, cap), pl.ds(half * dh, dh)],
                    y_out.at[p, 2 * k + i, half, pl.ds(el * cap, cap)], ysem.at[el]).start()

    def wait_kept(el):
        pltpu.make_async_copy(ys.at[el], ys.at[el], ysem.at[el]).wait()

    load_u(ugs[0], 0)
    for el in BOTH:
        weights(el)

    @pl.loop(0, 2 * STEPS)
    def _(step):
        p, k = step // STEPS, step % STEPS
        before(step)

        @pl.when(step == STEPS)
        def _():
            load_u(ugs[1], 0)

        @pl.loop(0, 2)
        def _(i):
            pltpu.make_async_copy(u.at[i], u.at[i], usem.at[i]).wait()
            pltpu.make_async_copy(ur.at[i], ur.at[i], usem.at[2 + i]).wait()
            ex, sl, _ = _routing(ur[i], t)
            slot = lax.broadcasted_iota(jnp.int32, (cap, t), 0).astype(F32)
            for el in BOTH:
                mine = (me * 2 + el).astype(F32)
                q = jnp.sum(jnp.where(ex == mine, sl + 1.0, 0.0), axis=0, keepdims=True) - 1.0
                pm[pl.ds(el * cap, cap)] = jnp.where(slot == q, 1.0, 0.0).astype(BF16)
            wide = min(512, d)
            for m in range(d // wide):
                cols = pl.ds(m * wide, wide)
                got = jnp.dot(pm[...], u[i, :, cols], preferred_element_type=F32).astype(BF16)
                for el in BOTH:
                    xs[el, pl.ds(pl.multiple_of(i * cap, 16), cap), cols] = got[el * cap:(el + 1) * cap]

        @pl.when(step < STEPS - 1)
        def _():
            load_u(ugs[0], k + 1)

        @pl.when((step >= STEPS) & (step < 2 * STEPS - 1))
        def _():
            load_u(ugs[1], k + 1)

        @pl.loop(0, 2)
        def _(el):
            @pl.when(step == 0)
            def _():
                pltpu.make_async_copy(w13.at[el], w13.at[el], wsem.at[el]).wait()
                pltpu.make_async_copy(w2.at[el], w2.at[el], w2sem.at[el]).wait()

            group = 2
            for j in range(0, f // LANES, group):
                g = min(group, f // LANES - j)
                a = jnp.dot(xs[el], w13[el, :, pl.ds(256 * j, 256 * g)], preferred_element_type=F32)
                for i in range(g):
                    a1, a3 = a[:, 256 * i:256 * i + LANES], a[:, 256 * i + LANES:256 * i + 256]
                    h[:, pl.ds(LANES * (j + i), LANES)] = (jax.nn.silu(a1) * a3).astype(BF16)

            @pl.when(step >= 1)
            def _():
                wait_kept(el)

            wide = min(512, d)
            for m in range(d // wide):
                cols = pl.ds(m * wide, wide)
                ys[el, :, cols] = jnp.dot(h[...], w2[el, :, cols], preferred_element_type=F32).astype(BF16)
            keep(p, k, el)

    for el in BOTH:
        wait_kept(el)


def _ffn_scratch(t, d, f, cap):
    cap2 = 2 * cap
    return [
        pltpu.VMEM((2, d, 2 * f), BF16),
        pltpu.VMEM((2, f, d), BF16),
        pltpu.VMEM((2, t, d), BF16),
        pltpu.VMEM((2, 2, 8, d), BF16),
        pltpu.VMEM((cap2, t), BF16),
        pltpu.VMEM((2, cap2, d), BF16),
        pltpu.VMEM((cap2, f), BF16),
        pltpu.VMEM((2, cap2, d), BF16),
    ]


FFN_SEMS = [SEM2] * 2 + [SEM4, SEM2]


def _split(a, b):
    return a + ((b - a) // 8 + 1) // 2 * 8


BOTH_NEAR, BOTH_FAR = ((0, -1), (1, 1)), ((0, 2), (1, 2))
STAGE = {0: 1, -1: 2, 1: 3, 2: 4}


class _Gather:
    def __init__(self, n, own, out, send_sem, recv_sem, pair_sem):
        self.side, self.me, self.x, self.y, self.c = _place(n)
        self.own, self.out = own, out
        self.send_sem, self.recv_sem, self.pair_sem = send_sem, recv_sem, pair_sem
        rows = own.shape[0]
        mid = _split(0, rows)
        self.rows = ((0, mid), (mid, rows))

    def device(self, axis, off, cc):
        side = self.side
        return ((self.y + axis * off) % side * side + (self.x + (1 - axis) * off) % side) * CORES + cc

    def place(self, color, j, s, part=None):
        side = self.side
        dx, dy = (j, s) if color == 0 else (s, j)
        chip = (self.y + dy + side) % side * side + (self.x + dx + side) % side
        a, b = self.rows[color]
        if part is not None:
            mid = _split(a, b)
            a, b = (a, mid) if part == 0 else (mid, b)
        return self.out.at[chip, self.c, pl.ds(a, b - a)]

    def copy(self, color, src, dst, axis, way, sem):
        dest = self.device(axis, 1 - 2 * way, self.c)
        pltpu.make_async_remote_copy(src, dst, self.send_sem, sem, device_id={'ep': dest}, device_id_type=MESH).start()

    def share(self, src, dst):
        other = self.device(0, 0, 1 - self.c)
        pltpu.make_async_remote_copy(src, dst, self.pair_sem.at[0], self.pair_sem.at[1], device_id={'ep': other}, device_id_type=MESH).start()

    def wait(self, ref, sem):
        pltpu.make_async_copy(ref, ref, sem).wait()

    def start(self):
        for color in BOTH:
            a, b = self.rows[color]
            src, dst = self.own.at[pl.ds(a, b - a)], self.place(color, 0, 0)
            for stage in BOTH:
                for way in BOTH:
                    self.copy(color, src, dst, color if stage == 0 else 1 - color, way, self.recv_sem.at[color, stage, way])
            self.share(src, dst)

    def along(self, j):
        items = []
        for color in BOTH:
            for way, off in (BOTH_FAR if j == 2 else BOTH_NEAR):
                if j == 2:
                    self.wait(self.place(color, off, 0, way), self.recv_sem.at[color, 0, 2 + way])
                else:
                    self.wait(self.place(color, off, 0), self.recv_sem.at[color, 0, way])
                    half = self.place(color, off, 0, way)
                    self.copy(color, half, half, color, way, self.recv_sem.at[color, 0, 2 + way])
                    items.append((color, off))
            if j == 2:
                items.append((color, j))
        for color, off in items:
            item = self.place(color, off, 0)
            for way in BOTH:
                self.copy(color, item, item, 1 - color, way, self.recv_sem.at[color, STAGE[off], way])
            self.share(item, item)

    def across(self, offs):
        for color in BOTH:
            for off in offs:
                at = STAGE[off]
                for way, s in BOTH_NEAR:
                    item = self.place(color, off, s)
                    self.wait(item, self.recv_sem.at[color, at, way])
                    half = self.place(color, off, s, way)
                    self.copy(color, half, half, 1 - color, way, self.recv_sem.at[color, at, 2 + way])
                    self.share(item, item)

    def last(self, offs):
        for color in BOTH:
            for off in offs:
                at = STAGE[off]
                for way in BOTH:
                    self.wait(self.place(color, off, 2, way), self.recv_sem.at[color, at, 2 + way])
                item = self.place(color, off, 2)
                self.share(item, item)

    def finish(self):
        got = self.out.at[:, 0]
        self.wait(got, self.pair_sem.at[1])

    def drain(self):
        chips = self.out.shape[0]
        self.wait(self.out.at[:, 0], self.pair_sem.at[0])
        self.wait(self.out.at[pl.ds(0, chips - 1), 0], self.send_sem)


def _k2(n, cap, keep, ug0, part1, ue1, ue3, ue2, rxf, ug1, ys, r, rl, rx2, mr, wsem, w2sem, usem, ysem,
        gsem, grsem, pairsem, osem, ssem, rsem, relsem, fsem, lsem, msem, bsem, r2sem, rfsem):
    side, me, x, y, c = _place(n)
    t, d = rxf.shape[1], rxf.shape[2]
    f = ue1.shape[2]
    kk, dh = r.shape[2], r.shape[3]
    tile = rx2.shape[3]
    experts = kk // cap
    far = side // 2
    units = 16
    th, cap2 = t // 2, 2 * cap
    gather = _Gather(n, part1, ug1, gsem, grsem, pairsem)

    def device(axis, off, cc):
        return ((y + axis * off) % side * side + (x + (1 - axis) * off) % side) * CORES + cc

    def remote(src, dst, send_sem, recv_sem, dest):
        return pltpu.make_async_remote_copy(src, dst, send_sem, recv_sem, device_id={'ep': dest}, device_id_type=MESH)

    def routing_rows(p, ug):
        axis = (c + p) % 2
        for off in range(side):
            pltpu.make_async_copy(ug.at[device(axis, off, 0) // CORES, :, pl.ds(th, 8)], mr.at[p, off], msem).start()

    kept = pltpu.make_async_copy(part1, ug1.at[me // CORES, c], osem)
    kept.start()
    routing_rows(0, ug0)

    barrier = pltpu.get_barrier_semaphore()
    peers = 0
    for off in range(side):
        for dc in range(CORES):
            for axis in BOTH:
                if off or (dc and not axis):
                    pl.semaphore_signal(barrier, inc=1, device_id={'ep': device(axis, off, (c + dc) % CORES)}, device_id_type=MESH)
                    peers += 1
    pl.semaphore_wait(barrier, peers)

    def send(p, k, want_far):
        for i in BOTH:
            dx, dy = _order(k, i)
            for half, off, other, mine, line in ((0, dy, dx, y, (x + dx) % side), (1, dx, dy, x, (y + dy) % side)):
                cc = (p + half) % 2
                src = ys.at[p, 2 * k + i, half]

                def near():
                    own = (off == 0) & (c == cc)
                    dst = r.at[p, line, pl.ds((mine * CORES + c) * cap2, cap2)]

                    @pl.when(own)
                    def _():
                        pltpu.make_async_copy(src, dst, rsem.at[p, line]).start()

                    @pl.when(jnp.logical_not(own) & (off != far))
                    def _():
                        remote(src, dst, ssem.at[p], rsem.at[p, line], device(1 - half, off, cc)).start()

                def relayed():
                    @pl.when(off == far)
                    def _():
                        for el in BOTH:
                            at = (p, half, el, other)
                            remote(src.at[pl.ds(el * cap, cap)], rl.at[at], ssem.at[p], relsem.at[at], device(1 - half, 1 - 2 * el, c)).start()

                if want_far != 0:
                    relayed()
                if want_far != 1:
                    near()

    def forward(p, other):
        for half, mine, line in ((0, y, (x + other) % side), (1, x, (y + other) % side)):
            for el in BOTH:
                at = (p, half, el, other)
                step = 1 - 2 * el
                pltpu.make_async_copy(rl.at[at], rl.at[at], relsem.at[at]).wait()
                origin = (mine - step + side) % side
                dst = r.at[p, line, pl.ds((origin * CORES + c) * cap2 + el * cap, cap)]
                remote(rl.at[at], dst, fsem.at[p], rsem.at[p, line], device(1 - half, step, (p + half) % 2)).start()

    gather.start()

    def before(step):
        def at(s):
            return pl.when(step == s)

        @at(1)
        def _():
            gather.along(1)

        @at(2)
        def _():
            gather.across((0,))

        @at(4)
        def _():
            gather.along(2)

        @at(5)
        def _():
            gather.across((-1, 1))

        @at(6)
        def _():
            gather.last((0,))

        @at(7)
        def _():
            gather.across((2,))

            @pl.loop(0, 6)
            def _(k):
                send(0, k, 1)

            @pl.loop(0, 6)
            def _(k):
                send(0, k, 0)

        @at(8)
        def _():
            gather.last((-1, 1, 2))
            kept.wait()
            gather.finish()
            routing_rows(1, ug1)

        @pl.when((step == 8) | (step == 9))
        def _():
            send(0, step - 2, 0)

        @at(10)
        def _():
            @pl.loop(0, side)
            def _(other):
                forward(0, other)

        @pl.when((step >= 10) & (step < 14))
        def _():
            send(1, step - 10, 2)

    def experts_phase(*refs):
        _ffn(n, cap, (ug0, ug1), ue1, ue3, ue2, ys, *refs, wsem, w2sem, usem, ysem, before=before)

    pl.run_scoped(experts_phase, *_ffn_scratch(t, d, f, cap))

    def role(w):
        p, q, b = w // 8, w % 8 // 2, w % 2
        first = 1 - (q + 3) // 4
        middle = (q + 1) // 2 % 2
        off = first * far + middle * (1 + (side - 2) * b)
        return p, (c + p) % 2, off, b + middle * (q % 2) * (1 - 2 * b)

    def combine_phase(rb, mt, pma, pmb, sb):
        def load(w):
            p, axis, off, _ = role(w)
            line = (x * (1 - axis) + y * axis + off) % side
            return r.at[p, line], rsem.at[p, line], pltpu.make_async_copy(r.at[p, line], rb.at[w % 2], lsem.at[w % 2])

        def start_load(w):
            rows, sem, copy = load(w)
            q, b = w % 8 // 2, w % 2

            @pl.when((q == 1) | ((b == 0) & (q != 2)))
            def _():
                pltpu.make_async_copy(rows, rows, sem).wait()

            copy.start()

        def prepare(w):
            p, axis, off, mh = role(w)
            af = axis.astype(F32)
            ex, sl, g = _routing(mr[p, off], t)
            cy = jnp.floor(ex * (1.0 / (2 * CORES * side)))
            cx = jnp.floor((ex - cy * (2 * CORES * side)) * (1.0 / (2 * CORES)))
            low = ex - cy * (2 * CORES * side) - cx * (2 * CORES)
            mine = x.astype(F32) * (1.0 - af) + y.astype(F32) * af
            across = cx * (1.0 - af) + cy * af
            along = cy * (1.0 - af) + cx * af
            e = jnp.where(across == mine, along * (2 * CORES) + low, -1.0)
            gap = jnp.zeros((2, t), F32)
            m = jnp.concatenate([e, gap, sl, gap, g, jnp.zeros((106, t), F32)], axis=0)
            for i in BOTH:
                @pl.when(mh == i)
                def _():
                    mt[w % 2] = m[:, i * 2 * tile:(i + 1) * 2 * tile].T

        def build(pm, w, i):
            rows = mt[w % 2, pl.ds(i * tile, tile)]
            lane = lax.broadcasted_iota(jnp.int32, (tile, LANES), 1).astype(F32)
            slot = jnp.zeros((tile, LANES), F32)
            gate = jnp.zeros((tile, LANES), F32)
            for j in range(6):
                hit = lane == rows[:, j:j + 1]
                slot = slot + jnp.where(hit, rows[:, 8 + j:9 + j] + 4096.0, 0.0)
                gate = gate + jnp.where(hit, rows[:, 16 + j:17 + j], 0.0)
            slot = slot - 4096.0
            for k0 in range(0, kk, LANES):
                v = jnp.zeros((tile, LANES), F32)
                for e in range(k0 // cap, min(experts - 1, (k0 + 127) // cap) + 1):
                    v = jnp.where(lane + float(k0 - e * cap) == slot[:, e:e + 1], gate[:, e:e + 1], v)
                for i_part, part in enumerate(_parts(v)):
                    pm[pl.ds(i_part * tile, tile), pl.ds(k0, LANES)] = part

        def send_sum(w, i):
            p, axis, off, mh = role(w)
            b = w % keep
            src = sb.at[b * 2 + i]
            rows = pl.ds((mh * 2 + i) * tile, tile)
            out = [rxf.at[j, rows, pl.ds(pl.multiple_of(axis * dh, dh), dh)] for j in range(3)]

            for way in BOTH:
                step = 1 - 2 * way

                @pl.when((off == far) & (mh == way))
                def _():
                    remote(src, rx2.at[p, way, i], bsem.at[b], r2sem.at[p, way, i], device(axis, step, c)).start()

                @pl.when(off == (side + step) % side)
                def _():
                    remote(src, out[way], bsem.at[b], rfsem.at[way], device(axis, step, p)).start()

            @pl.when((off == 0) & (axis == 0))
            def _():
                pltpu.make_async_copy(src, out[2], bsem.at[b]).start()

            @pl.when((off == 0) & (axis == 1))
            def _():
                remote(src, out[2], bsem.at[b], rfsem.at[2], device(axis, 0, p)).start()

        def wait_sent(b):
            sent = sb.at[pl.ds(b * 2, 2)]
            pltpu.make_async_copy(sent, sent, bsem.at[b]).wait()

        pltpu.make_async_copy(mr, mr, msem).wait()
        start_load(0)
        prepare(0)
        build(pma, 0, 0)

        @pl.loop(0, units)
        def _(w):
            p, axis, off, mh = role(w)
            after = w + 1 - (w + 1) // units
            load(w)[2].wait()

            @pl.when(w + 1 < units)
            def _():
                start_load(w + 1)
                prepare(w + 1)

            @pl.when(w == 2)
            def _():
                forward(1, far)

                @pl.loop(4, STEPS)
                def _(k):
                    send(1, k, 0)

            @pl.when(w == 4)
            def _():
                for other in range(side):
                    if other != far:
                        forward(1, other)

            @pl.when(w >= keep)
            def _():
                wait_sent(w % keep)

            for i, pm in ((0, pma), (1, pmb)):
                here = w % keep * 2 + i
                wide = min(512, dh)
                for j in range(dh // wide):
                    cols = pl.ds(j * wide, wide)
                    o = jnp.dot(pm[...], rb[w % 2, :, cols], preferred_element_type=F32)
                    sb[here, :, cols] = o[:tile] + o[tile:2 * tile] + o[2 * tile:]
                if i == 0:
                    build(pmb, w, 1)
                else:
                    build(pma, after, 0)

                for way in BOTH:
                    @pl.when((off == (side + 1 - 2 * way) % side) & (mh == way))
                    def _():
                        got = rx2.at[p, way, i]
                        pltpu.make_async_copy(got, got, r2sem.at[p, way, i]).wait()
                        sb[here] = sb[here] + rx2[p, way, i]

                send_sum(w, i)

        for w in range(units - keep, units):
            wait_sent(w % keep)

    pl.run_scoped(
        combine_phase,
        pltpu.VMEM((2, kk, dh), BF16),
        pltpu.VMEM((2, 2 * tile, LANES), F32),
        pltpu.VMEM((3 * tile, kk), BF16),
        pltpu.VMEM((3 * tile, kk), BF16),
        pltpu.VMEM((keep * 2, tile, dh), F32),
    )

    gather.drain()
    for p in BOTH:
        blocks = ys.at[p, pl.ds(0, 2 * STEPS - 2)]
        pltpu.make_async_copy(blocks, blocks, ssem.at[p]).wait()
        pltpu.make_async_copy(rl.at[p], rl.at[p], fsem.at[p]).wait()
    for j, got in enumerate((rxf.at[0], rxf.at[1], rxf.at[2, :, pl.ds(dh, dh)])):
        pltpu.make_async_copy(got, got, rfsem.at[j]).wait()


ANY = pl.BlockSpec(memory_space=pl.ANY)


def _rows(h0, idx, slot, ln, wr, n):
    t, d = h0.shape
    vmem = pl.BlockSpec(memory_space=pltpu.VMEM)
    return pl.pallas_call(
        functools.partial(_k0, n),
        out_shape=(jax.ShapeDtypeStruct((t // 2 + 8, d), BF16),) * CORES,
        in_specs=[ANY] + [vmem] * 4,
        out_specs=(ANY,) * CORES,
        scratch_shapes=[
            pltpu.VMEM((t, d), BF16),
            pltpu.VMEM((2, t // 2, d), BF16),
            pltpu.VMEM((2, 8, d), BF16),
            SEM4,
            SEM2,
            SEM2,
            SEM2,
        ],
        cost_estimate=pl.CostEstimate(flops=2 * t * d * 64, bytes_accessed=8 * t * d, transcendentals=0),
        compiler_params=pltpu.CompilerParams(collective_id=1, has_side_effects=True),
        name='rows',
    )(h0, idx, slot, ln, wr)


def _exchange(ug0, part1, ue1, ue3, ue2, n, cap, t):
    d, f = part1.shape[-1], ue1.shape[-1]
    dh = d // 2
    side = math.isqrt(n // CORES)
    tile = t // 4
    kk = CORES * side * 2 * cap
    keep = 4
    cap2 = 2 * cap
    flops = 2 * n * cap * (2 * t * d + 6 * d * f) + 2 * side * 3 * 2 * t * kk * dh
    return pl.pallas_call(
        functools.partial(_k2, n, cap, keep),
        out_shape=(
            jax.ShapeDtypeStruct((3, t, d), F32),
            jax.ShapeDtypeStruct(ug0.shape, BF16),
            jax.ShapeDtypeStruct((2, 2 * STEPS, 2, cap2, dh), BF16),
            jax.ShapeDtypeStruct((2, side, kk, dh), BF16),
            jax.ShapeDtypeStruct((2, 2, 2, side, cap, dh), BF16),
        ),
        in_specs=[ANY] * 5,
        out_specs=(ANY,) * 5,
        scratch_shapes=[
            pltpu.VMEM((2, 2, 2, tile, dh), F32),
            pltpu.VMEM((2, side, 2, 8, d), BF16),
        ] + FFN_SEMS + [
            SEM,
            pltpu.SemaphoreType.DMA((2, 5, 4)),
            SEM2,
            SEM,
            SEM2,
            pltpu.SemaphoreType.DMA((2, side)),
            pltpu.SemaphoreType.DMA((2, 2, 2, side)),
            SEM2,
            SEM2,
            SEM,
            pltpu.SemaphoreType.DMA((keep,)),
            pltpu.SemaphoreType.DMA((2, 2, 2)),
            pltpu.SemaphoreType.DMA((3,)),
        ],
        cost_estimate=pl.CostEstimate(flops=flops, bytes_accessed=4 * n * t * d, transcendentals=2 * n * cap * f),
        compiler_params=pltpu.CompilerParams(collective_id=0, has_side_effects=True, vmem_limit_bytes=67043328),
        name='exchange',
    )(ug0, part1, ue1, ue3, ue2)[0]


def solution(mesh):
    n = mesh.shape['ep']
    rows = P(('dp', 'ep'))
    rep = P()

    def local(h0, idx, slot, ln_attn, wq, wk, wv, wo, ln_ffn, ws1, ws3, ws2, ln_moe, wr, ue1, ue3, ue2):
        b, s, d = h0.shape
        top = idx.shape[-1]
        ne = ue1.shape[0] * n
        t = b * s
        cap = CAP_FACTOR * t * top // ne
        parts = _rows(h0.reshape(t, d), idx.reshape(t, top).T, slot.reshape(t, top).T, ln_moe.reshape(1, d), wr.T, n)
        ug0 = lax.all_gather(parts[0], 'ep').reshape(n // CORES, CORES, -1, d)
        a, fo = _dense(h0, ln_attn, wq, wk, wv, wo, ln_ffn, ws1, ws3, ws2)
        z = (a.astype(F32) + fo).reshape(t, d)
        ug0, z = lax.optimization_barrier((ug0, z))
        r = _exchange(ug0, parts[1], ue1, ue3, ue2, n, cap, t)
        return (z + (r[0] + r[1] + r[2])).astype(BF16).reshape(b, s, d)

    specs = (rows, rows, rows) + (rep,) * 11 + (P('ep'), P('ep'), P('ep'))
    return jax.shard_map(local, mesh=mesh, in_specs=specs, out_specs=rows, check_vma=False)
```

```python
import functools
import math

import jax
import jax.numpy as jnp
from jax import lax
from jax.experimental import pallas as pl
from jax.experimental.pallas import tpu as pltpu
from jax.sharding import PartitionSpec as P

HEAD = 128
LANES = 128
EPS = 1e-6
CAP_FACTOR = 2
CORES = 2
F32 = jnp.float32
BF16 = jnp.bfloat16
MESH = pl.DeviceIdType.MESH
BOTH = (0, 1)
PAIR = 2
NT = (((1,), (1,)), ((), ()))
STEP = (1, -1)
loop = functools.partial(pl.loop, 0)
SEM = pltpu.SemaphoreType.DMA
SEM2, SEM4 = SEM((2,)), SEM((4,))


def _turns(t):
    half = HEAD // 2
    freq = 10000.0 ** (-jnp.arange(half, dtype=F32) / half)
    ang = jnp.arange(t, dtype=F32)[:, None] * freq[None, :]
    c, s = jnp.cos(ang), jnp.sin(ang)
    return jnp.stack([jnp.concatenate([c, c], axis=1), jnp.concatenate([-s, s], axis=1)])


def _norm(xf, w):
    return (xf * lax.rsqrt(jnp.mean(xf * xf, axis=-1, keepdims=True) + EPS) * w).astype(BF16)


def _dot(a, b):
    return jnp.dot(a, b, preferred_element_type=F32)


def _parts(c):
    hi = c.astype(jnp.bfloat16)
    r = c - hi.astype(jnp.float32)
    mid = r.astype(jnp.bfloat16)
    lo = (r - mid.astype(jnp.float32)).astype(jnp.bfloat16)
    return hi, mid, lo


def _place(n):
    side = math.isqrt(n // CORES)
    me = lax.axis_index('ep')
    return side, me, (me // CORES) % side, me // (CORES * side), me % CORES


def _pick(table, k):
    power = (1 + 3 * (k % 2)) * (1 + 15 * (k // 2 % 2)) * (1 + 255 * (k // 4))
    return table // power % 4


def _pack(values):
    return sum(int(v) * 4 ** i for i, v in enumerate(values))


STEP_X = (_pack('22101110'), _pack('22303330'))
STEP_Y = (_pack('21221301'), _pack('03203103'))
STEPS = 8


def _order(k, i):
    return _pick(STEP_X[i], k), _pick(STEP_Y[i], k)


def _routing(rows, t):
    e = rows.astype(F32)
    half = t // 2

    def block(q):
        return jnp.concatenate([e[i][:, q * half:(q + 1) * half] for i in BOTH], axis=1)

    b = [block(q) for q in range(4)]
    lo = jnp.concatenate([b[0][6:], b[1][6:], b[2][6:]])
    return b[0][:6], b[1][:6], b[2][:6] + b[3][:6] + lo


def _k0(n, h0, idx, slot, ln, wr, out0, out1, hb, ub, eb, hsem, lsem, ssem, rsem):
    side, me, x, y, c = _place(n)
    t = hb.shape[0]
    half, tile, ne = t // 2, t // 4, wr.shape[0]
    order = (1 - c, c)

    def h_copy(o, i):
        rows = pl.ds(pl.multiple_of((order[o] * 2 + i) * tile, tile), tile)
        return pltpu.make_async_copy(h0.at[rows], hb.at[pl.ds((o * 2 + i) * tile, tile)], hsem.at[o * 2 + i])

    for o in BOTH:
        for i in BOTH:
            h_copy(o, i).start()

    other = me + 1 - 2 * c
    barrier = pltpu.get_barrier_semaphore()
    pl.semaphore_signal(barrier, device_id={'ep': other}, device_id_type=MESH)
    pl.semaphore_wait(barrier, 1)

    def gives(out):
        return [
            pltpu.make_async_remote_copy(src, out.at[rows], ssem.at[j], rsem.at[j], device_id={'ep': other}, device_id_type=MESH)
            for j, (src, rows) in enumerate(((ub.at[0], pl.ds(0, half)), (eb.at[0], pl.ds(half, 8))))
        ]

    def keeps(out):
        return [
            pltpu.make_async_copy(src, out.at[rows], lsem.at[j])
            for j, (src, rows) in enumerate(((ub.at[1], pl.ds(0, half)), (eb.at[1], pl.ds(half, 8))))
        ]

    w = ln[...].astype(F32)
    expert = lax.broadcasted_iota(jnp.int32, (ne, tile), 0)
    for o in BOTH:
        for i in BOTH:
            h_copy(o, i).wait()
            xf = hb[pl.ds((o * 2 + i) * tile, tile)].astype(F32)
            u = _norm(xf, w)
            ub[o, pl.ds(i * tile, tile)] = u
            lg = lax.dot_general(wr[...], u, NT, preferred_element_type=F32)
            cols = pl.ds(pl.multiple_of((order[o] * 2 + i) * tile, tile), tile)
            ex, sl = idx[:, cols], slot[:, cols]
            pick = [jnp.sum(jnp.where(expert == ex[j:j + 1], lg, 0.0), axis=0, keepdims=True) for j in range(6)]
            top = functools.reduce(jnp.maximum, pick)
            e = [jnp.exp(v - top) for v in pick]
            total = functools.reduce(jnp.add, e)
            parts = [_parts(v / total) for v in e]
            hi, mid, lo = ([p[q].astype(F32) for p in parts] for q in range(3))
            exf, slf = ex.astype(F32), sl.astype(F32)
            zero = jnp.zeros((1, tile), F32)
            blocks = ([exf] + lo[:2], [slf] + lo[2:4], hi + lo[4:], mid + [zero, zero])
            for q, rows in enumerate(blocks):
                eb[o, :, pl.ds(q * half + i * tile, tile)] = jnp.concatenate(rows).astype(BF16)
        for p, out in enumerate((out0, out1)):
            @pl.when(c == p)
            def _():
                for cp in (gives(out) if o == 0 else keeps(out)):
                    cp.start()
    for cp in gives(out0) + keeps(out0):
        cp.wait()


def _ffn(n, cap, ugs, ue1, ue3, ue2, y_out, w13, w2, u, ur, pm, xs, h, ys, wsem, w2sem, usem, ysem, before):
    side, me, x, y, c = _place(n)
    t, d = pm.shape[1], u.shape[2]
    f = h.shape[1]
    dh, th = d // 2, t // 2

    def load_u(ug, k):
        for i in BOTH:
            dx, dy = _order(k, i)
            chip = (y + dy) % side * side + (x + dx) % side
            for j in BOTH:
                pltpu.make_async_copy(ug.at[chip, j, pl.ds(0, th)], u.at[i, pl.ds(j * th, th)], usem.at[i]).start()
                pltpu.make_async_copy(ug.at[chip, j, pl.ds(th, 8)], ur.at[i, j], usem.at[2 + i]).start()

    def weights(el):
        for j in range(f // LANES):
            pltpu.make_async_copy(ue1.at[el, :, pl.ds(LANES * j, LANES)], w13.at[el, :, pl.ds(256 * j, LANES)], wsem.at[el]).start()
            pltpu.make_async_copy(ue3.at[el, :, pl.ds(LANES * j, LANES)], w13.at[el, :, pl.ds(256 * j + LANES, LANES)], wsem.at[el]).start()
        pltpu.make_async_copy(ue2.at[el], w2.at[el], w2sem.at[el]).start()

    def keep(p, k, el):
        for i in BOTH:
            for half in BOTH:
                pltpu.make_async_copy(
                    ys.at[el, pl.ds(i * cap, cap), pl.ds(half * dh, dh)],
                    y_out.at[p, 2 * k + i, half, pl.ds(el * cap, cap)], ysem.at[el]).start()

    def wait_kept(el):
        pltpu.make_async_copy(ys.at[el], ys.at[el], ysem.at[el]).wait()

    load_u(ugs[0], 0)
    for el in BOTH:
        weights(el)

    @loop(2 * STEPS)
    def _(step):
        p, k = step // STEPS, step % STEPS
        before(step)

        @pl.when(step == STEPS)
        def _():
            load_u(ugs[1], 0)

        @loop(2)
        def _(i):
            pltpu.make_async_copy(u.at[i], u.at[i], usem.at[i]).wait()
            pltpu.make_async_copy(ur.at[i], ur.at[i], usem.at[2 + i]).wait()
            ex, sl, _ = _routing(ur[i], t)
            slot = lax.broadcasted_iota(jnp.int32, (cap, t), 0).astype(F32)
            for el in BOTH:
                mine = (me * 2 + el).astype(F32)
                q = jnp.sum(jnp.where(ex == mine, sl + 1.0, 0.0), axis=0, keepdims=True) - 1.0
                pm[pl.ds(el * cap, cap)] = jnp.where(slot == q, 1.0, 0.0).astype(BF16)
            wide = min(512, d)
            for m in range(d // wide):
                cols = pl.ds(m * wide, wide)
                got = jnp.dot(pm[...], u[i, :, cols], preferred_element_type=F32).astype(BF16)
                for el in BOTH:
                    xs[el, pl.ds(pl.multiple_of(i * cap, 16), cap), cols] = got[el * cap:(el + 1) * cap]

        @pl.when(step < STEPS - 1)
        def _():
            load_u(ugs[0], k + 1)

        @pl.when((step >= STEPS) & (step < 2 * STEPS - 1))
        def _():
            load_u(ugs[1], k + 1)

        @loop(2)
        def _(el):
            @pl.when(step == 0)
            def _():
                pltpu.make_async_copy(w13.at[el], w13.at[el], wsem.at[el]).wait()
                pltpu.make_async_copy(w2.at[el], w2.at[el], w2sem.at[el]).wait()

            group = 2
            for j in range(0, f // LANES, group):
                g = min(group, f // LANES - j)
                a = jnp.dot(xs[el], w13[el, :, pl.ds(256 * j, 256 * g)], preferred_element_type=F32)
                for i in range(g):
                    a1, a3 = a[:, 256 * i:256 * i + LANES], a[:, 256 * i + LANES:256 * i + 256]
                    h[:, pl.ds(LANES * (j + i), LANES)] = (jax.nn.silu(a1) * a3).astype(BF16)

            @pl.when(step >= 1)
            def _():
                wait_kept(el)

            wide = min(512, d)
            for m in range(d // wide):
                cols = pl.ds(m * wide, wide)
                ys[el, :, cols] = jnp.dot(h[...], w2[el, :, cols], preferred_element_type=F32).astype(BF16)
            keep(p, k, el)

    for el in BOTH:
        wait_kept(el)


def _dense(h0, cs, ln1, wq, wk, wv, wo, ln2, ws1, ws3, ws2, z, hb, xb, wa, wf, wg, qb, kb, vb, ob, hs, ct, zs, hsem, asem, fsem, gsem, zsem, hook):
    t, d = hb.shape
    wide, narrow = qb.shape[1], wf.shape[3]
    groups, chunks = d // wide, ws1.shape[1] // narrow
    tall, tile = t // 2, t // 4

    def load_a(i):
        b, cols = i % 2, pl.ds(pl.multiple_of(i % groups * wide, wide), wide)

        @pl.when(i < groups)
        def _():
            for j, w in enumerate((wq, wk, wv)):
                pltpu.make_async_copy(w.at[:, cols], wa.at[b, j], asem.at[b]).start()

        @pl.when((i >= groups) & (i < 2 * groups))
        def _():
            pltpu.make_async_copy(wo.at[:, cols], wa.at[b, 0], asem.at[b]).start()

    def load_f(j):
        @pl.when(j < chunks)
        def _():
            for i, w in enumerate((ws1, ws3)):
                cols = pl.ds(pl.multiple_of(j * narrow, narrow), narrow)
                pltpu.make_async_copy(w.at[:, cols], wf.at[j % 2, i], fsem.at[j % 2]).start()

    def load_g(j):
        @pl.when(j < groups)
        def _():
            pltpu.make_async_copy(ws2.at[:, pl.ds(pl.multiple_of(j * wide, wide), wide)], wg.at[j % 2], gsem.at[j % 2]).start()

    def wait(ref, sem):
        pltpu.make_async_copy(ref, ref, sem).wait()

    pltpu.make_async_copy(h0, hb, hsem).start()
    pltpu.make_async_copy(cs, ct, hsem).start()
    for load in (load_a, load_f, load_g):
        for i in BOTH:
            load(jnp.int32(i))
    wait(hb, hsem)
    wait(ct, hsem)

    def norm(ln):
        w = ln[...].astype(F32)

        @loop(t // tile)
        def _(i):
            rows = pl.ds(pl.multiple_of(i * tile, tile), tile)
            xb[rows] = _norm(hb[rows].astype(F32), w)

    norm(ln1)

    @loop(groups)
    def _(g):
        b = g % 2
        hook('group', g)
        wait(wa.at[b], asem.at[b])

        @loop(t // tall)
        def _(m):
            rows = pl.ds(pl.multiple_of(m * tall, tall), tall)
            c, s = ct[0, rows], ct[1, rows]
            for j, out in enumerate((qb, kb)):
                v = _dot(xb[rows], wa[b, j])
                for i in range(wide // HEAD):
                    head = v[:, i * HEAD:(i + 1) * HEAD]
                    out[rows, pl.ds(i * HEAD, HEAD)] = (head * c + pltpu.roll(head, HEAD // 2, 1) * s).astype(BF16)
            vb[rows] = _dot(xb[rows], wa[b, 2]).astype(BF16)

        load_a(g + 2)

        @loop(wide // HEAD)
        def _(i):
            cols = pl.ds(pl.multiple_of(i * HEAD, HEAD), HEAD)
            causal = lax.broadcasted_iota(jnp.int32, (tile, tile), 0) >= lax.broadcasted_iota(jnp.int32, (tile, tile), 1)
            for m in range(t // tile):
                rows, past = pl.ds(m * tile, tile), pl.ds(0, m * tile)
                q = qb[rows, cols]

                def scores(keys):
                    return lax.dot_general(q, kb[keys, cols], NT, preferred_element_type=F32) * HEAD ** -0.5

                here = jnp.where(causal, scores(rows), -1e30)
                top = jnp.max(here, axis=-1, keepdims=True)
                if m:
                    before = scores(past)
                    top = jnp.maximum(top, jnp.max(before, axis=-1, keepdims=True))
                    before = jnp.exp(before - top)
                here = jnp.exp(here - top)
                total = jnp.sum(here, axis=-1, keepdims=True)
                if m:
                    total = total + jnp.sum(before, axis=-1, keepdims=True)
                share = 1.0 / total
                o = _dot((here * share).astype(BF16), vb[rows, cols])
                if m:
                    o = o + _dot((before * share).astype(BF16), vb[past, cols])
                ob[rows, pl.ds(pl.multiple_of(g * wide + i * HEAD, HEAD), HEAD)] = o.astype(BF16)

    @loop(groups)
    def _(g):
        b = g % 2
        cols = pl.ds(pl.multiple_of(g * wide, wide), wide)
        wait(wa.at[b, 0], asem.at[b])

        @loop(t // tall)
        def _(m):
            rows = pl.ds(pl.multiple_of(m * tall, tall), tall)
            hb[rows, cols] = (hb[rows, cols].astype(F32) + _dot(ob[rows], wa[b, 0])).astype(BF16)

        load_a(g + groups + 2)

    norm(ln2)

    @loop(chunks)
    def _(j):
        b = j % 2
        hook('chunk', j)
        wait(wf.at[b], fsem.at[b])

        @loop(t // tall)
        def _(m):
            rows = pl.ds(pl.multiple_of(m * tall, tall), tall)
            x = xb[rows]
            a1, a3 = _dot(x, wf[b, 0]), _dot(x, wf[b, 1])
            hs[rows, pl.ds(pl.multiple_of(j * narrow, narrow), narrow)] = (jax.nn.silu(a1) * a3).astype(BF16)

        load_f(j + 2)

    hook('down', None)

    def z_copy(g, m):
        cols = pl.ds(pl.multiple_of(g * wide, wide), wide)
        return pltpu.make_async_copy(zs.at[m], z.at[pl.ds(pl.multiple_of(m * tall, tall), tall), cols], zsem.at[m])

    @loop(groups)
    def _(g):
        b = g % 2
        cols = pl.ds(pl.multiple_of(g * wide, wide), wide)
        wait(wg.at[b], gsem.at[b])

        @loop(t // tall)
        def _(m):
            rows = pl.ds(pl.multiple_of(m * tall, tall), tall)

            @pl.when(g >= 1)
            def _():
                z_copy(g, m).wait()

            zs[m] = hb[rows, cols].astype(F32) + _dot(hs[rows], wg[b])
            z_copy(g, m).start()

        load_g(g + 2)

    for m in BOTH:
        wait(zs.at[m], zsem.at[m])


def _dense_scratch(t, d, fs):
    wide, narrow = 4 * HEAD, 2 * HEAD
    head = pltpu.VMEM((t, wide), BF16)
    full = pltpu.VMEM((t, d), BF16)
    return [
        full,
        full,
        pltpu.VMEM((PAIR, 3, d, wide), BF16),
        pltpu.VMEM((PAIR, PAIR, d, narrow), BF16),
        pltpu.VMEM((PAIR, fs, wide), BF16),
        head,
        head,
        head,
        full,
        pltpu.VMEM((t, fs), BF16),
        pltpu.VMEM((PAIR, t, HEAD), F32),
        pltpu.VMEM((PAIR, t // 2, wide), F32),
    ]


DENSE_SEMS = [SEM, SEM2, SEM2, SEM2, SEM2]


def _ffn_scratch(t, d, f, cap):
    cap2 = 2 * cap
    return [
        pltpu.VMEM((PAIR, d, 2 * f), BF16),
        pltpu.VMEM((PAIR, f, d), BF16),
        pltpu.VMEM((PAIR, t, d), BF16),
        pltpu.VMEM((PAIR, PAIR, 8, d), BF16),
        pltpu.VMEM((cap2, t), BF16),
        pltpu.VMEM((PAIR, cap2, d), BF16),
        pltpu.VMEM((cap2, f), BF16),
        pltpu.VMEM((PAIR, cap2, d), BF16),
    ]


FFN_SEMS = [SEM2] * 2 + [SEM4, SEM2]


def _split(a, b):
    return a + ((b - a) // 8 + 1) // 2 * 8


BOTH_NEAR, BOTH_FAR = ((0, -1), (1, 1)), ((0, 2), (1, 2))
STAGE = {0: 1, -1: 2, 1: 3, 2: 4}


class _Gather:
    def __init__(self, n, own, out, send_sem, recv_sem, pair_sem):
        self.side, self.me, self.x, self.y, self.c = _place(n)
        self.own, self.out = own, out
        self.send_sem, self.recv_sem, self.pair_sem = send_sem, recv_sem, pair_sem
        rows = own.shape[0]
        mid = _split(0, rows)
        self.rows = ((0, mid), (mid, rows))

    def device(self, axis, off, cc):
        side = self.side
        return ((self.y + axis * off) % side * side + (self.x + (1 - axis) * off) % side) * CORES + cc

    def place(self, color, j, s, part=None):
        side = self.side
        dx, dy = (j, s) if color == 0 else (s, j)
        chip = (self.y + dy + side) % side * side + (self.x + dx + side) % side
        a, b = self.rows[color]
        if part is not None:
            mid = _split(a, b)
            a, b = (a, mid) if part == 0 else (mid, b)
        return self.out.at[chip, self.c, pl.ds(a, b - a)]

    def copy(self, color, src, dst, axis, way, sem):
        dest = self.device(axis, STEP[way], self.c)
        pltpu.make_async_remote_copy(src, dst, self.send_sem, sem, device_id={'ep': dest}, device_id_type=MESH).start()

    def share(self, src, dst):
        other = self.device(0, 0, 1 - self.c)
        pltpu.make_async_remote_copy(src, dst, self.pair_sem.at[0], self.pair_sem.at[1], device_id={'ep': other}, device_id_type=MESH).start()

    def wait(self, ref, sem):
        pltpu.make_async_copy(ref, ref, sem).wait()

    def start(self):
        for color in BOTH:
            a, b = self.rows[color]
            src, dst = self.own.at[pl.ds(a, b - a)], self.place(color, 0, 0)
            for stage in BOTH:
                for way in BOTH:
                    self.copy(color, src, dst, color if stage == 0 else 1 - color, way, self.recv_sem.at[color, stage, way])
            self.share(src, dst)

    def along(self, j):
        items = []
        for color in BOTH:
            for way, off in (BOTH_FAR if j == 2 else BOTH_NEAR):
                if j == 2:
                    self.wait(self.place(color, off, 0, way), self.recv_sem.at[color, 0, 2 + way])
                else:
                    self.wait(self.place(color, off, 0), self.recv_sem.at[color, 0, way])
                    half = self.place(color, off, 0, way)
                    self.copy(color, half, half, color, way, self.recv_sem.at[color, 0, 2 + way])
                    items.append((color, off))
            if j == 2:
                items.append((color, j))
        for color, off in items:
            item = self.place(color, off, 0)
            for way in BOTH:
                self.copy(color, item, item, 1 - color, way, self.recv_sem.at[color, STAGE[off], way])
            self.share(item, item)

    def across(self, offs):
        for color in BOTH:
            for off in offs:
                at = STAGE[off]
                for way, s in BOTH_NEAR:
                    item = self.place(color, off, s)
                    self.wait(item, self.recv_sem.at[color, at, way])
                    half = self.place(color, off, s, way)
                    self.copy(color, half, half, 1 - color, way, self.recv_sem.at[color, at, 2 + way])
                    self.share(item, item)

    def last(self, offs):
        for color in BOTH:
            for off in offs:
                at = STAGE[off]
                for way in BOTH:
                    self.wait(self.place(color, off, 2, way), self.recv_sem.at[color, at, 2 + way])
                item = self.place(color, off, 2)
                self.share(item, item)

    def finish(self):
        got = self.out.at[:, 0]
        self.wait(got, self.pair_sem.at[1])

    def drain(self):
        chips = self.out.shape[0]
        self.wait(self.out.at[:, 0], self.pair_sem.at[0])
        self.wait(self.out.at[pl.ds(0, chips - 1), 0], self.send_sem)


def _k2(n, cap, keep, part0, part1, ue1, ue3, ue2, *refs):
    dense_in, refs = refs[:11], refs[11:]
    rxf, z, ug0, ug1, ys, r, rl, rx2, mr, *refs = refs
    dense_sems, refs = refs[:5], refs[5:]
    wsem, w2sem, usem, ysem, gsem, grsem, pairsem, osem, ssem, rsem, relsem, fsem, lsem, msem, bsem, r2sem, rfsem = refs
    side, me, x, y, c = _place(n)
    t, d = rxf.shape[1], rxf.shape[2]
    f = ue1.shape[2]
    kk, dh = r.shape[2], r.shape[3]
    tile = rx2.shape[3]
    experts = kk // cap
    far = side // 2
    units = 16
    th, cap2 = t // 2, 2 * cap
    gathers = [_Gather(n, part, ug, gsem.at[p], grsem.at[p], pairsem.at[p]) for p, (part, ug) in enumerate(((part0, ug0), (part1, ug1)))]

    def device(axis, off, cc):
        return ((y + axis * off) % side * side + (x + (1 - axis) * off) % side) * CORES + cc

    def remote(src, dst, send_sem, recv_sem, dest):
        return pltpu.make_async_remote_copy(src, dst, send_sem, recv_sem, device_id={'ep': dest}, device_id_type=MESH)

    def routing_rows(p, ug):
        axis = (c + p) % 2
        for off in range(side):
            pltpu.make_async_copy(ug.at[device(axis, off, 0) // CORES, :, pl.ds(th, 8)], mr.at[p, off], msem).start()

    kept = [pltpu.make_async_copy(part, ug.at[me // CORES, c], osem.at[p]) for p, (part, ug) in enumerate(((part0, ug0), (part1, ug1)))]
    for cp in kept:
        cp.start()

    barrier = pltpu.get_barrier_semaphore()
    peers = 0
    for off in range(side):
        for dc in range(CORES):
            for axis in BOTH:
                if off or (dc and not axis):
                    pl.semaphore_signal(barrier, device_id={'ep': device(axis, off, (c + dc) % CORES)}, device_id_type=MESH)
                    peers += 1
    pl.semaphore_wait(barrier, peers)

    def send(p, k, want_far):
        for i in BOTH:
            dx, dy = _order(k, i)
            for half, off, other, mine, line in ((0, dy, dx, y, (x + dx) % side), (1, dx, dy, x, (y + dy) % side)):
                cc = (p + half) % 2
                src = ys.at[p, 2 * k + i, half]

                def near():
                    own = (off == 0) & (c == cc)
                    dst = r.at[p, line, pl.ds((mine * CORES + c) * cap2, cap2)]

                    @pl.when(own)
                    def _():
                        pltpu.make_async_copy(src, dst, rsem.at[p, line]).start()

                    @pl.when(jnp.logical_not(own) & (off != far))
                    def _():
                        remote(src, dst, ssem.at[p], rsem.at[p, line], device(1 - half, off, cc)).start()

                def relayed():
                    @pl.when(off == far)
                    def _():
                        for el in BOTH:
                            at = (p, half, el, other)
                            remote(src.at[pl.ds(el * cap, cap)], rl.at[at], ssem.at[p], relsem.at[at], device(1 - half, STEP[el], c)).start()

                if want_far != 0:
                    relayed()
                if want_far != 1:
                    near()

    def forward(p, other):
        for half, mine, line in ((0, y, (x + other) % side), (1, x, (y + other) % side)):
            for el in BOTH:
                at = (p, half, el, other)
                step = STEP[el]
                pltpu.make_async_copy(rl.at[at], rl.at[at], relsem.at[at]).wait()
                origin = (mine - step + side) % side
                dst = r.at[p, line, pl.ds((origin * CORES + c) * cap2 + el * cap, cap)]
                remote(rl.at[at], dst, fsem.at[p], rsem.at[p, line], device(1 - half, step, (p + half) % 2)).start()

    first, second = gathers
    first.start()

    def hook(name, i):
        if name == 'group':
            @pl.when(i == 2)
            def _():
                first.along(1)

            @pl.when(i == 3)
            def _():
                first.across((0,))
        elif name == 'chunk':
            @pl.when(i == 4)
            def _():
                first.along(2)
        else:
            first.across((-1, 1))

    def dense_phase(*refs):
        _dense(*dense_in, z, *refs, *dense_sems, hook=hook)

    pl.run_scoped(dense_phase, *_dense_scratch(t, d, dense_in[8].shape[1]))
    first.last((0,))
    first.across((2,))
    second.start()
    first.last((-1, 1, 2))
    kept[0].wait()
    first.finish()
    routing_rows(0, ug0)

    def before(step):
        def at(s):
            return pl.when(step == s)

        @at(1)
        def _():
            second.along(1)

        @at(2)
        def _():
            second.across((0,))

        @at(3)
        def _():
            second.along(2)

        @at(4)
        def _():
            second.across((-1, 1))

        @at(5)
        def _():
            second.last((0,))

        @at(6)
        def _():
            second.across((2,))

            for want in (1, 0):
                @loop(5)
                def _(k):
                    send(0, k, want)

        @at(8)
        def _():
            second.last((-1, 1, 2))
            kept[1].wait()
            second.finish()
            routing_rows(1, ug1)

        @pl.when((step >= 7) & (step < 10))
        def _():
            send(0, step - 2, 0)

        @at(10)
        def _():
            @loop(side)
            def _(other):
                forward(0, other)

        @pl.when(step >= 10)
        def _():
            send(1, step - 10, 2)

    def experts_phase(*refs):
        _ffn(n, cap, (ug0, ug1), ue1, ue3, ue2, ys, *refs, wsem, w2sem, usem, ysem, before=before)

    pl.run_scoped(experts_phase, *_ffn_scratch(t, d, f, cap))
    for k in (6, 7):
        send(1, k, 0)

    def role(w):
        p, q, b = w // 8, w % 8 // 2, w % 2
        first = 1 - (q + 3) // 4
        middle = (q + 1) // 2 % 2
        off = first * far + middle * (1 + (side - 2) * b)
        return p, (c + p) % 2, off, b + middle * (q % 2) * (1 - 2 * b)

    def combine_phase(rb, mt, pma, pmb, sb):
        def load(w):
            p, axis, off, _ = role(w)
            line = (x * (1 - axis) + y * axis + off) % side
            return r.at[p, line], rsem.at[p, line], pltpu.make_async_copy(r.at[p, line], rb.at[w % 2], lsem.at[w % 2])

        def start_load(w):
            rows, sem, copy = load(w)
            q, b = w % 8 // 2, w % 2

            @pl.when((q == 1) | ((b == 0) & (q != 2)))
            def _():
                pltpu.make_async_copy(rows, rows, sem).wait()

            copy.start()

        def prepare(w):
            p, axis, off, mh = role(w)
            af = axis.astype(F32)
            ex, sl, g = _routing(mr[p, off], t)
            cy = jnp.floor(ex * (1.0 / (2 * CORES * side)))
            cx = jnp.floor((ex - cy * (2 * CORES * side)) * (1.0 / (2 * CORES)))
            low = ex - cy * (2 * CORES * side) - cx * (2 * CORES)
            mine = x.astype(F32) * (1.0 - af) + y.astype(F32) * af
            across = cx * (1.0 - af) + cy * af
            along = cy * (1.0 - af) + cx * af
            e = jnp.where(across == mine, along * (2 * CORES) + low, -1.0)
            gap = jnp.zeros((2, t), F32)
            m = jnp.concatenate([e, gap, sl, gap, g, jnp.zeros((106, t), F32)])
            for i in BOTH:
                @pl.when(mh == i)
                def _():
                    mt[w % 2] = m[:, i * 2 * tile:(i + 1) * 2 * tile].T

        def build(pm, w, i):
            rows = mt[w % 2, pl.ds(i * tile, tile)]
            lane = lax.broadcasted_iota(jnp.int32, (tile, LANES), 1).astype(F32)
            slot = jnp.zeros((tile, LANES), F32)
            gate = jnp.zeros((tile, LANES), F32)
            for j in range(6):
                hit = lane == rows[:, j:j + 1]
                slot = slot + jnp.where(hit, rows[:, 8 + j:9 + j] + 4096.0, 0.0)
                gate = gate + jnp.where(hit, rows[:, 16 + j:17 + j], 0.0)
            slot = slot - 4096.0
            for k0 in range(0, kk, LANES):
                v = jnp.zeros((tile, LANES), F32)
                for e in range(k0 // cap, min(experts - 1, (k0 + 127) // cap) + 1):
                    v = jnp.where(lane + float(k0 - e * cap) == slot[:, e:e + 1], gate[:, e:e + 1], v)
                for i_part, part in enumerate(_parts(v)):
                    pm[pl.ds(i_part * tile, tile), pl.ds(k0, LANES)] = part

        def send_sum(w, i):
            p, axis, off, mh = role(w)
            b = w % keep
            src = sb.at[b * 2 + i]
            rows = pl.ds((mh * 2 + i) * tile, tile)
            out = [rxf.at[j, rows, pl.ds(pl.multiple_of(axis * dh, dh), dh)] for j in range(3)]

            for way in BOTH:
                step = STEP[way]

                @pl.when((off == far) & (mh == way))
                def _():
                    remote(src, rx2.at[p, way, i], bsem.at[b], r2sem.at[p, way, i], device(axis, step, c)).start()

                @pl.when(off == (side + step) % side)
                def _():
                    remote(src, out[way], bsem.at[b], rfsem.at[way], device(axis, step, p)).start()

            @pl.when((off == 0) & (axis == 0))
            def _():
                pltpu.make_async_copy(src, out[2], bsem.at[b]).start()

            @pl.when((off == 0) & (axis == 1))
            def _():
                remote(src, out[2], bsem.at[b], rfsem.at[2], device(axis, 0, p)).start()

        def wait_sent(b):
            sent = sb.at[pl.ds(b * 2, 2)]
            pltpu.make_async_copy(sent, sent, bsem.at[b]).wait()

        pltpu.make_async_copy(mr, mr, msem).wait()
        start_load(0)
        prepare(0)
        build(pma, 0, 0)

        @loop(units)
        def _(w):
            p, axis, off, mh = role(w)
            after = w + 1 - (w + 1) // units
            load(w)[2].wait()

            @pl.when(w + 1 < units)
            def _():
                start_load(w + 1)
                prepare(w + 1)

            @pl.when(w == 2)
            def _():
                forward(1, far)

            @pl.when(w == 3)
            def _():
                for other in range(side):
                    if other != far:
                        forward(1, other)

            @pl.when(w >= keep)
            def _():
                wait_sent(w % keep)

            for i, pm in ((0, pma), (1, pmb)):
                here = w % keep * 2 + i
                wide = min(512, dh)
                for j in range(dh // wide):
                    cols = pl.ds(j * wide, wide)
                    o = jnp.dot(pm[...], rb[w % 2, :, cols], preferred_element_type=F32)
                    sb[here, :, cols] = o[:tile] + o[tile:2 * tile] + o[2 * tile:]
                if i == 0:
                    build(pmb, w, 1)
                else:
                    build(pma, after, 0)

                for way in BOTH:
                    @pl.when((off == (side + STEP[way]) % side) & (mh == way))
                    def _():
                        got = rx2.at[p, way, i]
                        pltpu.make_async_copy(got, got, r2sem.at[p, way, i]).wait()
                        sb[here] = sb[here] + rx2[p, way, i]

                send_sum(w, i)

        for w in range(units - keep, units):
            wait_sent(w % keep)

    pl.run_scoped(
        combine_phase,
        pltpu.VMEM((PAIR, kk, dh), BF16),
        pltpu.VMEM((PAIR, 2 * tile, LANES), F32),
        pltpu.VMEM((3 * tile, kk), BF16),
        pltpu.VMEM((3 * tile, kk), BF16),
        pltpu.VMEM((keep * 2, tile, dh), F32),
    )

    for gather in gathers:
        gather.drain()
    for p in BOTH:
        blocks = ys.at[p, pl.ds(0, 2 * STEPS - 2)]
        pltpu.make_async_copy(blocks, blocks, ssem.at[p]).wait()
        pltpu.make_async_copy(rl.at[p], rl.at[p], fsem.at[p]).wait()
    for j, got in enumerate((rxf.at[0], rxf.at[1], rxf.at[2, :, pl.ds(dh, dh)])):
        pltpu.make_async_copy(got, got, rfsem.at[j]).wait()


ANY = pl.BlockSpec(memory_space=pl.ANY)


def _rows(h0, idx, slot, ln, wr, n):
    t, d = h0.shape
    vmem = pl.BlockSpec(memory_space=pltpu.VMEM)
    return pl.pallas_call(
        functools.partial(_k0, n),
        out_shape=(jax.ShapeDtypeStruct((t // 2 + 8, d), BF16),) * CORES,
        in_specs=[ANY] + [vmem] * 4,
        out_specs=(ANY,) * CORES,
        scratch_shapes=[
            pltpu.VMEM((t, d), BF16),
            pltpu.VMEM((PAIR, t // 2, d), BF16),
            pltpu.VMEM((PAIR, 8, d), BF16),
            SEM4,
            SEM2,
            SEM2,
            SEM2,
        ],
        cost_estimate=pl.CostEstimate(flops=2 * t * d * 64, bytes_accessed=8 * t * d, transcendentals=0),
        compiler_params=pltpu.CompilerParams(collective_id=1, has_side_effects=True),
        name='rows',
    )(h0, idx, slot, ln, wr)


def _layer(parts, experts, dense, n, cap, t):
    d, f, fs = parts[0].shape[-1], experts[0].shape[-1], dense[8].shape[-1]
    dh = d // 2
    side = math.isqrt(n // CORES)
    tile = t // 4
    kk = CORES * side * 2 * cap
    keep = 4
    cap2 = 2 * cap
    vmem = pl.BlockSpec(memory_space=pltpu.VMEM)
    gathered = jax.ShapeDtypeStruct((n // CORES, CORES) + parts[0].shape, BF16)
    return pl.pallas_call(
        functools.partial(_k2, n, cap, keep),
        out_shape=(
            jax.ShapeDtypeStruct((3, t, d), F32),
            jax.ShapeDtypeStruct((t, d), F32),
            gathered,
            gathered,
            jax.ShapeDtypeStruct((PAIR, PAIR * STEPS, PAIR, cap2, dh), BF16),
            jax.ShapeDtypeStruct((PAIR, side, kk, dh), BF16),
            jax.ShapeDtypeStruct((PAIR, PAIR, PAIR, side, cap, dh), BF16),
        ),
        in_specs=[ANY] * 7 + [vmem, ANY, ANY, ANY, ANY, vmem, ANY, ANY, ANY],
        out_specs=(ANY,) * 7,
        scratch_shapes=[
            pltpu.VMEM((PAIR, PAIR, PAIR, tile, dh), F32),
            pltpu.VMEM((PAIR, side, 2, 8, d), BF16),
        ] + DENSE_SEMS + FFN_SEMS + [
            SEM2,
            SEM((PAIR, PAIR, 5, 4)),
            SEM((PAIR, PAIR)),
            SEM2,
            SEM2,
            SEM((PAIR, side)),
            SEM((PAIR, PAIR, PAIR, side)),
            SEM2,
            SEM2,
            SEM,
            SEM((keep,)),
            SEM((PAIR, PAIR, PAIR)),
            SEM((3,)),
        ],
        compiler_params=pltpu.CompilerParams(collective_id=0, has_side_effects=True, vmem_limit_bytes=67043328),
        name='layer',
    )(*parts, *experts, *dense)[:2]


def solution(mesh):
    n = mesh.shape['ep']
    rows = P(('dp', 'ep'))
    rep = P()

    def local(h0, idx, slot, ln_attn, wq, wk, wv, wo, ln_ffn, ws1, ws3, ws2, ln_moe, wr, ue1, ue3, ue2):
        b, s, d = h0.shape
        top = idx.shape[-1]
        ne = ue1.shape[0] * n
        t = b * s
        cap = CAP_FACTOR * t * top // ne
        parts = _rows(h0.reshape(t, d), idx.reshape(t, top).T, slot.reshape(t, top).T, ln_moe.reshape(1, d), wr.T, n)
        flat = h0.reshape(t, d)
        dense = (flat, _turns(t), ln_attn.reshape(1, d), wq, wk, wv, wo, ln_ffn.reshape(1, d), ws1, ws3, ws2)
        r, z = _layer(parts, (ue1, ue3, ue2), dense, n, cap, t)
        return (z + (r[0] + r[1] + r[2])).astype(BF16).reshape(b, s, d)

    specs = (rows, rows, rows) + (rep,) * 11 + (P('ep'), P('ep'), P('ep'))
    return jax.shard_map(local, mesh=mesh, in_specs=specs, out_specs=rows, check_vma=False)
```

```python
import functools
import math

import jax
import jax.numpy as jnp
from jax import lax
from jax.experimental import pallas as pl
from jax.experimental.pallas import tpu as pltpu
from jax.sharding import PartitionSpec as P

HEAD = 128
LANES = 128
EPS = 1e-6
CAP_FACTOR = 2
CORES = 2
F32 = jnp.float32
BF16 = jnp.bfloat16
MESH = pl.DeviceIdType.MESH
BOTH = (0, 1)
PAIR = 2
NT = (((1,), (1,)), ((), ()))
STEP = (1, -1)
loop = functools.partial(pl.loop, 0)
SEM = pltpu.SemaphoreType.DMA
SEM2, SEM4 = SEM((2,)), SEM((4,))


def _turns(t):
    half = HEAD // 2
    freq = 10000.0 ** (-jnp.arange(half, dtype=F32) / half)
    ang = jnp.arange(t, dtype=F32)[:, None] * freq[None, :]
    return jnp.cos(ang), jnp.sin(ang)


def _norm(xf, w):
    return (xf * lax.rsqrt(jnp.mean(xf * xf, axis=-1, keepdims=True) + EPS) * w).astype(BF16)


def _weight(ln):
    w = ln[...].astype(F32)
    return jnp.concatenate([w[i:i + 1] for i in range(w.shape[0])], axis=1)


def _dot(a, b):
    return jnp.dot(a, b, preferred_element_type=F32)


def _parts(c):
    hi = c.astype(jnp.bfloat16)
    r = c - hi.astype(jnp.float32)
    mid = r.astype(jnp.bfloat16)
    lo = (r - mid.astype(jnp.float32)).astype(jnp.bfloat16)
    return hi, mid, lo


def _place(n):
    side = math.isqrt(n // CORES)
    me = lax.axis_index('ep')
    return side, me, (me // CORES) % side, me // (CORES * side), me % CORES


def _pick(table, k):
    power = (1 + 3 * (k % 2)) * (1 + 15 * (k // 2 % 2)) * (1 + 255 * (k // 4))
    return table // power % 4


def _pack(values):
    return sum(int(v) * 4 ** i for i, v in enumerate(values))


STEP_X = (_pack('22101110'), _pack('22303330'))
STEP_Y = (_pack('21221301'), _pack('03203103'))
STEPS = 8


def _order(k, i):
    return _pick(STEP_X[i], k), _pick(STEP_Y[i], k)


def _routing(rows, t):
    e = rows.astype(F32)
    half = t // 2

    def block(q):
        return jnp.concatenate([e[i][:, q * half:(q + 1) * half] for i in BOTH], axis=1)

    b = [block(q) for q in range(4)]
    lo = jnp.concatenate([b[0][6:], b[1][6:], b[2][6:]])
    return b[0][:6], b[1][:6], b[2][:6] + b[3][:6] + lo


def _own_rows(n, h0, idx, slot, ln, wr, out0, out1, hb, ub, eb, hsem, lsem, ssem, rsem, barrier):
    side, me, x, y, c = _place(n)
    t = hb.shape[0]
    half, tile, ne = t // 2, t // 4, wr.shape[0]
    order = (1 - c, c)

    def h_copy(o, i):
        rows = pl.ds(pl.multiple_of((order[o] * 2 + i) * tile, tile), tile)
        return pltpu.make_async_copy(h0.at[rows], hb.at[pl.ds((o * 2 + i) * tile, tile)], hsem.at[o * 2 + i])

    for o in BOTH:
        for i in BOTH:
            h_copy(o, i).start()

    other = me + 1 - 2 * c
    barrier()

    def gives(out):
        return [
            pltpu.make_async_remote_copy(src, out.at[rows], ssem.at[j], rsem.at[j], device_id={'ep': other}, device_id_type=MESH)
            for j, (src, rows) in enumerate(((ub.at[0], pl.ds(0, half)), (eb.at[0], pl.ds(half, 8))))
        ]

    def keeps(out):
        return [
            pltpu.make_async_copy(src, out.at[rows], lsem.at[j])
            for j, (src, rows) in enumerate(((ub.at[1], pl.ds(0, half)), (eb.at[1], pl.ds(half, 8))))
        ]

    w = _weight(ln)
    expert = lax.broadcasted_iota(jnp.int32, (ne, tile), 0)
    for o in BOTH:
        for i in BOTH:
            h_copy(o, i).wait()
            xf = hb[pl.ds((o * 2 + i) * tile, tile)].astype(F32)
            u = _norm(xf, w)
            ub[o, pl.ds(i * tile, tile)] = u
            lg = lax.dot_general(wr[...], u, NT, preferred_element_type=F32)
            cols = pl.ds(pl.multiple_of((order[o] * 2 + i) * tile, tile), tile)
            ex, sl = idx[:, cols], slot[:, cols]
            pick = [jnp.sum(jnp.where(expert == ex[j:j + 1], lg, 0.0), axis=0, keepdims=True) for j in range(6)]
            top = functools.reduce(jnp.maximum, pick)
            e = [jnp.exp(v - top) for v in pick]
            total = functools.reduce(jnp.add, e)
            parts = [_parts(v / total) for v in e]
            hi, mid, lo = ([p[q].astype(F32) for p in parts] for q in range(3))
            exf, slf = ex.astype(F32), sl.astype(F32)
            zero = jnp.zeros((1, tile), F32)
            blocks = ([exf] + lo[:2], [slf] + lo[2:4], hi + lo[4:], mid + [zero, zero])
            for q, rows in enumerate(blocks):
                eb[o, :, pl.ds(q * half + i * tile, tile)] = jnp.concatenate(rows).astype(BF16)
        for p, out in enumerate((out0, out1)):
            @pl.when(c == p)
            def _():
                for cp in (gives(out) if o == 0 else keeps(out)):
                    cp.start()
    for cp in gives(out0) + keeps(out0):
        cp.wait()


def _ffn(n, cap, ugs, ue1, ue3, ue2, y_out, w13, w2, u, ur, pm, xs, h, ys, wsem, w2sem, usem, ysem, before):
    side, me, x, y, c = _place(n)
    t, d = pm.shape[1], u.shape[2]
    f = h.shape[1]
    dh, th = d // 2, t // 2

    def load_u(ug, k):
        for i in BOTH:
            dx, dy = _order(k, i)
            chip = (y + dy) % side * side + (x + dx) % side
            for j in BOTH:
                pltpu.make_async_copy(ug.at[chip, j, pl.ds(0, th)], u.at[i, pl.ds(j * th, th)], usem.at[i]).start()
                pltpu.make_async_copy(ug.at[chip, j, pl.ds(th, 8)], ur.at[i, j], usem.at[2 + i]).start()

    def weights(el):
        for j in range(f // LANES):
            pltpu.make_async_copy(ue1.at[el, :, pl.ds(LANES * j, LANES)], w13.at[el, :, pl.ds(256 * j, LANES)], wsem.at[el]).start()
            pltpu.make_async_copy(ue3.at[el, :, pl.ds(LANES * j, LANES)], w13.at[el, :, pl.ds(256 * j + LANES, LANES)], wsem.at[el]).start()
        pltpu.make_async_copy(ue2.at[el], w2.at[el], w2sem.at[el]).start()

    def keep(p, k, el):
        for i in BOTH:
            for half in BOTH:
                pltpu.make_async_copy(
                    ys.at[el, pl.ds(i * cap, cap), pl.ds(half * dh, dh)],
                    y_out.at[p, 2 * k + i, half, pl.ds(el * cap, cap)], ysem.at[el]).start()

    def wait_kept(el):
        pltpu.make_async_copy(ys.at[el], ys.at[el], ysem.at[el]).wait()

    load_u(ugs[0], 0)
    for el in BOTH:
        weights(el)

    @loop(2 * STEPS)
    def _(step):
        p, k = step // STEPS, step % STEPS
        before(step)

        @pl.when(step == STEPS)
        def _():
            load_u(ugs[1], 0)

        @loop(2)
        def _(i):
            pltpu.make_async_copy(u.at[i], u.at[i], usem.at[i]).wait()
            pltpu.make_async_copy(ur.at[i], ur.at[i], usem.at[2 + i]).wait()
            ex, sl, _ = _routing(ur[i], t)
            slot = lax.broadcasted_iota(jnp.int32, (cap, t), 0).astype(F32)
            for el in BOTH:
                mine = (me * 2 + el).astype(F32)
                q = jnp.sum(jnp.where(ex == mine, sl + 1.0, 0.0), axis=0, keepdims=True) - 1.0
                pm[pl.ds(el * cap, cap)] = jnp.where(slot == q, 1.0, 0.0).astype(BF16)
            wide = min(512, d)
            for m in range(d // wide):
                cols = pl.ds(m * wide, wide)
                got = jnp.dot(pm[...], u[i, :, cols], preferred_element_type=F32).astype(BF16)
                for el in BOTH:
                    xs[el, pl.ds(pl.multiple_of(i * cap, 16), cap), cols] = got[el * cap:(el + 1) * cap]

        @pl.when(step < STEPS - 1)
        def _():
            load_u(ugs[0], k + 1)

        @pl.when((step >= STEPS) & (step < 2 * STEPS - 1))
        def _():
            load_u(ugs[1], k + 1)

        @loop(2)
        def _(el):
            @pl.when(step == 0)
            def _():
                pltpu.make_async_copy(w13.at[el], w13.at[el], wsem.at[el]).wait()
                pltpu.make_async_copy(w2.at[el], w2.at[el], w2sem.at[el]).wait()

            group = 2
            for j in range(0, f // LANES, group):
                g = min(group, f // LANES - j)
                a = jnp.dot(xs[el], w13[el, :, pl.ds(256 * j, 256 * g)], preferred_element_type=F32)
                for i in range(g):
                    a1, a3 = a[:, 256 * i:256 * i + LANES], a[:, 256 * i + LANES:256 * i + 256]
                    h[:, pl.ds(LANES * (j + i), LANES)] = (jax.nn.silu(a1) * a3).astype(BF16)

            @pl.when(step >= 1)
            def _():
                wait_kept(el)

            wide = min(512, d)
            for m in range(d // wide):
                cols = pl.ds(m * wide, wide)
                ys[el, :, cols] = jnp.dot(h[...], w2[el, :, cols], preferred_element_type=F32).astype(BF16)
            keep(p, k, el)

    for el in BOTH:
        wait_kept(el)


def _dense(h0, cos, sin, wq, wk, wv, wo, ws1, ws3, ws2, lns, z, hb, xb, wa, wf, wg, qb, kb, vb, ob, hs, ct, zs, hsem, asem, fsem, gsem, zsem, hook):
    t, d = hb.shape
    wide, narrow = qb.shape[1], wf.shape[3]
    groups, chunks = d // wide, ws1.shape[1] // narrow
    tall, tile = t // 2, t // 4

    def load_a(i):
        b, cols = i % 2, pl.ds(pl.multiple_of(i % groups * wide, wide), wide)

        @pl.when(i < groups)
        def _():
            for j, w in enumerate((wq, wk, wv)):
                pltpu.make_async_copy(w.at[:, cols], wa.at[b, j], asem.at[b]).start()

        @pl.when((i >= groups) & (i < 2 * groups))
        def _():
            pltpu.make_async_copy(wo.at[:, cols], wa.at[b, 0], asem.at[b]).start()

    def load_f(j):
        @pl.when(j < chunks)
        def _():
            for i, w in enumerate((ws1, ws3)):
                cols = pl.ds(pl.multiple_of(j * narrow, narrow), narrow)
                pltpu.make_async_copy(w.at[:, cols], wf.at[j % 2, i], fsem.at[j % 2]).start()

    def load_g(j):
        @pl.when(j < groups)
        def _():
            pltpu.make_async_copy(ws2.at[:, pl.ds(pl.multiple_of(j * wide, wide), wide)], wg.at[j % 2], gsem.at[j % 2]).start()

    def wait(ref, sem):
        pltpu.make_async_copy(ref, ref, sem).wait()

    pltpu.make_async_copy(h0, hb, hsem).start()
    for i, v in enumerate((cos, sin)):
        pltpu.make_async_copy(v, ct.at[i], hsem).start()
    for load in (load_a, load_f, load_g):
        for i in BOTH:
            load(jnp.int32(i))
    wait(hb, hsem)
    wait(ct, hsem)

    def norm(ln):
        w = _weight(ln)

        @loop(t // tile)
        def _(i):
            rows = pl.ds(pl.multiple_of(i * tile, tile), tile)
            xb[rows] = _norm(hb[rows].astype(F32), w)

    norm(lns[0])

    @loop(groups)
    def _(g):
        b = g % 2
        hook('group', g)
        wait(wa.at[b], asem.at[b])

        @loop(t // tall)
        def _(m):
            rows = pl.ds(pl.multiple_of(m * tall, tall), tall)
            c, s = ct[0, rows], ct[1, rows]
            c, s = jnp.concatenate([c, c], axis=1), jnp.concatenate([-s, s], axis=1)
            for j, out in enumerate((qb, kb)):
                v = _dot(xb[rows], wa[b, j])
                for i in range(wide // HEAD):
                    head = v[:, i * HEAD:(i + 1) * HEAD]
                    out[rows, pl.ds(i * HEAD, HEAD)] = (head * c + pltpu.roll(head, HEAD // 2, 1) * s).astype(BF16)
            vb[rows] = _dot(xb[rows], wa[b, 2]).astype(BF16)

        load_a(g + 2)

        @loop(wide // HEAD)
        def _(i):
            cols = pl.ds(pl.multiple_of(i * HEAD, HEAD), HEAD)
            causal = lax.broadcasted_iota(jnp.int32, (tile, tile), 0) >= lax.broadcasted_iota(jnp.int32, (tile, tile), 1)
            for m in range(t // tile):
                rows, past = pl.ds(m * tile, tile), pl.ds(0, m * tile)
                q = qb[rows, cols]

                def scores(keys):
                    return lax.dot_general(q, kb[keys, cols], NT, preferred_element_type=F32) * HEAD ** -0.5

                here = jnp.where(causal, scores(rows), -1e30)
                top = jnp.max(here, axis=-1, keepdims=True)
                if m:
                    before = scores(past)
                    top = jnp.maximum(top, jnp.max(before, axis=-1, keepdims=True))
                    before = jnp.exp(before - top)
                here = jnp.exp(here - top)
                total = jnp.sum(here, axis=-1, keepdims=True)
                if m:
                    total = total + jnp.sum(before, axis=-1, keepdims=True)
                share = 1.0 / total
                o = _dot((here * share).astype(BF16), vb[rows, cols])
                if m:
                    o = o + _dot((before * share).astype(BF16), vb[past, cols])
                ob[rows, pl.ds(pl.multiple_of(g * wide + i * HEAD, HEAD), HEAD)] = o.astype(BF16)

    @loop(groups)
    def _(g):
        b = g % 2
        cols = pl.ds(pl.multiple_of(g * wide, wide), wide)
        wait(wa.at[b, 0], asem.at[b])

        @loop(t // tall)
        def _(m):
            rows = pl.ds(pl.multiple_of(m * tall, tall), tall)
            hb[rows, cols] = (hb[rows, cols].astype(F32) + _dot(ob[rows], wa[b, 0])).astype(BF16)

        load_a(g + groups + 2)

    norm(lns[1])

    @loop(chunks)
    def _(j):
        b = j % 2
        hook('chunk', j)
        wait(wf.at[b], fsem.at[b])

        @loop(t // tall)
        def _(m):
            rows = pl.ds(pl.multiple_of(m * tall, tall), tall)
            x = xb[rows]
            a1, a3 = _dot(x, wf[b, 0]), _dot(x, wf[b, 1])
            hs[rows, pl.ds(pl.multiple_of(j * narrow, narrow), narrow)] = (jax.nn.silu(a1) * a3).astype(BF16)

        load_f(j + 2)

    hook('down', None)

    def z_copy(g, m):
        cols = pl.ds(pl.multiple_of(g * wide, wide), wide)
        return pltpu.make_async_copy(zs.at[m], z.at[pl.ds(pl.multiple_of(m * tall, tall), tall), cols], zsem.at[m])

    @loop(groups)
    def _(g):
        b = g % 2
        cols = pl.ds(pl.multiple_of(g * wide, wide), wide)
        wait(wg.at[b], gsem.at[b])

        @loop(t // tall)
        def _(m):
            rows = pl.ds(pl.multiple_of(m * tall, tall), tall)

            @pl.when(g >= 1)
            def _():
                z_copy(g, m).wait()

            zs[m] = hb[rows, cols].astype(F32) + _dot(hs[rows], wg[b])
            z_copy(g, m).start()

        load_g(g + 2)

    for m in BOTH:
        wait(zs.at[m], zsem.at[m])


def _dense_scratch(t, d, fs):
    wide, narrow = 4 * HEAD, 2 * HEAD
    head = pltpu.VMEM((t, wide), BF16)
    full = pltpu.VMEM((t, d), BF16)
    return [
        full,
        full,
        pltpu.VMEM((PAIR, 3, d, wide), BF16),
        pltpu.VMEM((PAIR, PAIR, d, narrow), BF16),
        pltpu.VMEM((PAIR, fs, wide), BF16),
        head,
        head,
        head,
        full,
        pltpu.VMEM((t, fs), BF16),
        pltpu.VMEM((PAIR, t, HEAD // 2), F32),
        pltpu.VMEM((PAIR, t // 2, wide), F32),
    ]


DENSE_SEMS = [SEM, SEM2, SEM2, SEM2, SEM2]


def _ffn_scratch(t, d, f, cap):
    cap2 = 2 * cap
    return [
        pltpu.VMEM((PAIR, d, 2 * f), BF16),
        pltpu.VMEM((PAIR, f, d), BF16),
        pltpu.VMEM((PAIR, t, d), BF16),
        pltpu.VMEM((PAIR, PAIR, 8, d), BF16),
        pltpu.VMEM((cap2, t), BF16),
        pltpu.VMEM((PAIR, cap2, d), BF16),
        pltpu.VMEM((cap2, f), BF16),
        pltpu.VMEM((PAIR, cap2, d), BF16),
    ]


FFN_SEMS = [SEM2] * 2 + [SEM4, SEM2]


def _split(a, b):
    return a + ((b - a) // 8 + 1) // 2 * 8


BOTH_NEAR, BOTH_FAR = ((0, -1), (1, 1)), ((0, 2), (1, 2))
STAGE = {0: 1, -1: 2, 1: 3, 2: 4}


class _Gather:
    def __init__(self, n, own, out, send_sem, recv_sem, pair_sem):
        self.side, self.me, self.x, self.y, self.c = _place(n)
        self.own, self.out = own, out
        self.send_sem, self.recv_sem, self.pair_sem = send_sem, recv_sem, pair_sem
        rows = own.shape[0]
        mid = _split(0, rows)
        self.rows = ((0, mid), (mid, rows))

    def device(self, axis, off, cc):
        side = self.side
        return ((self.y + axis * off) % side * side + (self.x + (1 - axis) * off) % side) * CORES + cc

    def place(self, color, j, s, part=None):
        side = self.side
        dx, dy = (j, s) if color == 0 else (s, j)
        chip = (self.y + dy + side) % side * side + (self.x + dx + side) % side
        a, b = self.rows[color]
        if part is not None:
            mid = _split(a, b)
            a, b = (a, mid) if part == 0 else (mid, b)
        return self.out.at[chip, self.c, pl.ds(a, b - a)]

    def copy(self, color, src, dst, axis, way, sem):
        dest = self.device(axis, STEP[way], self.c)
        pltpu.make_async_remote_copy(src, dst, self.send_sem, sem, device_id={'ep': dest}, device_id_type=MESH).start()

    def share(self, src, dst):
        other = self.device(0, 0, 1 - self.c)
        pltpu.make_async_remote_copy(src, dst, self.pair_sem.at[0], self.pair_sem.at[1], device_id={'ep': other}, device_id_type=MESH).start()

    def wait(self, ref, sem):
        pltpu.make_async_copy(ref, ref, sem).wait()

    def start(self):
        for color in BOTH:
            a, b = self.rows[color]
            src, dst = self.own.at[pl.ds(a, b - a)], self.place(color, 0, 0)
            for stage in BOTH:
                for way in BOTH:
                    self.copy(color, src, dst, color if stage == 0 else 1 - color, way, self.recv_sem.at[color, stage, way])
            self.share(src, dst)

    def along(self, j):
        items = []
        for color in BOTH:
            for way, off in (BOTH_FAR if j == 2 else BOTH_NEAR):
                if j == 2:
                    self.wait(self.place(color, off, 0, way), self.recv_sem.at[color, 0, 2 + way])
                else:
                    self.wait(self.place(color, off, 0), self.recv_sem.at[color, 0, way])
                    half = self.place(color, off, 0, way)
                    self.copy(color, half, half, color, way, self.recv_sem.at[color, 0, 2 + way])
                    items.append((color, off))
            if j == 2:
                items.append((color, j))
        for color, off in items:
            item = self.place(color, off, 0)
            for way in BOTH:
                self.copy(color, item, item, 1 - color, way, self.recv_sem.at[color, STAGE[off], way])
            self.share(item, item)

    def across(self, offs):
        for color in BOTH:
            for off in offs:
                at = STAGE[off]
                for way, s in BOTH_NEAR:
                    item = self.place(color, off, s)
                    self.wait(item, self.recv_sem.at[color, at, way])
                    half = self.place(color, off, s, way)
                    self.copy(color, half, half, 1 - color, way, self.recv_sem.at[color, at, 2 + way])
                    self.share(item, item)

    def last(self, offs):
        for color in BOTH:
            for off in offs:
                at = STAGE[off]
                for way in BOTH:
                    self.wait(self.place(color, off, 2, way), self.recv_sem.at[color, at, 2 + way])
                item = self.place(color, off, 2)
                self.share(item, item)

    def finish(self):
        got = self.out.at[:, 0]
        self.wait(got, self.pair_sem.at[1])

    def drain(self):
        chips = self.out.shape[0]
        self.wait(self.out.at[:, 0], self.pair_sem.at[0])
        self.wait(self.out.at[pl.ds(0, chips - 1), 0], self.send_sem)


def _k2(n, cap, keep, idx, slot, ln_moe, ln_attn, ln_ffn, wr, ue1, ue3, ue2, *refs):
    dense_in, refs = refs[:10], refs[10:]
    rxf, z, zx, part0, part1, ug0, ug1, ys, r, rl, rx2, mr, *refs = refs
    row_sems, dense_sems, refs = refs[:4], refs[4:9], refs[9:]
    wsem, w2sem, usem, ysem, gsem, grsem, pairsem, osem, ssem, rsem, relsem, fsem, lsem, msem, bsem, r2sem, rfsem, zsem, zbsem = refs
    side, me, x, y, c = _place(n)
    t, d = rxf.shape[1], rxf.shape[2]
    f = ue1.shape[2]
    kk, dh = r.shape[2], r.shape[3]
    tile = rx2.shape[3]
    experts = kk // cap
    far = side // 2
    units = 16
    th, cap2 = t // 2, 2 * cap
    gathers = [_Gather(n, part, ug, gsem.at[p], grsem.at[p], pairsem.at[p]) for p, (part, ug) in enumerate(((part0, ug0), (part1, ug1)))]

    def device(axis, off, cc):
        return ((y + axis * off) % side * side + (x + (1 - axis) * off) % side) * CORES + cc

    def remote(src, dst, send_sem, recv_sem, dest):
        return pltpu.make_async_remote_copy(src, dst, send_sem, recv_sem, device_id={'ep': dest}, device_id_type=MESH)

    def routing_rows(p, ug):
        axis = (c + p) % 2
        for off in range(side):
            pltpu.make_async_copy(ug.at[device(axis, off, 0) // CORES, :, pl.ds(th, 8)], mr.at[p, off], msem).start()

    def barrier():
        here = pltpu.get_barrier_semaphore()
        peers = 0
        for off in range(side):
            for dc in range(CORES):
                for axis in BOTH:
                    if off or (dc and not axis):
                        pl.semaphore_signal(here, device_id={'ep': device(axis, off, (c + dc) % CORES)}, device_id_type=MESH)
                        peers += 1
        pl.semaphore_wait(here, peers)

    def rows_phase(*refs):
        _own_rows(n, dense_in[0], idx, slot, ln_moe, wr, part0, part1, *refs, *row_sems, barrier)

    pl.run_scoped(rows_phase, pltpu.VMEM((t, d), BF16), pltpu.VMEM((PAIR, th, d), BF16), pltpu.VMEM((PAIR, 8, d), BF16))
    kept = [pltpu.make_async_copy(part, ug.at[me // CORES, c], osem.at[p]) for p, (part, ug) in enumerate(((part0, ug0), (part1, ug1)))]

    def send(p, k, want_far):
        for i in BOTH:
            dx, dy = _order(k, i)
            for half, off, other, mine, line in ((0, dy, dx, y, (x + dx) % side), (1, dx, dy, x, (y + dy) % side)):
                cc = (p + half) % 2
                src = ys.at[p, 2 * k + i, half]

                def near():
                    own = (off == 0) & (c == cc)
                    dst = r.at[p, line, pl.ds((mine * CORES + c) * cap2, cap2)]

                    @pl.when(own)
                    def _():
                        pltpu.make_async_copy(src, dst, rsem.at[p, line]).start()

                    @pl.when(jnp.logical_not(own) & (off != far))
                    def _():
                        remote(src, dst, ssem.at[p], rsem.at[p, line], device(1 - half, off, cc)).start()

                def relayed():
                    @pl.when(off == far)
                    def _():
                        for el in BOTH:
                            at = (p, half, el, other)
                            remote(src.at[pl.ds(el * cap, cap)], rl.at[at], ssem.at[p], relsem.at[at], device(1 - half, STEP[el], c)).start()

                if want_far != 0:
                    relayed()
                if want_far != 1:
                    near()

    def forward(p, other):
        for half, mine, line in ((0, y, (x + other) % side), (1, x, (y + other) % side)):
            for el in BOTH:
                at = (p, half, el, other)
                step = STEP[el]
                pltpu.make_async_copy(rl.at[at], rl.at[at], relsem.at[at]).wait()
                origin = (mine - step + side) % side
                dst = r.at[p, line, pl.ds((origin * CORES + c) * cap2 + el * cap, cap)]
                remote(rl.at[at], dst, fsem.at[p], rsem.at[p, line], device(1 - half, step, (p + half) % 2)).start()

    first, second = gathers
    first.start()
    for cp in kept:
        cp.start()

    def hook(name, i):
        if name == 'group':
            @pl.when(i == 2)
            def _():
                first.along(1)

            @pl.when(i == 3)
            def _():
                first.across((0,))
        elif name == 'chunk':
            @pl.when(i == 4)
            def _():
                first.along(2)
        else:
            first.across((-1, 1))

    def dense_phase(*refs):
        _dense(*dense_in, (ln_attn, ln_ffn), z, *refs, *dense_sems, hook=hook)

    pl.run_scoped(dense_phase, *_dense_scratch(t, d, dense_in[7].shape[1]))
    z_given = remote(z.at[:, pl.ds(dh, dh)], zx, zsem.at[0], zsem.at[1], device(0, 0, 1 - c))
    z_given.start()
    first.last((0,))
    first.across((2,))
    second.start()
    first.last((-1, 1, 2))
    kept[0].wait()
    first.finish()
    routing_rows(0, ug0)

    def before(step):
        def at(s):
            return pl.when(step == s)

        @at(1)
        def _():
            second.along(1)

        @at(2)
        def _():
            second.across((0,))

        @at(3)
        def _():
            second.along(2)

        @at(4)
        def _():
            second.across((-1, 1))

        @at(5)
        def _():
            second.last((0,))

        @at(6)
        def _():
            second.across((2,))

            for want in (1, 0):
                @loop(5)
                def _(k):
                    send(0, k, want)

        @at(8)
        def _():
            second.last((-1, 1, 2))
            kept[1].wait()
            second.finish()
            routing_rows(1, ug1)

        @pl.when((step >= 7) & (step < 10))
        def _():
            send(0, step - 2, 0)

        @at(10)
        def _():
            @loop(side)
            def _(other):
                forward(0, other)

        @pl.when(step >= 10)
        def _():
            send(1, step - 10, 2)

    def experts_phase(*refs):
        _ffn(n, cap, (ug0, ug1), ue1, ue3, ue2, ys, *refs, wsem, w2sem, usem, ysem, before=before)

    pl.run_scoped(experts_phase, *_ffn_scratch(t, d, f, cap))
    for k in (6, 7):
        send(1, k, 0)

    def role(w):
        p, q, b = w // 8, w % 8 // 2, w % 2
        first = 1 - (q + 3) // 4
        middle = (q + 1) // 2 % 2
        off = first * far + middle * (1 + (side - 2) * b)
        return p, (c + p) % 2, off, b + middle * (q % 2) * (1 - 2 * b)

    def combine_phase(rb, mt, pma, pmb, sb, zb):
        def load_z(axis, m, i):
            rows = pl.ds(pl.multiple_of(m * tile, tile), tile)
            for j, src in enumerate((z.at[rows, pl.ds(0, dh)], zx.at[rows])):
                @pl.when(axis == j)
                def _():
                    pltpu.make_async_copy(src, zb.at[i], zbsem.at[i]).start()

        def load(w):
            p, axis, off, _ = role(w)
            line = (x * (1 - axis) + y * axis + off) % side
            return r.at[p, line], rsem.at[p, line], pltpu.make_async_copy(r.at[p, line], rb.at[w % 2], lsem.at[w % 2])

        def start_load(w):
            rows, sem, copy = load(w)
            q, b = w % 8 // 2, w % 2

            @pl.when((q == 1) | ((b == 0) & (q != 2)))
            def _():
                pltpu.make_async_copy(rows, rows, sem).wait()

            copy.start()

        def prepare(w):
            p, axis, off, mh = role(w)
            af = axis.astype(F32)
            ex, sl, g = _routing(mr[p, off], t)
            cy = jnp.floor(ex * (1.0 / (2 * CORES * side)))
            cx = jnp.floor((ex - cy * (2 * CORES * side)) * (1.0 / (2 * CORES)))
            low = ex - cy * (2 * CORES * side) - cx * (2 * CORES)
            mine = x.astype(F32) * (1.0 - af) + y.astype(F32) * af
            across = cx * (1.0 - af) + cy * af
            along = cy * (1.0 - af) + cx * af
            e = jnp.where(across == mine, along * (2 * CORES) + low, -1.0)
            gap = jnp.zeros((2, t), F32)
            m = jnp.concatenate([e, gap, sl, gap, g, jnp.zeros((106, t), F32)])
            for i in BOTH:
                @pl.when(mh == i)
                def _():
                    mt[w % 2] = m[:, i * 2 * tile:(i + 1) * 2 * tile].T

        def build(pm, w, i):
            rows = mt[w % 2, pl.ds(i * tile, tile)]
            lane = lax.broadcasted_iota(jnp.int32, (tile, LANES), 1).astype(F32)
            slot = jnp.zeros((tile, LANES), F32)
            gate = jnp.zeros((tile, LANES), F32)
            for j in range(6):
                hit = lane == rows[:, j:j + 1]
                slot = slot + jnp.where(hit, rows[:, 8 + j:9 + j] + 4096.0, 0.0)
                gate = gate + jnp.where(hit, rows[:, 16 + j:17 + j], 0.0)
            slot = slot - 4096.0
            for k0 in range(0, kk, LANES):
                v = jnp.zeros((tile, LANES), F32)
                for e in range(k0 // cap, min(experts - 1, (k0 + 127) // cap) + 1):
                    v = jnp.where(lane + float(k0 - e * cap) == slot[:, e:e + 1], gate[:, e:e + 1], v)
                for i_part, part in enumerate(_parts(v)):
                    pm[pl.ds(i_part * tile, tile), pl.ds(k0, LANES)] = part

        def send_sum(w, i):
            p, axis, off, mh = role(w)
            b = w % keep
            src = sb.at[b * 2 + i]
            rows = pl.ds((mh * 2 + i) * tile, tile)
            out = [rxf.at[j, rows, pl.ds(pl.multiple_of(axis * dh, dh), dh)] for j in range(3)]

            for way in BOTH:
                step = STEP[way]

                @pl.when((off == far) & (mh == way))
                def _():
                    remote(src, rx2.at[p, way, i], bsem.at[b], r2sem.at[p, way, i], device(axis, step, c)).start()

                @pl.when(off == (side + step) % side)
                def _():
                    remote(src, out[way], bsem.at[b], rfsem.at[way], device(axis, step, p)).start()

            @pl.when((off == 0) & (axis == 0))
            def _():
                pltpu.make_async_copy(src, out[2], bsem.at[b]).start()

            @pl.when((off == 0) & (axis == 1))
            def _():
                remote(src, out[2], bsem.at[b], rfsem.at[2], device(axis, 0, p)).start()

        def wait_sent(b):
            sent = sb.at[pl.ds(b * 2, 2)]
            pltpu.make_async_copy(sent, sent, bsem.at[b]).wait()

        pltpu.make_async_copy(mr, mr, msem).wait()
        start_load(0)
        prepare(0)
        build(pma, 0, 0)

        @loop(units)
        def _(w):
            p, axis, off, mh = role(w)
            after = w + 1 - (w + 1) // units
            load(w)[2].wait()

            @pl.when(w + 1 < units)
            def _():
                start_load(w + 1)
                prepare(w + 1)

            @pl.when(w == 2)
            def _():
                forward(1, far)

            @pl.when(w == 3)
            def _():
                for other in range(side):
                    if other != far:
                        forward(1, other)

            @pl.when(w >= keep)
            def _():
                wait_sent(w % keep)

            @pl.when(off == 0)
            def _():
                for i in BOTH:
                    load_z(axis, mh * 2 + i, i)

            for i, pm in ((0, pma), (1, pmb)):
                here = w % keep * 2 + i
                wide = min(512, dh)
                for j in range(dh // wide):
                    cols = pl.ds(j * wide, wide)
                    o = jnp.dot(pm[...], rb[w % 2, :, cols], preferred_element_type=F32)
                    sb[here, :, cols] = o[:tile] + o[tile:2 * tile] + o[2 * tile:]
                if i == 0:
                    build(pmb, w, 1)
                else:
                    build(pma, after, 0)

                for way in BOTH:
                    @pl.when((off == (side + STEP[way]) % side) & (mh == way))
                    def _():
                        got = rx2.at[p, way, i]
                        pltpu.make_async_copy(got, got, r2sem.at[p, way, i]).wait()
                        sb[here] = sb[here] + rx2[p, way, i]

                @pl.when(off == 0)
                def _():
                    pltpu.make_async_copy(zb.at[i], zb.at[i], zbsem.at[i]).wait()
                    sb[here] = sb[here] + zb[i]

                send_sum(w, i)

        for w in range(units - keep, units):
            wait_sent(w % keep)

    z_given.wait()
    pl.run_scoped(
        combine_phase,
        pltpu.VMEM((PAIR, kk, dh), BF16),
        pltpu.VMEM((PAIR, 2 * tile, LANES), F32),
        pltpu.VMEM((3 * tile, kk), BF16),
        pltpu.VMEM((3 * tile, kk), BF16),
        pltpu.VMEM((keep * 2, tile, dh), F32),
        pltpu.VMEM((PAIR, tile, dh), F32),
    )

    for gather in gathers:
        gather.drain()
    for p in BOTH:
        blocks = ys.at[p, pl.ds(0, 2 * STEPS - 2)]
        pltpu.make_async_copy(blocks, blocks, ssem.at[p]).wait()
        pltpu.make_async_copy(rl.at[p], rl.at[p], fsem.at[p]).wait()
    for j, got in enumerate((rxf.at[0], rxf.at[1], rxf.at[2, :, pl.ds(dh, dh)])):
        pltpu.make_async_copy(got, got, rfsem.at[j]).wait()


ANY = pl.BlockSpec(memory_space=pl.ANY)


def _layer(routing, experts, dense, n, cap):
    (t, d), f, fs = dense[0].shape, experts[0].shape[-1], dense[7].shape[-1]
    dh = d // 2
    side = math.isqrt(n // CORES)
    tile = t // 4
    kk = CORES * side * 2 * cap
    keep = 4
    cap2 = 2 * cap
    vmem = pl.BlockSpec(memory_space=pltpu.VMEM)
    part = jax.ShapeDtypeStruct((t // 2 + 8, d), BF16)
    gathered = jax.ShapeDtypeStruct((n // CORES, CORES) + part.shape, BF16)
    outs = (
        jax.ShapeDtypeStruct((3, t, d), F32),
        jax.ShapeDtypeStruct((t, d), F32),
        jax.ShapeDtypeStruct((t, dh), F32),
        part,
        part,
        gathered,
        gathered,
        jax.ShapeDtypeStruct((PAIR, PAIR * STEPS, PAIR, cap2, dh), BF16),
        jax.ShapeDtypeStruct((PAIR, side, kk, dh), BF16),
        jax.ShapeDtypeStruct((PAIR, PAIR, PAIR, side, cap, dh), BF16),
    )
    return pl.pallas_call(
        functools.partial(_k2, n, cap, keep),
        out_shape=outs,
        in_specs=[vmem] * len(routing) + [ANY] * (len(experts) + len(dense)),
        out_specs=(ANY,) * len(outs),
        scratch_shapes=[
            pltpu.VMEM((PAIR, PAIR, PAIR, tile, dh), F32),
            pltpu.VMEM((PAIR, side, PAIR, 8, d), BF16),
            SEM4,
            SEM2,
            SEM2,
            SEM2,
        ] + DENSE_SEMS + FFN_SEMS + [
            SEM2,
            SEM((PAIR, PAIR, 5, 4)),
            SEM((PAIR, PAIR)),
            SEM2,
            SEM2,
            SEM((PAIR, side)),
            SEM((PAIR, PAIR, PAIR, side)),
            SEM2,
            SEM2,
            SEM,
            SEM((keep,)),
            SEM((PAIR, PAIR, PAIR)),
            SEM((3,)),
            SEM2,
            SEM2,
        ],
        compiler_params=pltpu.CompilerParams(collective_id=0, has_side_effects=True, vmem_limit_bytes=67043328),
        name='layer',
    )(*routing, *experts, *dense)[0]


def _add(r, out):
    out[...] = (r[0] + r[1] + r[2]).astype(BF16)


def _total(r):
    ways, t, d = r.shape
    tile = t // 8
    return pl.pallas_call(
        _add,
        grid=(t // tile,),
        out_shape=jax.ShapeDtypeStruct((t, d), BF16),
        in_specs=[pl.BlockSpec((ways, tile, d), lambda i: (0, i, 0))],
        out_specs=pl.BlockSpec((tile, d), lambda i: (i, 0)),
        name='total',
    )(r)


def solution(mesh):
    n = mesh.shape['ep']
    rows = P(('dp', 'ep'))
    rep = P()

    def local(h0, idx, slot, ln_attn, wq, wk, wv, wo, ln_ffn, ws1, ws3, ws2, ln_moe, wr, ue1, ue3, ue2):
        b, s, d = h0.shape
        top = idx.shape[-1]
        ne = ue1.shape[0] * n
        t = b * s
        cap = CAP_FACTOR * t * top // ne
        routing = (idx.reshape(t, top).T, slot.reshape(t, top).T, *(v.reshape(d // LANES, LANES) for v in (ln_moe, ln_attn, ln_ffn)), wr.T)
        dense = (h0.reshape(t, d), *_turns(t), wq, wk, wv, wo, ws1, ws3, ws2)
        return _total(_layer(routing, (ue1, ue3, ue2), dense, n, cap)).reshape(b, s, d)

    specs = (rows, rows, rows) + (rep,) * 11 + (P('ep'), P('ep'), P('ep'))
    return jax.shard_map(local, mesh=mesh, in_specs=specs, out_specs=rows, check_vma=False)
```

```python
import functools
import math

import jax
import jax.numpy as jnp
from jax import lax
from jax.experimental import pallas as pl
from jax.experimental.pallas import tpu as pltpu
from jax.sharding import PartitionSpec as P

HEAD = 128
LANES = 128
EPS = 1e-6
CAP_FACTOR = 2
CORES = 2
F32 = jnp.float32
BF16 = jnp.bfloat16
MESH = pl.DeviceIdType.MESH
BOTH = (0, 1)
PAIR = 2
NT = (((1,), (1,)), ((), ()))
STEP = (1, -1)
loop = functools.partial(pl.loop, 0)
SEM = pltpu.SemaphoreType.DMA
SEM2, SEM4 = SEM((2,)), SEM((4,))


FINE = 32


def _turns(t):
    half = HEAD // 2
    freq = 10000.0 ** (-jnp.arange(half, dtype=F32) / half)
    pos = jnp.concatenate([FINE * jnp.arange(t // FINE, dtype=F32), jnp.arange(FINE, dtype=F32)])
    ang = pos[:, None] * freq[None, :]
    return jnp.stack([jnp.cos(ang), jnp.sin(ang)])


def _norm(xf, w):
    return (xf * lax.rsqrt(jnp.mean(xf * xf, axis=-1, keepdims=True) + EPS) * w).astype(BF16)


def _weight(ln):
    w = ln[...].astype(F32)
    return jnp.concatenate([w[i:i + 1] for i in range(w.shape[0])], axis=1)


def _dot(a, b):
    return jnp.dot(a, b, preferred_element_type=F32)


def _parts(c):
    hi = c.astype(jnp.bfloat16)
    r = c - hi.astype(jnp.float32)
    mid = r.astype(jnp.bfloat16)
    lo = (r - mid.astype(jnp.float32)).astype(jnp.bfloat16)
    return hi, mid, lo


def _place(n):
    side = math.isqrt(n // CORES)
    me = lax.axis_index('ep')
    return side, me, (me // CORES) % side, me // (CORES * side), me % CORES


def _pick(table, k):
    power = (1 + 3 * (k % 2)) * (1 + 15 * (k // 2 % 2)) * (1 + 255 * (k // 4))
    return table // power % 4


def _pack(values):
    return sum(int(v) * 4 ** i for i, v in enumerate(values))


STEP_X = (_pack('22101110'), _pack('22303330'))
STEP_Y = (_pack('21221301'), _pack('03203103'))
STEPS = 8


def _order(k, i):
    return _pick(STEP_X[i], k), _pick(STEP_Y[i], k)


def _routing(rows, t):
    e = rows.astype(F32)
    half = t // 2

    def block(q):
        return jnp.concatenate([e[i][:, q * half:(q + 1) * half] for i in BOTH], axis=1)

    b = [block(q) for q in range(4)]
    lo = jnp.concatenate([b[0][6:], b[1][6:], b[2][6:]])
    return b[0][:6], b[1][:6], b[2][:6] + b[3][:6] + lo


def _own_rows(n, h0, idx, slot, ln, wr, out0, out1, hb, ub, eb, hsem, lsem, ssem, rsem, barrier):
    side, me, x, y, c = _place(n)
    t = hb.shape[0]
    half, tile, ne = t // 2, t // 4, wr.shape[0]
    order = (1 - c, c)

    def h_copy(o, i):
        rows = pl.ds(pl.multiple_of((order[o] * 2 + i) * tile, tile), tile)
        return pltpu.make_async_copy(h0.at[rows], hb.at[pl.ds((o * 2 + i) * tile, tile)], hsem.at[o * 2 + i])

    for o in BOTH:
        for i in BOTH:
            h_copy(o, i).start()

    other = me + 1 - 2 * c
    ready = barrier()

    def gives(out):
        return [
            pltpu.make_async_remote_copy(src, out.at[rows], ssem.at[j], rsem.at[j], device_id={'ep': other}, device_id_type=MESH)
            for j, (src, rows) in enumerate(((ub.at[0], pl.ds(0, half)), (eb.at[0], pl.ds(half, 8))))
        ]

    def keeps(out):
        return [
            pltpu.make_async_copy(src, out.at[rows], lsem.at[j])
            for j, (src, rows) in enumerate(((ub.at[1], pl.ds(0, half)), (eb.at[1], pl.ds(half, 8))))
        ]

    w = _weight(ln)
    expert = lax.broadcasted_iota(jnp.int32, (ne, tile), 0)
    for o in BOTH:
        for i in BOTH:
            h_copy(o, i).wait()
            xf = hb[pl.ds((o * 2 + i) * tile, tile)].astype(F32)
            u = _norm(xf, w)
            ub[o, pl.ds(i * tile, tile)] = u
            lg = lax.dot_general(wr[...], u, NT, preferred_element_type=F32)
            cols = pl.ds(pl.multiple_of((order[o] * 2 + i) * tile, tile), tile)
            ex, sl = ([v[j, :, cols] for j in range(v.shape[0])] for v in (idx, slot))
            pick = [jnp.sum(jnp.where(expert == v, lg, 0.0), axis=0, keepdims=True) for v in ex]
            top = functools.reduce(jnp.maximum, pick)
            e = [jnp.exp(v - top) for v in pick]
            total = functools.reduce(jnp.add, e)
            parts = [_parts(v / total) for v in e]
            hi, mid, lo = ([p[q].astype(F32) for p in parts] for q in range(3))
            exf, slf = ([v.astype(F32) for v in rows] for rows in (ex, sl))
            zero = jnp.zeros((1, tile), F32)
            blocks = (exf + lo[:2], slf + lo[2:4], hi + lo[4:], mid + [zero, zero])
            for q, rows in enumerate(blocks):
                eb[o, :, pl.ds(q * half + i * tile, tile)] = jnp.concatenate(rows).astype(BF16)
        if o == 0:
            ready()
        for p, out in enumerate((out0, out1)):
            @pl.when(c == p)
            def _():
                for cp in (gives(out) if o == 0 else keeps(out)):
                    cp.start()
    for cp in gives(out0) + keeps(out0):
        cp.wait()


def _ffn(n, cap, ugs, ue1, ue3, ue2, y_out, w13, w2, u, ur, pm, xs, h, ys, wsem, w2sem, usem, ysem, before):
    side, me, x, y, c = _place(n)
    t, d = pm.shape[1], u.shape[2]
    f = h.shape[1]
    dh, th = d // 2, t // 2

    def load_u(ug, k):
        for i in BOTH:
            dx, dy = _order(k, i)
            chip = (y + dy) % side * side + (x + dx) % side
            for j in BOTH:
                pltpu.make_async_copy(ug.at[chip, j, pl.ds(0, th)], u.at[i, pl.ds(j * th, th)], usem.at[i]).start()
                pltpu.make_async_copy(ug.at[chip, j, pl.ds(th, 8)], ur.at[i, j], usem.at[2 + i]).start()

    def weights(el):
        for j in range(f // LANES):
            pltpu.make_async_copy(ue1.at[el, :, pl.ds(LANES * j, LANES)], w13.at[el, :, pl.ds(256 * j, LANES)], wsem.at[el]).start()
            pltpu.make_async_copy(ue3.at[el, :, pl.ds(LANES * j, LANES)], w13.at[el, :, pl.ds(256 * j + LANES, LANES)], wsem.at[el]).start()
        pltpu.make_async_copy(ue2.at[el], w2.at[el], w2sem.at[el]).start()

    def keep(p, k, el):
        for i in BOTH:
            for half in BOTH:
                pltpu.make_async_copy(
                    ys.at[el, pl.ds(i * cap, cap), pl.ds(half * dh, dh)],
                    y_out.at[p, 2 * k + i, half, pl.ds(el * cap, cap)], ysem.at[el]).start()

    def wait_kept(el):
        pltpu.make_async_copy(ys.at[el], ys.at[el], ysem.at[el]).wait()

    load_u(ugs[0], 0)
    for el in BOTH:
        weights(el)

    @loop(2 * STEPS)
    def _(step):
        p, k = step // STEPS, step % STEPS
        before(step)

        @pl.when(step == STEPS)
        def _():
            load_u(ugs[1], 0)

        @loop(2)
        def _(i):
            pltpu.make_async_copy(u.at[i], u.at[i], usem.at[i]).wait()
            pltpu.make_async_copy(ur.at[i], ur.at[i], usem.at[2 + i]).wait()
            ex, sl, _ = _routing(ur[i], t)
            slot = lax.broadcasted_iota(jnp.int32, (cap, t), 0).astype(F32)
            for el in BOTH:
                mine = (me * 2 + el).astype(F32)
                q = jnp.sum(jnp.where(ex == mine, sl + 1.0, 0.0), axis=0, keepdims=True) - 1.0
                pm[pl.ds(el * cap, cap)] = jnp.where(slot == q, 1.0, 0.0).astype(BF16)
            wide = min(512, d)
            for m in range(d // wide):
                cols = pl.ds(m * wide, wide)
                got = jnp.dot(pm[...], u[i, :, cols], preferred_element_type=F32).astype(BF16)
                for el in BOTH:
                    xs[el, pl.ds(pl.multiple_of(i * cap, 16), cap), cols] = got[el * cap:(el + 1) * cap]

        @pl.when(step < STEPS - 1)
        def _():
            load_u(ugs[0], k + 1)

        @pl.when((step >= STEPS) & (step < 2 * STEPS - 1))
        def _():
            load_u(ugs[1], k + 1)

        @loop(2)
        def _(el):
            @pl.when(step == 0)
            def _():
                pltpu.make_async_copy(w13.at[el], w13.at[el], wsem.at[el]).wait()
                pltpu.make_async_copy(w2.at[el], w2.at[el], w2sem.at[el]).wait()

            group = 2
            for j in range(0, f // LANES, group):
                g = min(group, f // LANES - j)
                a = jnp.dot(xs[el], w13[el, :, pl.ds(256 * j, 256 * g)], preferred_element_type=F32)
                for i in range(g):
                    a1, a3 = a[:, 256 * i:256 * i + LANES], a[:, 256 * i + LANES:256 * i + 256]
                    h[:, pl.ds(LANES * (j + i), LANES)] = (jax.nn.silu(a1) * a3).astype(BF16)

            @pl.when(step >= 1)
            def _():
                wait_kept(el)

            wide = min(512, d)
            for m in range(d // wide):
                cols = pl.ds(m * wide, wide)
                ys[el, :, cols] = jnp.dot(h[...], w2[el, :, cols], preferred_element_type=F32).astype(BF16)
            keep(p, k, el)

    for el in BOTH:
        wait_kept(el)


def _dense(h0, wq, wk, wv, wo, ws1, ws3, ws2, lns, turns, z, hb, xb, wa, wf, wg, qb, kb, vb, ob, hs, ct, zs, hsem, asem, fsem, gsem, zsem, hook):
    t, d = hb.shape
    wide, narrow = qb.shape[1], wf.shape[3]
    groups, chunks = d // wide, ws1.shape[1] // narrow
    tall, tile = t // 2, t // 4

    def load_a(i):
        b, cols = i % 2, pl.ds(pl.multiple_of(i % groups * wide, wide), wide)

        @pl.when(i < groups)
        def _():
            for j, w in enumerate((wq, wk, wv)):
                pltpu.make_async_copy(w.at[:, cols], wa.at[b, j], asem.at[b]).start()

        @pl.when((i >= groups) & (i < 2 * groups))
        def _():
            pltpu.make_async_copy(wo.at[:, cols], wa.at[b, 0], asem.at[b]).start()

    def load_f(j):
        @pl.when(j < chunks)
        def _():
            for i, w in enumerate((ws1, ws3)):
                cols = pl.ds(pl.multiple_of(j * narrow, narrow), narrow)
                pltpu.make_async_copy(w.at[:, cols], wf.at[j % 2, i], fsem.at[j % 2]).start()

    def load_g(j):
        @pl.when(j < groups)
        def _():
            pltpu.make_async_copy(ws2.at[:, pl.ds(pl.multiple_of(j * wide, wide), wide)], wg.at[j % 2], gsem.at[j % 2]).start()

    def wait(ref, sem):
        pltpu.make_async_copy(ref, ref, sem).wait()

    pltpu.make_async_copy(h0, hb, hsem).start()
    for load in (load_a, load_f, load_g):
        for i in BOTH:
            load(jnp.int32(i))
    coarse = t // FINE

    @loop(coarse)
    def _(i):
        c1, s1 = (turns[j, pl.ds(i, 1)] for j in BOTH)
        c2, s2 = (turns[j, pl.ds(coarse, FINE)] for j in BOTH)
        rows = pl.ds(pl.multiple_of(i * FINE, FINE), FINE)
        ct[0, rows] = c1 * c2 - s1 * s2
        ct[1, rows] = s1 * c2 + c1 * s2

    wait(hb, hsem)

    def norm(ln):
        w = _weight(ln)

        @loop(t // tile)
        def _(i):
            rows = pl.ds(pl.multiple_of(i * tile, tile), tile)
            xb[rows] = _norm(hb[rows].astype(F32), w)

    norm(lns[0])

    @loop(groups)
    def _(g):
        b = g % 2
        hook('group', g)
        wait(wa.at[b], asem.at[b])

        @loop(t // tall)
        def _(m):
            rows = pl.ds(pl.multiple_of(m * tall, tall), tall)
            c, s = ct[0, rows], ct[1, rows]
            c, s = jnp.concatenate([c, c], axis=1), jnp.concatenate([-s, s], axis=1)
            for j, out in enumerate((qb, kb)):
                v = _dot(xb[rows], wa[b, j])
                for i in range(wide // HEAD):
                    head = v[:, i * HEAD:(i + 1) * HEAD]
                    out[rows, pl.ds(i * HEAD, HEAD)] = (head * c + pltpu.roll(head, HEAD // 2, 1) * s).astype(BF16)
            vb[rows] = _dot(xb[rows], wa[b, 2]).astype(BF16)

        load_a(g + 2)

        @loop(wide // HEAD)
        def _(i):
            cols = pl.ds(pl.multiple_of(i * HEAD, HEAD), HEAD)
            causal = lax.broadcasted_iota(jnp.int32, (tile, tile), 0) >= lax.broadcasted_iota(jnp.int32, (tile, tile), 1)
            for m in range(t // tile):
                rows, past = pl.ds(m * tile, tile), pl.ds(0, m * tile)
                q = qb[rows, cols]

                def scores(keys):
                    return lax.dot_general(q, kb[keys, cols], NT, preferred_element_type=F32) * HEAD ** -0.5

                here = jnp.where(causal, scores(rows), -1e30)
                top = jnp.max(here, axis=-1, keepdims=True)
                if m:
                    before = scores(past)
                    top = jnp.maximum(top, jnp.max(before, axis=-1, keepdims=True))
                    before = jnp.exp(before - top)
                here = jnp.exp(here - top)
                total = jnp.sum(here, axis=-1, keepdims=True)
                if m:
                    total = total + jnp.sum(before, axis=-1, keepdims=True)
                share = 1.0 / total
                o = _dot((here * share).astype(BF16), vb[rows, cols])
                if m:
                    o = o + _dot((before * share).astype(BF16), vb[past, cols])
                ob[rows, pl.ds(pl.multiple_of(g * wide + i * HEAD, HEAD), HEAD)] = o.astype(BF16)

    @loop(groups)
    def _(g):
        b = g % 2
        cols = pl.ds(pl.multiple_of(g * wide, wide), wide)
        wait(wa.at[b, 0], asem.at[b])

        @loop(t // tall)
        def _(m):
            rows = pl.ds(pl.multiple_of(m * tall, tall), tall)
            hb[rows, cols] = (hb[rows, cols].astype(F32) + _dot(ob[rows], wa[b, 0])).astype(BF16)

        load_a(g + groups + 2)

    norm(lns[1])

    @loop(chunks)
    def _(j):
        b = j % 2
        hook('chunk', j)
        wait(wf.at[b], fsem.at[b])

        @loop(t // tall)
        def _(m):
            rows = pl.ds(pl.multiple_of(m * tall, tall), tall)
            x = xb[rows]
            a1, a3 = _dot(x, wf[b, 0]), _dot(x, wf[b, 1])
            hs[rows, pl.ds(pl.multiple_of(j * narrow, narrow), narrow)] = (jax.nn.silu(a1) * a3).astype(BF16)

        load_f(j + 2)

    hook('down', None)

    def z_copy(g, m):
        cols = pl.ds(pl.multiple_of(g * wide, wide), wide)
        return pltpu.make_async_copy(zs.at[m], z.at[pl.ds(pl.multiple_of(m * tall, tall), tall), cols], zsem.at[m])

    @loop(groups)
    def _(g):
        b = g % 2
        cols = pl.ds(pl.multiple_of(g * wide, wide), wide)
        wait(wg.at[b], gsem.at[b])

        @loop(t // tall)
        def _(m):
            rows = pl.ds(pl.multiple_of(m * tall, tall), tall)

            @pl.when(g >= 1)
            def _():
                z_copy(g, m).wait()

            zs[m] = hb[rows, cols].astype(F32) + _dot(hs[rows], wg[b])
            z_copy(g, m).start()

        load_g(g + 2)

    for m in BOTH:
        wait(zs.at[m], zsem.at[m])


def _dense_scratch(t, d, fs):
    wide, narrow = 4 * HEAD, 2 * HEAD
    head = pltpu.VMEM((t, wide), BF16)
    full = pltpu.VMEM((t, d), BF16)
    return [
        full,
        full,
        pltpu.VMEM((PAIR, 3, d, wide), BF16),
        pltpu.VMEM((PAIR, PAIR, d, narrow), BF16),
        pltpu.VMEM((PAIR, fs, wide), BF16),
        head,
        head,
        head,
        full,
        pltpu.VMEM((t, fs), BF16),
        pltpu.VMEM((PAIR, t, HEAD // 2), F32),
        pltpu.VMEM((PAIR, t // 2, wide), F32),
    ]


DENSE_SEMS = [SEM, SEM2, SEM2, SEM2, SEM2]


def _ffn_scratch(t, d, f, cap):
    cap2 = 2 * cap
    return [
        pltpu.VMEM((PAIR, d, 2 * f), BF16),
        pltpu.VMEM((PAIR, f, d), BF16),
        pltpu.VMEM((PAIR, t, d), BF16),
        pltpu.VMEM((PAIR, PAIR, 8, d), BF16),
        pltpu.VMEM((cap2, t), BF16),
        pltpu.VMEM((PAIR, cap2, d), BF16),
        pltpu.VMEM((cap2, f), BF16),
        pltpu.VMEM((PAIR, cap2, d), BF16),
    ]


FFN_SEMS = [SEM2] * 2 + [SEM4, SEM2]


def _split(a, b):
    return a + ((b - a) // 8 + 1) // 2 * 8


BOTH_NEAR, BOTH_FAR = ((0, -1), (1, 1)), ((0, 2), (1, 2))
STAGE = {0: 1, -1: 2, 1: 3, 2: 4}


class _Gather:
    def __init__(self, n, own, out, send_sem, recv_sem, pair_sem):
        self.side, self.me, self.x, self.y, self.c = _place(n)
        self.own, self.out = own, out
        self.send_sem, self.recv_sem, self.pair_sem = send_sem, recv_sem, pair_sem
        rows = own.shape[0]
        mid = _split(0, rows)
        self.rows = ((0, mid), (mid, rows))

    def device(self, axis, off, cc):
        side = self.side
        return ((self.y + axis * off) % side * side + (self.x + (1 - axis) * off) % side) * CORES + cc

    def place(self, color, j, s, part=None):
        side = self.side
        dx, dy = (j, s) if color == 0 else (s, j)
        chip = (self.y + dy + side) % side * side + (self.x + dx + side) % side
        a, b = self.rows[color]
        if part is not None:
            mid = _split(a, b)
            a, b = (a, mid) if part == 0 else (mid, b)
        return self.out.at[chip, self.c, pl.ds(a, b - a)]

    def copy(self, color, src, dst, axis, way, sem):
        dest = self.device(axis, STEP[way], self.c)
        pltpu.make_async_remote_copy(src, dst, self.send_sem, sem, device_id={'ep': dest}, device_id_type=MESH).start()

    def share(self, src, dst):
        other = self.device(0, 0, 1 - self.c)
        pltpu.make_async_remote_copy(src, dst, self.pair_sem.at[0], self.pair_sem.at[1], device_id={'ep': other}, device_id_type=MESH).start()

    def wait(self, ref, sem):
        pltpu.make_async_copy(ref, ref, sem).wait()

    def start(self):
        for color in BOTH:
            a, b = self.rows[color]
            src, dst = self.own.at[pl.ds(a, b - a)], self.place(color, 0, 0)
            for stage in BOTH:
                for way in BOTH:
                    self.copy(color, src, dst, color if stage == 0 else 1 - color, way, self.recv_sem.at[color, stage, way])
            self.share(src, dst)

    def along(self, j):
        items = []
        for color in BOTH:
            for way, off in (BOTH_FAR if j == 2 else BOTH_NEAR):
                if j == 2:
                    self.wait(self.place(color, off, 0, way), self.recv_sem.at[color, 0, 2 + way])
                else:
                    self.wait(self.place(color, off, 0), self.recv_sem.at[color, 0, way])
                    half = self.place(color, off, 0, way)
                    self.copy(color, half, half, color, way, self.recv_sem.at[color, 0, 2 + way])
                    items.append((color, off))
            if j == 2:
                items.append((color, j))
        for color, off in items:
            item = self.place(color, off, 0)
            for way in BOTH:
                self.copy(color, item, item, 1 - color, way, self.recv_sem.at[color, STAGE[off], way])
            self.share(item, item)

    def across(self, offs):
        for color in BOTH:
            for off in offs:
                at = STAGE[off]
                for way, s in BOTH_NEAR:
                    item = self.place(color, off, s)
                    self.wait(item, self.recv_sem.at[color, at, way])
                    half = self.place(color, off, s, way)
                    self.copy(color, half, half, 1 - color, way, self.recv_sem.at[color, at, 2 + way])
                    self.share(item, item)

    def last(self, offs):
        for color in BOTH:
            for off in offs:
                at = STAGE[off]
                for way in BOTH:
                    self.wait(self.place(color, off, 2, way), self.recv_sem.at[color, at, 2 + way])
                item = self.place(color, off, 2)
                self.share(item, item)

    def finish(self):
        got = self.out.at[:, 0]
        self.wait(got, self.pair_sem.at[1])

    def drain(self):
        chips = self.out.shape[0]
        self.wait(self.out.at[:, 0], self.pair_sem.at[0])
        self.wait(self.out.at[pl.ds(0, chips - 1), 0], self.send_sem)


def _k2(n, cap, keep, idx, slot, ln_moe, ln_attn, ln_ffn, turns, wr, ue1, ue3, ue2, *refs):
    dense_in, refs = refs[:8], refs[8:]
    rxf, z, zx, part0, part1, ug0, ug1, ys, r, rl, rx2, mr, *refs = refs
    row_sems, dense_sems, refs = refs[:4], refs[4:9], refs[9:]
    wsem, w2sem, usem, ysem, gsem, grsem, pairsem, osem, ssem, rsem, relsem, fsem, lsem, msem, bsem, r2sem, rfsem, zsem, zbsem = refs
    side, me, x, y, c = _place(n)
    t, d = rxf.shape[1], rxf.shape[2]
    f = ue1.shape[2]
    kk, dh = r.shape[2], r.shape[3]
    tile = rx2.shape[3]
    experts = kk // cap
    far = side // 2
    units = 16
    th, cap2 = t // 2, 2 * cap
    gathers = [_Gather(n, part, ug, gsem.at[p], grsem.at[p], pairsem.at[p]) for p, (part, ug) in enumerate(((part0, ug0), (part1, ug1)))]

    def device(axis, off, cc):
        return ((y + axis * off) % side * side + (x + (1 - axis) * off) % side) * CORES + cc

    def remote(src, dst, send_sem, recv_sem, dest):
        return pltpu.make_async_remote_copy(src, dst, send_sem, recv_sem, device_id={'ep': dest}, device_id_type=MESH)

    def routing_rows(p, ug):
        axis = (c + p) % 2
        for off in range(side):
            pltpu.make_async_copy(ug.at[device(axis, off, 0) // CORES, :, pl.ds(th, 8)], mr.at[p, off], msem).start()

    def barrier():
        here = pltpu.get_barrier_semaphore()
        peers = 0
        for off in range(side):
            for dc in range(CORES):
                for axis in BOTH:
                    if off or (dc and not axis):
                        pl.semaphore_signal(here, device_id={'ep': device(axis, off, (c + dc) % CORES)}, device_id_type=MESH)
                        peers += 1
        return functools.partial(pl.semaphore_wait, here, peers)

    def rows_phase(*refs):
        _own_rows(n, dense_in[0], idx, slot, ln_moe, wr, part0, part1, *refs, *row_sems, barrier)

    pl.run_scoped(rows_phase, pltpu.VMEM((t, d), BF16), pltpu.VMEM((PAIR, th, d), BF16), pltpu.VMEM((PAIR, 8, d), BF16))
    kept = [pltpu.make_async_copy(part, ug.at[me // CORES, c], osem.at[p]) for p, (part, ug) in enumerate(((part0, ug0), (part1, ug1)))]

    def send(p, k, want_far):
        for i in BOTH:
            dx, dy = _order(k, i)
            for half, off, other, mine, line in ((0, dy, dx, y, (x + dx) % side), (1, dx, dy, x, (y + dy) % side)):
                cc = (p + half) % 2
                src = ys.at[p, 2 * k + i, half]

                def near():
                    own = (off == 0) & (c == cc)
                    dst = r.at[p, line, pl.ds((mine * CORES + c) * cap2, cap2)]

                    @pl.when(own)
                    def _():
                        pltpu.make_async_copy(src, dst, rsem.at[p, line]).start()

                    @pl.when(jnp.logical_not(own) & (off != far))
                    def _():
                        remote(src, dst, ssem.at[p], rsem.at[p, line], device(1 - half, off, cc)).start()

                def relayed():
                    @pl.when(off == far)
                    def _():
                        for el in BOTH:
                            at = (p, half, el, other)
                            remote(src.at[pl.ds(el * cap, cap)], rl.at[at], ssem.at[p], relsem.at[at], device(1 - half, STEP[el], c)).start()

                if want_far != 0:
                    relayed()
                if want_far != 1:
                    near()

    def forward(p, other):
        for half, mine, line in ((0, y, (x + other) % side), (1, x, (y + other) % side)):
            for el in BOTH:
                at = (p, half, el, other)
                step = STEP[el]
                pltpu.make_async_copy(rl.at[at], rl.at[at], relsem.at[at]).wait()
                origin = (mine - step + side) % side
                dst = r.at[p, line, pl.ds((origin * CORES + c) * cap2 + el * cap, cap)]
                remote(rl.at[at], dst, fsem.at[p], rsem.at[p, line], device(1 - half, step, (p + half) % 2)).start()

    first, second = gathers
    first.start()
    for cp in kept:
        cp.start()

    def hook(name, i):
        if name == 'group':
            @pl.when(i == 2)
            def _():
                first.along(1)

            @pl.when(i == 3)
            def _():
                first.across((0,))
        elif name == 'chunk':
            @pl.when(i == 4)
            def _():
                first.along(2)
        else:
            first.across((-1, 1))

    def dense_phase(*refs):
        _dense(*dense_in, (ln_attn, ln_ffn), turns, z, *refs, *dense_sems, hook=hook)

    pl.run_scoped(dense_phase, *_dense_scratch(t, d, dense_in[5].shape[1]))
    z_given = remote(z.at[:, pl.ds(dh, dh)], zx, zsem.at[0], zsem.at[1], device(0, 0, 1 - c))
    z_given.start()
    first.last((0,))
    first.across((2,))
    second.start()
    first.last((-1, 1, 2))
    kept[0].wait()
    first.finish()
    routing_rows(0, ug0)

    def before(step):
        def at(s):
            return pl.when(step == s)

        @at(1)
        def _():
            second.along(1)

        @at(2)
        def _():
            second.across((0,))

        @at(3)
        def _():
            second.along(2)

        @at(4)
        def _():
            second.across((-1, 1))

        @at(5)
        def _():
            second.last((0,))

        @at(6)
        def _():
            second.across((2,))

            for want in (1, 0):
                @loop(5)
                def _(k):
                    send(0, k, want)

        @at(8)
        def _():
            second.last((-1, 1, 2))
            kept[1].wait()
            second.finish()
            routing_rows(1, ug1)

        @pl.when((step >= 7) & (step < 10))
        def _():
            send(0, step - 2, 0)

        @at(10)
        def _():
            @loop(side)
            def _(other):
                forward(0, other)

        @pl.when(step >= 10)
        def _():
            send(1, step - 10, 2)

    def experts_phase(*refs):
        _ffn(n, cap, (ug0, ug1), ue1, ue3, ue2, ys, *refs, wsem, w2sem, usem, ysem, before=before)

    pl.run_scoped(experts_phase, *_ffn_scratch(t, d, f, cap))
    for k in (6, 7):
        send(1, k, 0)

    def role(w):
        p, q, b = w // 8, w % 8 // 2, w % 2
        first = 1 - (q + 3) // 4
        middle = (q + 1) // 2 % 2
        off = first * far + middle * (1 + (side - 2) * b)
        return p, (c + p) % 2, off, b + middle * (q % 2) * (1 - 2 * b)

    def combine_phase(rb, mt, pma, pmb, sb, zb):
        def load_z(axis, m, i):
            rows = pl.ds(pl.multiple_of(m * tile, tile), tile)
            for j, src in enumerate((z.at[rows, pl.ds(0, dh)], zx.at[rows])):
                @pl.when(axis == j)
                def _():
                    pltpu.make_async_copy(src, zb.at[i], zbsem.at[i]).start()

        def load(w):
            p, axis, off, _ = role(w)
            line = (x * (1 - axis) + y * axis + off) % side
            return r.at[p, line], rsem.at[p, line], pltpu.make_async_copy(r.at[p, line], rb.at[w % 2], lsem.at[w % 2])

        def start_load(w):
            rows, sem, copy = load(w)
            q, b = w % 8 // 2, w % 2

            @pl.when((q == 1) | ((b == 0) & (q != 2)))
            def _():
                pltpu.make_async_copy(rows, rows, sem).wait()

            copy.start()

        def prepare(w):
            p, axis, off, mh = role(w)
            af = axis.astype(F32)
            ex, sl, g = _routing(mr[p, off], t)
            cy = jnp.floor(ex * (1.0 / (2 * CORES * side)))
            cx = jnp.floor((ex - cy * (2 * CORES * side)) * (1.0 / (2 * CORES)))
            low = ex - cy * (2 * CORES * side) - cx * (2 * CORES)
            mine = x.astype(F32) * (1.0 - af) + y.astype(F32) * af
            across = cx * (1.0 - af) + cy * af
            along = cy * (1.0 - af) + cx * af
            e = jnp.where(across == mine, along * (2 * CORES) + low, -1.0)
            gap = jnp.zeros((2, t), F32)
            m = jnp.concatenate([e, gap, sl, gap, g, jnp.zeros((106, t), F32)])
            for i in BOTH:
                @pl.when(mh == i)
                def _():
                    mt[w % 2] = m[:, i * 2 * tile:(i + 1) * 2 * tile].T

        def build(pm, w, i):
            rows = mt[w % 2, pl.ds(i * tile, tile)]
            lane = lax.broadcasted_iota(jnp.int32, (tile, LANES), 1).astype(F32)
            slot = jnp.zeros((tile, LANES), F32)
            gate = jnp.zeros((tile, LANES), F32)
            for j in range(6):
                hit = lane == rows[:, j:j + 1]
                slot = slot + jnp.where(hit, rows[:, 8 + j:9 + j] + 4096.0, 0.0)
                gate = gate + jnp.where(hit, rows[:, 16 + j:17 + j], 0.0)
            slot = slot - 4096.0
            for k0 in range(0, kk, LANES):
                v = jnp.zeros((tile, LANES), F32)
                for e in range(k0 // cap, min(experts - 1, (k0 + 127) // cap) + 1):
                    v = jnp.where(lane + float(k0 - e * cap) == slot[:, e:e + 1], gate[:, e:e + 1], v)
                for i_part, part in enumerate(_parts(v)):
                    pm[pl.ds(i_part * tile, tile), pl.ds(k0, LANES)] = part

        def send_sum(w, i):
            p, axis, off, mh = role(w)
            b = w % keep
            src = sb.at[b * 2 + i]
            rows = pl.ds((mh * 2 + i) * tile, tile)
            out = [rxf.at[j, rows, pl.ds(pl.multiple_of(axis * dh, dh), dh)] for j in range(3)]

            for way in BOTH:
                step = STEP[way]

                @pl.when((off == far) & (mh == way))
                def _():
                    remote(src, rx2.at[p, way, i], bsem.at[b], r2sem.at[p, way, i], device(axis, step, c)).start()

                @pl.when(off == (side + step) % side)
                def _():
                    remote(src, out[way], bsem.at[b], rfsem.at[way], device(axis, step, p)).start()

            @pl.when((off == 0) & (axis == 0))
            def _():
                pltpu.make_async_copy(src, out[2], bsem.at[b]).start()

            @pl.when((off == 0) & (axis == 1))
            def _():
                remote(src, out[2], bsem.at[b], rfsem.at[2], device(axis, 0, p)).start()

        def wait_sent(b):
            sent = sb.at[pl.ds(b * 2, 2)]
            pltpu.make_async_copy(sent, sent, bsem.at[b]).wait()

        pltpu.make_async_copy(mr, mr, msem).wait()
        start_load(0)
        prepare(0)
        build(pma, 0, 0)

        @loop(units)
        def _(w):
            p, axis, off, mh = role(w)
            after = w + 1 - (w + 1) // units
            load(w)[2].wait()

            @pl.when(w + 1 < units)
            def _():
                start_load(w + 1)
                prepare(w + 1)

            @pl.when(w == 2)
            def _():
                forward(1, far)

            @pl.when(w == 3)
            def _():
                for other in range(side):
                    if other != far:
                        forward(1, other)

            @pl.when(w >= keep)
            def _():
                wait_sent(w % keep)

            @pl.when(off == 0)
            def _():
                for i in BOTH:
                    load_z(axis, mh * 2 + i, i)

            for i, pm in ((0, pma), (1, pmb)):
                here = w % keep * 2 + i
                wide = min(512, dh)
                for j in range(dh // wide):
                    cols = pl.ds(j * wide, wide)
                    o = jnp.dot(pm[...], rb[w % 2, :, cols], preferred_element_type=F32)
                    sb[here, :, cols] = o[:tile] + o[tile:2 * tile] + o[2 * tile:]
                if i == 0:
                    build(pmb, w, 1)
                else:
                    build(pma, after, 0)

                for way in BOTH:
                    @pl.when((off == (side + STEP[way]) % side) & (mh == way))
                    def _():
                        got = rx2.at[p, way, i]
                        pltpu.make_async_copy(got, got, r2sem.at[p, way, i]).wait()
                        sb[here] = sb[here] + rx2[p, way, i]

                @pl.when(off == 0)
                def _():
                    pltpu.make_async_copy(zb.at[i], zb.at[i], zbsem.at[i]).wait()
                    sb[here] = sb[here] + zb[i]

                send_sum(w, i)

        for w in range(units - keep, units):
            wait_sent(w % keep)

    z_given.wait()
    pl.run_scoped(
        combine_phase,
        pltpu.VMEM((PAIR, kk, dh), BF16),
        pltpu.VMEM((PAIR, 2 * tile, LANES), F32),
        pltpu.VMEM((3 * tile, kk), BF16),
        pltpu.VMEM((3 * tile, kk), BF16),
        pltpu.VMEM((keep * 2, tile, dh), F32),
        pltpu.VMEM((PAIR, tile, dh), F32),
    )

    for gather in gathers:
        gather.drain()
    for p in BOTH:
        blocks = ys.at[p, pl.ds(0, 2 * STEPS - 2)]
        pltpu.make_async_copy(blocks, blocks, ssem.at[p]).wait()
        pltpu.make_async_copy(rl.at[p], rl.at[p], fsem.at[p]).wait()
    for j, got in enumerate((rxf.at[0], rxf.at[1], rxf.at[2, :, pl.ds(dh, dh)])):
        pltpu.make_async_copy(got, got, rfsem.at[j]).wait()


ANY = pl.BlockSpec(memory_space=pl.ANY)


def _layer(routing, experts, dense, n, cap):
    (t, d), f, fs = dense[0].shape, experts[0].shape[-1], dense[5].shape[-1]
    dh = d // 2
    side = math.isqrt(n // CORES)
    tile = t // 4
    kk = CORES * side * 2 * cap
    keep = 4
    cap2 = 2 * cap
    vmem = pl.BlockSpec(memory_space=pltpu.VMEM)
    part = jax.ShapeDtypeStruct((t // 2 + 8, d), BF16)
    gathered = jax.ShapeDtypeStruct((n // CORES, CORES) + part.shape, BF16)
    outs = (
        jax.ShapeDtypeStruct((3, t, d), F32),
        jax.ShapeDtypeStruct((t, d), F32),
        jax.ShapeDtypeStruct((t, dh), F32),
        part,
        part,
        gathered,
        gathered,
        jax.ShapeDtypeStruct((PAIR, PAIR * STEPS, PAIR, cap2, dh), BF16),
        jax.ShapeDtypeStruct((PAIR, side, kk, dh), BF16),
        jax.ShapeDtypeStruct((PAIR, PAIR, PAIR, side, cap, dh), BF16),
    )
    return pl.pallas_call(
        functools.partial(_k2, n, cap, keep),
        out_shape=outs,
        in_specs=[vmem] * len(routing) + [ANY] * (len(experts) + len(dense)),
        out_specs=(ANY,) * len(outs),
        scratch_shapes=[
            pltpu.VMEM((PAIR, PAIR, PAIR, tile, dh), F32),
            pltpu.VMEM((PAIR, side, PAIR, 8, d), BF16),
            SEM4,
            SEM2,
            SEM2,
            SEM2,
        ] + DENSE_SEMS + FFN_SEMS + [
            SEM2,
            SEM((PAIR, PAIR, 5, 4)),
            SEM((PAIR, PAIR)),
            SEM2,
            SEM2,
            SEM((PAIR, side)),
            SEM((PAIR, PAIR, PAIR, side)),
            SEM2,
            SEM2,
            SEM,
            SEM((keep,)),
            SEM((PAIR, PAIR, PAIR)),
            SEM((3,)),
            SEM2,
            SEM2,
        ],
        compiler_params=pltpu.CompilerParams(collective_id=0, has_side_effects=True, vmem_limit_bytes=67043328),
        name='layer',
    )(*routing, *experts, *dense)[0]


def _add(r, out):
    out[...] = (r[0] + r[1] + r[2]).astype(BF16)


def _total(r):
    ways, t, d = r.shape
    tile = t // 16
    return pl.pallas_call(
        _add,
        grid=(t // tile,),
        out_shape=jax.ShapeDtypeStruct((t, d), BF16),
        in_specs=[pl.BlockSpec((ways, tile, d), lambda i: (0, i, 0))],
        out_specs=pl.BlockSpec((tile, d), lambda i: (i, 0)),
        name='total',
    )(r)


def solution(mesh):
    n = mesh.shape['ep']
    rows = P(('dp', 'ep'))
    rep = P()

    def local(h0, idx, slot, ln_attn, wq, wk, wv, wo, ln_ffn, ws1, ws3, ws2, ln_moe, wr, ue1, ue3, ue2):
        b, s, d = h0.shape
        top = idx.shape[-1]
        ne = ue1.shape[0] * n
        t = b * s
        cap = CAP_FACTOR * t * top // ne
        routing = (*(jnp.moveaxis(v, -1, 0) for v in (idx, slot)), *(v.reshape(d // LANES, LANES) for v in (ln_moe, ln_attn, ln_ffn)), _turns(t), wr.T)
        dense = (h0.reshape(t, d), wq, wk, wv, wo, ws1, ws3, ws2)
        return _total(_layer(routing, (ue1, ue3, ue2), dense, n, cap)).reshape(b, s, d)

    specs = (rows, rows, rows) + (rep,) * 11 + (P('ep'), P('ep'), P('ep'))
    return jax.shard_map(local, mesh=mesh, in_specs=specs, out_specs=rows, check_vma=False)
```
